16 devices in a mesh: dp: 2 (over z), tp: 8 (over y, x, core).
Axes of the slice: x: 2, y: 2, z: 2, core: 2. Of those that a mesh axis runs over, the one named last changes fastest.
Arguments:
- token_ids: int32 [16384], P('dp'), parts along dimension 0
- positions: int32 [16384], P('dp'), parts along dimension 0
- embed_table: bfloat16 [256000, 2304], P('tp')
- norm_scale: float32 [2304], replicated
- w_query: bfloat16 [2304, 2048], P(None, 'tp')
- w_key: bfloat16 [2304, 1024], replicated
- w_value: bfloat16 [2304, 1024], replicated
Outputs:
- output 1: bfloat16 [16384, 2304], P(('dp', 'tp')), parts along dimension 0
- output 2: bfloat16 [16384, 8, 256], P('dp', 'tp'), parts along dimension 0
- output 3: bfloat16 [16384, 8, 256], P('dp', 'tp'), parts along dimension 0
- output 4: bfloat16 [16384, 8, 256], P('dp', 'tp'), parts along dimension 0
There are 2 independent parts. The reference program is written for one: setup_inputs(seed, part) draws one part's arguments, and reference() takes and returns one part's arrays. A program takes and returns all parts, laid end to end along the dimension named above; an argument that names none is the same for every part.
All inputs are finite; a program needn't handle non-finite values.
Results may differ from the reference program's by a relative error of at most 0.0120345.
Values are sent between devices in bfloat16 or wider.
A program may use at most 1 GiB of HBM per device.

```python
import math
import numpy as np
import jax
import jax.numpy as jnp
from jax import lax

D = 2304
HEADS = 8
KV_HEADS = 4
VOCAB = 256000
HEAD_DIM = 256
TOKENS = 8192
KV_SLOTS = 8
START_ODDS = 256
LEVELS = 16

ID_CAPS = np.minimum(VOCAB, 16 * 2 ** np.arange(LEVELS))


def draw_ids(key):
    level_key, id_key = jax.random.split(key)
    levels_drawn = jax.random.randint(level_key, (TOKENS,), 0, LEVELS)
    upper_ids = jnp.asarray(ID_CAPS, dtype=jnp.int32)[levels_drawn]
    token_ids = jax.random.randint(id_key, (TOKENS,), 0, upper_ids, dtype=jnp.int32)
    return token_ids.at[0].set(VOCAB - 1).at[1].set(0)


def draw_positions(key):
    step_ids = jnp.arange(TOKENS, dtype=jnp.int32)
    is_start = jax.random.randint(key, (TOKENS,), 0, START_ODDS, dtype=jnp.int32) == 0
    is_start = is_start.at[0].set(True)
    start_ids = lax.cummax(jnp.where(is_start, step_ids, 0), axis=0)
    return step_ids - start_ids


def setup_inputs(seed: int = 0, part: int = 0) -> dict:
    root_key = jax.random.key(seed)
    part_key = jax.random.fold_in(root_key, part)
    id_key, pos_key = jax.random.split(part_key)
    shared = jax.random.split(root_key, 6)
    row_scale = jax.random.uniform(shared[0], (VOCAB, 1), jnp.float32, 0.25, 2.0)
    embed_table = (jax.random.normal(shared[1], (VOCAB, D), jnp.float32) * (row_scale * D ** -0.5)).astype(jnp.bfloat16)
    norm_scale = 0.5 * jax.random.normal(shared[2], (D,), jnp.float32)
    w_query = (jax.random.normal(shared[3], (D, HEADS * HEAD_DIM), jnp.float32) * D ** -0.5).astype(jnp.bfloat16)
    w_key = (jax.random.normal(shared[4], (D, KV_HEADS * HEAD_DIM), jnp.float32) * D ** -0.5).astype(jnp.bfloat16)
    w_value = (jax.random.normal(shared[5], (D, KV_HEADS * HEAD_DIM), jnp.float32) * D ** -0.5).astype(jnp.bfloat16)
    return {"token_ids": draw_ids(id_key), "positions": draw_positions(pos_key), "embed_table": embed_table, "norm_scale": norm_scale, "w_query": w_query, "w_key": w_key, "w_value": w_value}


def rotate(head_vals, cosines, sines):
    half_dim = HEAD_DIM // 2
    front_half = head_vals[..., :half_dim]
    back_half = head_vals[..., half_dim:]
    return jnp.concatenate([front_half * cosines - back_half * sines, back_half * cosines + front_half * sines], axis=-1)


def reference(token_ids, positions, embed_table, norm_scale, w_query, w_key, w_value):
    normalizer = jnp.asarray(math.sqrt(D), dtype=jnp.bfloat16)
    residual = jnp.take(embed_table, token_ids, axis=0) * normalizer
    widened = residual.astype(jnp.float32)
    inv_rms = lax.rsqrt(jnp.mean(widened * widened, axis=-1, keepdims=True) + 1e-6)
    normed = (widened * inv_rms * (1.0 + norm_scale)).astype(jnp.bfloat16)
    inv_freq = 10000.0 ** (-jnp.arange(0, HEAD_DIM, 2, dtype=jnp.float32) / HEAD_DIM)
    angles = positions.astype(jnp.float32)[:, None] * inv_freq[None, :]
    cosines = jnp.cos(angles)[:, None, :]
    sines = jnp.sin(angles)[:, None, :]
    q_lin = jnp.dot(normed, w_query, preferred_element_type=jnp.float32).astype(jnp.bfloat16)
    k_lin = jnp.dot(normed, w_key, preferred_element_type=jnp.float32).astype(jnp.bfloat16)
    v_lin = jnp.dot(normed, w_value, preferred_element_type=jnp.float32).astype(jnp.bfloat16)
    queries = (rotate(q_lin.reshape(TOKENS, HEADS, HEAD_DIM).astype(jnp.float32), cosines, sines) * HEAD_DIM ** -0.5).astype(jnp.bfloat16)
    keys_rot = rotate(k_lin.reshape(TOKENS, KV_HEADS, HEAD_DIM).astype(jnp.float32), cosines, sines).astype(jnp.bfloat16)
    repeats = KV_SLOTS // KV_HEADS
    key_heads = jnp.repeat(keys_rot, repeats, axis=1)
    value_heads = jnp.repeat(v_lin.reshape(TOKENS, KV_HEADS, HEAD_DIM), repeats, axis=1)
    return (residual, queries, key_heads, value_heads)
```

```python
import functools
import math
import jax
import jax.numpy as jnp
from jax import lax
from jax.experimental import pallas as pl
from jax.experimental.pallas import tpu as pltpu
from jax.sharding import PartitionSpec as P

HEAD_DIM = 256
EPSILON = 1e-6
ROPE_BASE = 10000.0
TILE = 128
CHUNKS = 4


def rope_tables(positions):
    inv_freq = ROPE_BASE ** (-jnp.arange(0, HEAD_DIM, 2, dtype=jnp.float32) / HEAD_DIM)
    angles = positions.astype(jnp.float32)[:, None] * inv_freq[None, :]
    return jnp.cos(angles)[:, None, :], jnp.sin(angles)[:, None, :]


def rotate(head_vals, cosines, sines):
    half_dim = head_vals.shape[-1] // 2
    front_half = head_vals[..., :half_dim]
    back_half = head_vals[..., half_dim:]
    return jnp.concatenate([front_half * cosines - back_half * sines, back_half * cosines + front_half * sines], axis=-1)


def rms_norm(resid_rows, norm_scale):
    widened = resid_rows.astype(jnp.float32)
    inv_rms = lax.rsqrt(jnp.mean(widened * widened, axis=-1, keepdims=True) + EPSILON)
    return (widened * inv_rms * (1.0 + norm_scale)).astype(jnp.bfloat16)


def project(normed, weight, cosines, sines, factor):
    linear = jnp.dot(normed, weight, preferred_element_type=jnp.float32).astype(jnp.bfloat16)
    head_view = linear.reshape(linear.shape[0], -1, HEAD_DIM).astype(jnp.float32)
    return (rotate(head_view, cosines, sines) * factor).astype(jnp.bfloat16)


def gather_kernel(tiles, width, pair_ids, cols_ref, table_ref, out_ref, pairs, sems):
    step = pl.program_id(0)
    normalizer = jnp.asarray(math.sqrt(width), dtype=jnp.bfloat16)

    def start(tile, slot, first, last):
        for row in range(first, last):
            src = pl.multiple_of(pair_ids[tile * TILE + row], 2)
            pltpu.make_async_copy(table_ref.at[pl.ds(src, 2), :], pairs.at[slot, pl.ds(2 * row, 2), :], sems.at[slot]).start()

    def wait(slot):
        pltpu.make_async_copy(table_ref.at[pl.ds(0, 2 * TILE), :], pairs.at[slot], sems.at[slot]).wait()

    @pl.when(step == 0)
    def _():
        start(0, 0, 0, TILE)
        start(1, 1, 0, TILE)

    slot = lax.rem(step, 3)
    ahead = lax.rem(step + 2, 3)
    wait(slot)
    lanes = lax.broadcasted_iota(jnp.int32, (TILE, 2 * TILE), 1)
    select = jnp.where(lanes == cols_ref[...], normalizer, jnp.zeros((), jnp.bfloat16))
    pieces = width // 256
    for piece in range(pieces):
        start(step + 2, ahead, piece * TILE // pieces, (piece + 1) * TILE // pieces)
        cols = pl.ds(piece * 256, 256)
        picked = jnp.dot(select, pairs[slot, :, cols], preferred_element_type=jnp.float32)
        out_ref[:, cols] = picked.astype(jnp.bfloat16)

    @pl.when(step == tiles - 1)
    def _():
        wait(lax.rem(step + 1, 3))
        wait(lax.rem(step + 2, 3))


def gather_rows(pair_ids, cols, table_rows):
    count = cols.shape[0]
    width = table_rows.shape[1]
    tiles = count // TILE
    padded = jnp.concatenate([pair_ids, jnp.zeros((2 * TILE,), jnp.int32)])
    grid_spec = pltpu.PrefetchScalarGridSpec(
        num_scalar_prefetch=1,
        grid=(tiles,),
        in_specs=[pl.BlockSpec((TILE, 1), lambda i, ids: (i, 0)), pl.BlockSpec(memory_space=pl.ANY)],
        out_specs=pl.BlockSpec((TILE, width), lambda i, ids: (i, 0)),
        scratch_shapes=[pltpu.VMEM((3, 2 * TILE, width), jnp.bfloat16), pltpu.SemaphoreType.DMA((3,))],
    )
    return pl.pallas_call(
        functools.partial(gather_kernel, tiles, width),
        grid_spec=grid_spec,
        out_shape=jax.ShapeDtypeStruct((count, width), jnp.bfloat16),
        compiler_params=pltpu.CompilerParams(dimension_semantics=("arbitrary",)),
        cost_estimate=pl.CostEstimate(flops=count * 25_000_000, bytes_accessed=count * width * 6, transcendentals=0),
    )(padded, cols, table_rows)


def solution(mesh):
    group_size = mesh.shape["tp"]

    def exchange(rows, bit):
        return lax.ppermute(rows, "tp", [(i, i ^ bit) for i in range(group_size)])

    def local_step(token_ids, positions, table_rows, norm_scale, w_query, w_key, w_value):
        dev_index = lax.axis_index("tp")
        vocab_rows, model_width = table_rows.shape
        local_ids = token_ids - dev_index * vocab_rows
        inside = (local_ids >= 0) & (local_ids < vocab_rows)
        safe_ids = jnp.where(inside, local_ids, 0)
        tokens = token_ids.shape[0]
        chunk_rows = tokens // group_size // CHUNKS
        half = chunk_rows // 2
        order = jnp.arange(tokens, dtype=jnp.int32)
        in_tile = (order % TILE) * 2

        def arrange(values):
            view = values.reshape(2, 2, 2, CHUNKS, 2, half)
            for axis, bit in ((0, 4), (1, 2), (2, 1)):
                flag = (dev_index // bit) % 2 == 1
                view = jnp.where(flag, jnp.flip(view, axis), view)
            halves = view.transpose(3, 2, 4, 0, 1, 5)
            first = halves[:, :, 0].transpose(0, 1, 3, 2, 4)
            second = halves[:, :, 1]
            return jnp.stack([first, second], axis=2).reshape(CHUNKS, 2, 4 * chunk_rows)

        ids = arrange(safe_ids)
        owned = arrange(inside.astype(jnp.int32))
        pair_ids = (ids // 2) * 2
        lane = (jnp.arange(4 * chunk_rows, dtype=jnp.int32) % TILE) * 2
        cols = jnp.where(owned > 0, lane + ids % 2, -1)

        pieces = []
        for chunk in range(CHUNKS):
            other = gather_rows(pair_ids[chunk, 1], cols[chunk, 1][:, None], table_rows)
            got = exchange(other, 1)
            mine = gather_rows(pair_ids[chunk, 0], cols[chunk, 0][:, None], table_rows)
            for part, bits in ((0, (2, 4)), (1, (4, 2))):
                base = part * 4 * half
                keep = [slice(base + k * half, base + (k + 1) * half) for k in range(4)]
                far = slice(base + 2 * half, base + 4 * half)
                sent = mine[far] + got[far]
                back = exchange(sent, bits[0])
                near_send = mine[keep[1]] + got[keep[1]] + back[half:]
                back2 = exchange(near_send, bits[1])
                pieces.append(mine[keep[0]] + got[keep[0]] + back[:half] + back2)
        residual = jnp.concatenate(pieces, axis=0)
        normed = lax.all_gather(rms_norm(residual, norm_scale), "tp", axis=0, tiled=True)
        cosines, sines = rope_tables(positions)
        queries = project(normed, w_query, cosines, sines, HEAD_DIM ** -0.5)
        kv_heads = w_key.shape[1] // HEAD_DIM
        slot_count = max(kv_heads, group_size)
        slots_here = slot_count // group_size
        first_head = (dev_index * slots_here) // (slot_count // kv_heads)
        key_cols = lax.dynamic_slice_in_dim(w_key, first_head * HEAD_DIM, slots_here * HEAD_DIM, axis=1)
        value_cols = lax.dynamic_slice_in_dim(w_value, first_head * HEAD_DIM, slots_here * HEAD_DIM, axis=1)
        key_heads = project(normed, key_cols, cosines, sines, 1.0)
        value_lin = jnp.dot(normed, value_cols, preferred_element_type=jnp.float32).astype(jnp.bfloat16)
        value_heads = value_lin.reshape(value_lin.shape[0], slots_here, HEAD_DIM)
        return residual, queries, key_heads, value_heads

    head_spec = P("dp", "tp", None)
    return jax.shard_map(local_step, mesh=mesh, in_specs=(P("dp"), P("dp"), P("tp", None), P(), P(None, "tp"), P(), P()), out_specs=(P(("dp", "tp"), None), head_spec, head_spec, head_spec), check_vma=False)
```

```python
import functools
import math
import jax
import jax.numpy as jnp
from jax import lax
from jax.experimental import pallas as pl
from jax.experimental.pallas import tpu as pltpu
from jax.sharding import PartitionSpec as P

HEAD_DIM = 256
EPSILON = 1e-6
ROPE_BASE = 10000.0
TILE = 128
CHUNKS = 4
SEND_ROWS = 512
CHIPS = 4
MESH_IDS = pl.DeviceIdType.MESH


def rope_tables(positions):
    inv_freq = ROPE_BASE ** (-jnp.arange(0, HEAD_DIM, 2, dtype=jnp.float32) / HEAD_DIM)
    angles = positions.astype(jnp.float32)[:, None] * inv_freq[None, :]
    return jnp.cos(angles), jnp.sin(angles)


def gather_kernel(tiles, width, pair_ids, counts, cols_ref, table_ref, *rest):
    out_ref, pairs, sems = rest[-3:]
    step = pl.program_id(0)
    normalizer = jnp.asarray(math.sqrt(width), dtype=jnp.bfloat16)

    def start(tile, slot):
        @pl.loop(0, TILE, unroll=8)
        def _(row):
            src = pair_ids[tile * TILE + row]

            @pl.when(src >= 0)
            def _():
                pltpu.make_async_copy(table_ref.at[pl.ds(pl.multiple_of(src, 2), 2), :], pairs.at[slot, pl.ds(pl.multiple_of(2 * row, 2), 2), :], sems.at[slot]).start()

    def wait(tile, slot):
        count = counts[tile]
        size = TILE
        while size:
            @pl.when((count // size) % 2 == 1)
            def _():
                pltpu.make_async_copy(table_ref.at[pl.ds(0, 2 * size), :], pairs.at[slot, pl.ds(0, 2 * size), :], sems.at[slot]).wait()
            size //= 2

    @pl.when(step == 0)
    def _():
        pairs[...] = jnp.zeros_like(pairs)
        start(0, 0)
        start(1, 1)

    slot = lax.rem(step, 3)

    @pl.when(step + 2 < tiles)
    def _():
        start(step + 2, lax.rem(step + 2, 3))

    wait(step, slot)
    lanes = lax.broadcasted_iota(jnp.int32, (TILE, 2 * TILE), 1)
    select = jnp.where(lanes == cols_ref[...], normalizer, jnp.zeros((), jnp.bfloat16))
    for piece in range(width // 256):
        cols = pl.ds(piece * 256, 256)
        picked = jnp.dot(select, pairs[slot, :, cols], preferred_element_type=jnp.float32)
        out_ref[:, cols] = picked.astype(jnp.bfloat16)


def gather_rows(pair_ids, counts, cols, table_rows, after):
    count = cols.shape[0]
    width = table_rows.shape[1]
    tiles = count // TILE
    anywhere = pl.BlockSpec(memory_space=pl.ANY)
    grid_spec = pltpu.PrefetchScalarGridSpec(
        num_scalar_prefetch=2,
        grid=(tiles,),
        in_specs=[pl.BlockSpec((TILE, 1), lambda i, *_: (i, 0)), anywhere] + [anywhere] * len(after),
        out_specs=pl.BlockSpec((TILE, width), lambda i, *_: (i, 0)),
        scratch_shapes=[pltpu.VMEM((3, 2 * TILE, width), jnp.bfloat16), pltpu.SemaphoreType.DMA((3,))],
    )
    return pl.pallas_call(
        functools.partial(gather_kernel, tiles, width),
        grid_spec=grid_spec,
        out_shape=jax.ShapeDtypeStruct((count, width), jnp.bfloat16),
        compiler_params=pltpu.CompilerParams(dimension_semantics=("arbitrary",)),
        cost_estimate=pl.CostEstimate(flops=count * 20_000_000, bytes_accessed=count * width * 6, transcendentals=0),
        name="gather_rows",
    )(pair_ids, counts, cols, table_rows, *after)


def heads_kernel(rows, resid_ref, gain_ref, cos_ref, sin_ref, wq_hbm, wk_hbm, wv_hbm, q_out, kv_out,
                 wq, wk, wv, normed, q_stage, kv_stage, w_sem, q_send, q_recv, kv_send, kv_recv,
                 own_recv, fwd_send, fwd_recv, keep_sem):
    group = lax.axis_index("dp")
    me = lax.axis_index("tp")
    core = lax.rem(me, 2)
    chip = me // 2
    partner = me + 1 - 2 * core
    tiles = rows // SEND_ROWS
    half = HEAD_DIM // 2

    loads = [pltpu.make_async_copy(src, dst, w_sem.at[n]) for n, (src, dst) in enumerate(((wk_hbm, wk), (wv_hbm, wv), (wq_hbm, wq)))]
    for load in loads:
        load.start()

    barrier = pltpu.get_barrier_semaphore()
    for step in range(1, 2 * CHIPS):
        pl.semaphore_signal(barrier, inc=1, device_id=(group, lax.rem(me + step, 2 * CHIPS)), device_id_type=MESH_IDS)

    @pl.loop(0, rows // 128)
    def _(part):
        span = pl.ds(pl.multiple_of(part * 128, 128), 128)
        widened = resid_ref[span, :].astype(jnp.float32)
        inv_rms = lax.rsqrt(jnp.mean(widened * widened, axis=-1, keepdims=True) + EPSILON)
        normed[span, :] = (widened * inv_rms * gain_ref[...]).astype(jnp.bfloat16)

    pl.semaphore_wait(barrier, 2 * CHIPS - 1)
    for load in loads:
        load.wait()

    def block(source, tile):
        return pl.ds(pl.multiple_of(source * rows + tile * SEND_ROWS, SEND_ROWS), SEND_ROWS)

    def whole(source):
        return pl.ds(pl.multiple_of(source * rows, rows), rows)

    def remote(src, dst, send, recv, device):
        return pltpu.make_async_remote_copy(src_ref=src, dst_ref=dst, send_sem=send, recv_sem=recv, device_id=(group, device), device_id_type=MESH_IDS)

    def rotated(linear, span, factor):
        front = linear[:, :half]
        back = linear[:, half:]
        cosines = cos_ref[span, :]
        sines = sin_ref[span, :]
        return jnp.concatenate([((front * cosines - back * sines) * factor).astype(jnp.bfloat16), ((back * cosines + front * sines) * factor).astype(jnp.bfloat16)], axis=-1)

    @pl.loop(0, CHIPS * tiles)
    def _(turn):
        offset = lax.rem(turn // tiles + 1, CHIPS)
        tile = lax.rem(turn, tiles)
        there = lax.rem(chip + offset, CHIPS)
        columns = pl.ds(pl.multiple_of(there * HEAD_DIM, HEAD_DIM), HEAD_DIM)
        sent = pl.ds(pl.multiple_of(tile * SEND_ROWS, SEND_ROWS), SEND_ROWS)

        @pl.loop(0, SEND_ROWS // 256)
        def _(part):
            span = pl.ds(pl.multiple_of(tile * SEND_ROWS + part * 256, 256), 256)
            lhs = normed[span, :]

            def linear(weight):
                return jnp.dot(lhs, weight, preferred_element_type=jnp.float32).astype(jnp.bfloat16)

            kv_stage[0, there, span, :] = rotated(linear(wk[:, columns]).astype(jnp.float32), span, 1.0)
            kv_stage[1, there, span, :] = linear(wv[:, columns])
            for side in range(2):
                q_stage[2 * there + side, span, :] = rotated(linear(wq[2 * there + side]).astype(jnp.float32), span, HEAD_DIM ** -0.5)

        @pl.when(offset != 0)
        def _():
            for side in range(2):
                remote(kv_stage.at[side, there, sent, :], kv_out.at[side, block(me, tile), :], kv_send.at[offset, side], kv_recv.at[offset, core, tile], 2 * there + side).start()
            for side in range(2):
                remote(q_stage.at[2 * there + side, sent, :], q_out.at[block(me, tile), :], q_send.at[offset, side], q_recv.at[offset, core], 2 * there + side).start()

    for side in range(2):
        remote(kv_stage.at[side, chip], kv_out.at[side, whole(me), :], kv_send.at[0, side], own_recv.at[side], partner).start()
    remote(q_stage.at[partner], q_out.at[whole(me), :], q_send.at[0, 0], q_recv.at[0, 0], partner).start()
    keeps = [pltpu.make_async_copy(q_stage.at[me], q_out.at[whole(me), :], keep_sem.at[0])]
    for side in range(2):
        keeps.append(pltpu.make_async_copy(kv_stage.at[side, chip], kv_out.at[side, whole(me), :], keep_sem.at[1 + side]))
    for keep in keeps:
        keep.start()

    for tile in range(tiles):
        for offset in range(1, CHIPS):
            for side in range(2):
                source = 2 * lax.rem(chip + CHIPS - offset, CHIPS) + side
                region = kv_out.at[core, block(source, tile), :]
                remote(region, region, kv_send.at[offset, side], kv_recv.at[offset, side, tile], partner).wait_recv()
                remote(region, region, fwd_send.at[offset, side], fwd_recv.at[offset, side], partner).start()

    for keep in keeps:
        keep.wait()
    for offset in range(1, CHIPS):
        there = lax.rem(chip + offset, CHIPS)
        for side in range(2):
            source = 2 * lax.rem(chip + CHIPS - offset, CHIPS) + side
            remote(kv_stage.at[side, there], kv_out.at[side, whole(me), :], kv_send.at[offset, side], own_recv.at[side], partner).wait_send()
            remote(q_stage.at[2 * there + side], q_out.at[whole(source), :], q_send.at[offset, side], q_recv.at[offset, side], partner).wait()
            mine = kv_out.at[core, whole(source), :]
            remote(mine, mine, fwd_send.at[offset, side], fwd_recv.at[offset, side], partner).wait_send()
            other = kv_out.at[1 - core, whole(source), :]
            remote(other, other, fwd_send.at[offset, side], fwd_recv.at[offset, side], partner).wait_recv()
    for side in range(2):
        remote(kv_stage.at[side, chip], kv_out.at[side, whole(partner), :], kv_send.at[0, side], own_recv.at[side], partner).wait()
    remote(q_stage.at[partner], q_out.at[whole(partner), :], q_send.at[0, 0], q_recv.at[0, 0], partner).wait()


def project_heads(residual, gain, cosines, sines, wq_all, w_key, w_value):
    rows, width = residual.shape
    heads = wq_all.shape[0]
    tokens = rows * heads
    tiles = rows // SEND_ROWS
    vmem = pl.BlockSpec(memory_space=pltpu.VMEM)
    anywhere = pl.BlockSpec(memory_space=pl.ANY)
    dma = pltpu.SemaphoreType.DMA
    return pl.pallas_call(
        functools.partial(heads_kernel, rows),
        out_shape=(jax.ShapeDtypeStruct((tokens, HEAD_DIM), jnp.bfloat16), jax.ShapeDtypeStruct((2, tokens, HEAD_DIM), jnp.bfloat16)),
        in_specs=[vmem, vmem, vmem, vmem, anywhere, anywhere, anywhere],
        out_specs=(anywhere, anywhere),
        scratch_shapes=[
            pltpu.VMEM(wq_all.shape, jnp.bfloat16),
            pltpu.VMEM(w_key.shape, jnp.bfloat16),
            pltpu.VMEM(w_value.shape, jnp.bfloat16),
            pltpu.VMEM((rows, width), jnp.bfloat16),
            pltpu.VMEM((heads, rows, HEAD_DIM), jnp.bfloat16),
            pltpu.VMEM((2, CHIPS, rows, HEAD_DIM), jnp.bfloat16),
            dma((3,)),
            dma((CHIPS, 2)), dma((CHIPS, 2)),
            dma((CHIPS, 2)), dma((CHIPS, 2, tiles)),
            dma((2,)),
            dma((CHIPS, 2)), dma((CHIPS, 2)),
            dma((3,)),
        ],
        compiler_params=pltpu.CompilerParams(collective_id=0, has_side_effects=True, vmem_limit_bytes=56 * 1024 * 1024),
        cost_estimate=pl.CostEstimate(flops=2 * rows * width * 4096, bytes_accessed=40_000_000, transcendentals=0),
        name="project_heads",
    )(residual, gain, cosines, sines, wq_all, w_key, w_value)


def solution(mesh):
    group_size = mesh.shape["tp"]

    def exchange(rows, bit):
        return lax.ppermute(rows, "tp", [(i, i ^ bit) for i in range(group_size)])

    def local_step(token_ids, positions, table_rows, norm_scale, w_query, w_key, w_value):
        dev_index = lax.axis_index("tp")
        vocab_rows, model_width = table_rows.shape
        wq_all = lax.all_gather(w_query, "tp", axis=0)
        local_ids = token_ids - dev_index * vocab_rows
        inside = (local_ids >= 0) & (local_ids < vocab_rows)
        local_ids = jnp.where(inside, local_ids, -1)
        tokens = token_ids.shape[0]
        block_rows = tokens // group_size
        chunk_rows = block_rows // CHUNKS
        half = chunk_rows // 2

        def arrange(values):
            view = values.reshape(2, 2, 2, CHUNKS, 2, half)
            for axis, bit in ((0, 4), (1, 2), (2, 1)):
                flag = (dev_index // bit) % 2 == 1
                view = jnp.where(flag, jnp.flip(view, axis), view)
            halves = view.transpose(3, 2, 4, 0, 1, 5)
            first = halves[:, :, 0].transpose(0, 1, 3, 2, 4)
            second = halves[:, :, 1]
            return jnp.stack([first, second], axis=2).reshape(CHUNKS, 2, 4 * chunk_rows)

        ids = arrange(local_ids)
        owned = ids >= 0
        pair_ids = jnp.where(owned, (ids // 2) * 2, -1)
        lane = (jnp.arange(4 * chunk_rows, dtype=jnp.int32) % TILE) * 2
        cols = jnp.where(owned, lane + ids % 2, -1)
        counts = jnp.sum(owned.astype(jnp.int32).reshape(CHUNKS, 2, 4 * chunk_rows // TILE, TILE), axis=-1)

        def gather(chunk, side, after):
            return gather_rows(pair_ids[chunk, side], counts[chunk, side], cols[chunk, side][:, None], table_rows, after)

        pieces = []
        after, late = [], []
        for chunk in range(CHUNKS):
            other = gather(chunk, 1, after)
            got = exchange(other, 1)
            mine = gather(chunk, 0, [other] + late)
            after, late = [], []
            for part, bits in ((0, (2, 4)), (1, (4, 2))):
                base = part * 4 * half
                keep = [slice(base + k * half, base + (k + 1) * half) for k in range(4)]
                far = slice(base + 2 * half, base + 4 * half)
                sent = mine[far] + got[far]
                back = exchange(sent, bits[0])
                near_send = mine[keep[1]] + got[keep[1]] + back[half:]
                back2 = exchange(near_send, bits[1])
                after.append(sent)
                late.append(near_send)
                pieces.append(mine[keep[0]] + got[keep[0]] + back[:half] + back2)
        residual = jnp.concatenate(pieces, axis=0)
        own = lax.dynamic_slice_in_dim(positions, dev_index * block_rows, block_rows)
        cosines, sines = rope_tables(own)
        queries, keys_values = project_heads(residual, (1.0 + norm_scale)[None, :], cosines, sines, wq_all, w_key, w_value)
        return residual, queries[:, None, :], keys_values[0][:, None, :], keys_values[1][:, None, :]

    head_spec = P("dp", "tp", None)
    return jax.shard_map(local_step, mesh=mesh, in_specs=(P("dp"), P("dp"), P("tp", None), P(), P(None, "tp"), P(), P()), out_specs=(P(("dp", "tp"), None), head_spec, head_spec, head_spec), check_vma=False)
```

```python
import functools
import math
import jax
import jax.numpy as jnp
from jax import lax
from jax.experimental import pallas as pl
from jax.experimental.pallas import tpu as pltpu
from jax.sharding import PartitionSpec as P

HEAD_DIM = 256
EPSILON = 1e-6
ROPE_BASE = 10000.0
TILE = 128
CHUNKS = 4
SEND_ROWS = 512
CHIPS = 4
MESH_IDS = pl.DeviceIdType.MESH


def rope_tables(positions):
    inv_freq = ROPE_BASE ** (-jnp.arange(0, HEAD_DIM, 2, dtype=jnp.float32) / HEAD_DIM)
    angles = positions.astype(jnp.float32)[:, None] * inv_freq[None, :]
    return jnp.cos(angles), jnp.sin(angles)


def gather_kernel(tiles, width, pair_ids, counts, cols_ref, table_ref, *rest):
    out_ref, pairs, sems = rest[-3:]
    step = pl.program_id(0)
    normalizer = jnp.asarray(math.sqrt(width), dtype=jnp.bfloat16)

    def start(tile, slot):
        @pl.loop(0, TILE, unroll=8)
        def _(row):
            src = pair_ids[tile * TILE + row]

            @pl.when(src >= 0)
            def _():
                pltpu.make_async_copy(table_ref.at[pl.ds(pl.multiple_of(src, 2), 2), :], pairs.at[slot, pl.ds(pl.multiple_of(2 * row, 2), 2), :], sems.at[slot]).start()

    def wait(tile, slot):
        count = counts[tile]
        size = TILE
        while size:
            @pl.when((count // size) % 2 == 1)
            def _():
                pltpu.make_async_copy(table_ref.at[pl.ds(0, 2 * size), :], pairs.at[slot, pl.ds(0, 2 * size), :], sems.at[slot]).wait()

            size //= 2

    @pl.when(step == 0)
    def _():
        pairs[...] = jnp.zeros_like(pairs)
        start(0, 0)
        start(1, 1)

    slot = lax.rem(step, 3)

    @pl.when(step + 2 < tiles)
    def _():
        start(step + 2, lax.rem(step + 2, 3))

    wait(step, slot)
    lanes = lax.broadcasted_iota(jnp.int32, (TILE, 2 * TILE), 1)
    select = jnp.where(lanes == cols_ref[...], normalizer, jnp.zeros((), jnp.bfloat16))
    for piece in range(width // 256):
        cols = pl.ds(piece * 256, 256)
        picked = jnp.dot(select, pairs[slot, :, cols], preferred_element_type=jnp.float32)
        out_ref[:, cols] = picked.astype(jnp.bfloat16)


def gather_rows(pair_ids, counts, cols, table_rows, after):
    count = cols.shape[0]
    width = table_rows.shape[1]
    tiles = count // TILE
    anywhere = pl.BlockSpec(memory_space=pl.ANY)
    grid_spec = pltpu.PrefetchScalarGridSpec(
        num_scalar_prefetch=2,
        grid=(tiles,),
        in_specs=[pl.BlockSpec((TILE, 1), lambda i, *_: (i, 0)), anywhere] + [anywhere] * len(after),
        out_specs=pl.BlockSpec((TILE, width), lambda i, *_: (i, 0)),
        scratch_shapes=[pltpu.VMEM((3, 2 * TILE, width), jnp.bfloat16), pltpu.SemaphoreType.DMA((3,))],
    )
    return pl.pallas_call(
        functools.partial(gather_kernel, tiles, width),
        grid_spec=grid_spec,
        out_shape=jax.ShapeDtypeStruct((count, width), jnp.bfloat16),
        compiler_params=pltpu.CompilerParams(dimension_semantics=("arbitrary",)),
        cost_estimate=pl.CostEstimate(flops=count * 20_000_000, bytes_accessed=count * width * 6, transcendentals=0),
        name="gather_rows",
    )(pair_ids, counts, cols, table_rows, *after)


def heads_kernel(rows, resid_ref, gain_ref, cos_ref, sin_ref, wq_hbm, wk_hbm, wv_hbm, q_out, kv_out,
                 wq, wk, wv, normed, q_stage, kv_stage, w_sem, q_send, q_recv, kv_send, kv_recv,
                 own_recv, fwd_send, fwd_recv, keep_sem):
    group = lax.axis_index("dp")
    me = lax.axis_index("tp")
    core = lax.rem(me, 2)
    chip = me // 2
    partner = me + 1 - 2 * core
    tiles = rows // SEND_ROWS
    half = HEAD_DIM // 2

    loads = [pltpu.make_async_copy(src, dst, w_sem.at[n]) for n, (src, dst) in enumerate(((wk_hbm, wk), (wv_hbm, wv), (wq_hbm, wq)))]
    for load in loads:
        load.start()

    barrier = pltpu.get_barrier_semaphore()
    for step in range(1, 2 * CHIPS):
        pl.semaphore_signal(barrier, inc=1, device_id=(group, lax.rem(me + step, 2 * CHIPS)), device_id_type=MESH_IDS)

    @pl.loop(0, rows // 128)
    def _(part):
        span = pl.ds(pl.multiple_of(part * 128, 128), 128)
        widened = resid_ref[span, :].astype(jnp.float32)
        inv_rms = lax.rsqrt(jnp.mean(widened * widened, axis=-1, keepdims=True) + EPSILON)
        normed[span, :] = (widened * inv_rms * gain_ref[...]).astype(jnp.bfloat16)

    pl.semaphore_wait(barrier, 2 * CHIPS - 1)
    for load in loads:
        load.wait()

    def block(source, tile):
        return pl.ds(pl.multiple_of(source * rows + tile * SEND_ROWS, SEND_ROWS), SEND_ROWS)

    def whole(source):
        return pl.ds(pl.multiple_of(source * rows, rows), rows)

    def remote(src, dst, send, recv, device):
        return pltpu.make_async_remote_copy(src_ref=src, dst_ref=dst, send_sem=send, recv_sem=recv, device_id=(group, device), device_id_type=MESH_IDS)

    def rotated(linear, span, factor):
        front = linear[:, :half]
        back = linear[:, half:]
        cosines = cos_ref[span, :]
        sines = sin_ref[span, :]
        return jnp.concatenate([((front * cosines - back * sines) * factor).astype(jnp.bfloat16), ((back * cosines + front * sines) * factor).astype(jnp.bfloat16)], axis=-1)

    @pl.loop(0, CHIPS * tiles)
    def _(turn):
        offset = lax.rem(turn // tiles + 1, CHIPS)
        tile = lax.rem(turn, tiles)
        there = lax.rem(chip + offset, CHIPS)
        columns = pl.ds(pl.multiple_of(there * HEAD_DIM, HEAD_DIM), HEAD_DIM)
        sent = pl.ds(pl.multiple_of(tile * SEND_ROWS, SEND_ROWS), SEND_ROWS)

        @pl.loop(0, SEND_ROWS // 256)
        def _(part):
            span = pl.ds(pl.multiple_of(tile * SEND_ROWS + part * 256, 256), 256)
            lhs = normed[span, :]

            def linear(weight):
                return jnp.dot(lhs, weight, preferred_element_type=jnp.float32).astype(jnp.bfloat16)

            kv_stage[0, there, span, :] = rotated(linear(wk[:, columns]).astype(jnp.float32), span, 1.0)
            kv_stage[1, there, span, :] = linear(wv[:, columns])
            for side in range(2):
                q_stage[2 * there + side, span, :] = rotated(linear(wq[2 * there + side]).astype(jnp.float32), span, HEAD_DIM ** -0.5)

        @pl.when(offset != 0)
        def _():
            for side in range(2):
                remote(kv_stage.at[side, there, sent, :], kv_out.at[side, block(me, tile), :], kv_send.at[offset, side], kv_recv.at[offset, core, tile], 2 * there + side).start()
            for side in range(2):
                remote(q_stage.at[2 * there + side, sent, :], q_out.at[block(me, tile), :], q_send.at[offset, side], q_recv.at[offset, core], 2 * there + side).start()

    for side in range(2):
        remote(kv_stage.at[side, chip], kv_out.at[side, whole(me), :], kv_send.at[0, side], own_recv.at[side], partner).start()
    remote(q_stage.at[partner], q_out.at[whole(me), :], q_send.at[0, 0], q_recv.at[0, 0], partner).start()
    keeps = [pltpu.make_async_copy(q_stage.at[me], q_out.at[whole(me), :], keep_sem.at[0])]
    for side in range(2):
        keeps.append(pltpu.make_async_copy(kv_stage.at[side, chip], kv_out.at[side, whole(me), :], keep_sem.at[1 + side]))
    for keep in keeps:
        keep.start()

    for tile in range(tiles):
        for offset in range(1, CHIPS):
            for side in range(2):
                source = 2 * lax.rem(chip + CHIPS - offset, CHIPS) + side
                region = kv_out.at[core, block(source, tile), :]
                remote(region, region, kv_send.at[offset, side], kv_recv.at[offset, side, tile], partner).wait_recv()
                remote(region, region, fwd_send.at[offset, side], fwd_recv.at[offset, side], partner).start()

    for keep in keeps:
        keep.wait()
    for offset in range(1, CHIPS):
        there = lax.rem(chip + offset, CHIPS)
        for side in range(2):
            source = 2 * lax.rem(chip + CHIPS - offset, CHIPS) + side
            remote(kv_stage.at[side, there], kv_out.at[side, whole(me), :], kv_send.at[offset, side], own_recv.at[side], partner).wait_send()
            remote(q_stage.at[2 * there + side], q_out.at[whole(source), :], q_send.at[offset, side], q_recv.at[offset, side], partner).wait()
            mine = kv_out.at[core, whole(source), :]
            remote(mine, mine, fwd_send.at[offset, side], fwd_recv.at[offset, side], partner).wait_send()
            other = kv_out.at[1 - core, whole(source), :]
            remote(other, other, fwd_send.at[offset, side], fwd_recv.at[offset, side], partner).wait_recv()
    for side in range(2):
        remote(kv_stage.at[side, chip], kv_out.at[side, whole(partner), :], kv_send.at[0, side], own_recv.at[side], partner).wait()
    remote(q_stage.at[partner], q_out.at[whole(partner), :], q_send.at[0, 0], q_recv.at[0, 0], partner).wait()


def project_heads(residual, gain, cosines, sines, wq_all, w_key, w_value):
    rows, width = residual.shape
    heads = wq_all.shape[0]
    tokens = rows * heads
    tiles = rows // SEND_ROWS
    vmem = pl.BlockSpec(memory_space=pltpu.VMEM)
    anywhere = pl.BlockSpec(memory_space=pl.ANY)
    dma = pltpu.SemaphoreType.DMA
    return pl.pallas_call(
        functools.partial(heads_kernel, rows),
        out_shape=(jax.ShapeDtypeStruct((tokens, HEAD_DIM), jnp.bfloat16), jax.ShapeDtypeStruct((2, tokens, HEAD_DIM), jnp.bfloat16)),
        in_specs=[vmem, vmem, vmem, vmem, anywhere, anywhere, anywhere],
        out_specs=(anywhere, anywhere),
        scratch_shapes=[
            pltpu.VMEM(wq_all.shape, jnp.bfloat16),
            pltpu.VMEM(w_key.shape, jnp.bfloat16),
            pltpu.VMEM(w_value.shape, jnp.bfloat16),
            pltpu.VMEM((rows, width), jnp.bfloat16),
            pltpu.VMEM((heads, rows, HEAD_DIM), jnp.bfloat16),
            pltpu.VMEM((2, CHIPS, rows, HEAD_DIM), jnp.bfloat16),
            dma((3,)),
            dma((CHIPS, 2)), dma((CHIPS, 2)),
            dma((CHIPS, 2)), dma((CHIPS, 2, tiles)),
            dma((2,)),
            dma((CHIPS, 2)), dma((CHIPS, 2)),
            dma((3,)),
        ],
        compiler_params=pltpu.CompilerParams(collective_id=0, has_side_effects=True, vmem_limit_bytes=56 * 1024 * 1024),
        cost_estimate=pl.CostEstimate(flops=2 * rows * width * 4096, bytes_accessed=40_000_000, transcendentals=0),
        name="project_heads",
    )(residual, gain, cosines, sines, wq_all, w_key, w_value)


def solution(mesh):
    group_size = mesh.shape["tp"]

    def exchange(rows, bit):
        return lax.ppermute(rows, "tp", [(i, i ^ bit) for i in range(group_size)])

    def local_body(token_ids, positions, table_rows, norm_scale, w_query, w_key, w_value):
        dev_index = lax.axis_index("tp")
        vocab_rows, _ = table_rows.shape
        wq_all = lax.all_gather(w_query, "tp", axis=0)
        local_ids = token_ids - dev_index * vocab_rows
        inside = (local_ids >= 0) & (local_ids < vocab_rows)
        local_ids = jnp.where(inside, local_ids, -1)
        tokens = token_ids.shape[0]
        block_rows = tokens // group_size
        chunk_rows = block_rows // CHUNKS
        half = chunk_rows // 2

        def arrange(values):
            view = values.reshape(2, 2, 2, CHUNKS, 2, half)
            for axis, bit in ((0, 4), (1, 2), (2, 1)):
                flag = (dev_index // bit) % 2 == 1
                view = jnp.where(flag, jnp.flip(view, axis), view)
            halves = view.transpose(3, 2, 4, 0, 1, 5)
            first = halves[:, :, 0].transpose(0, 1, 3, 2, 4)
            second = halves[:, :, 1]
            return jnp.stack([first, second], axis=2).reshape(CHUNKS, 2, 4 * chunk_rows)

        ids = arrange(local_ids)
        owned = ids >= 0
        pair_ids = jnp.where(owned, (ids // 2) * 2, -1)
        lane = (jnp.arange(4 * chunk_rows, dtype=jnp.int32) % TILE) * 2
        cols = jnp.where(owned, lane + ids % 2, -1)
        counts = jnp.sum(owned.astype(jnp.int32).reshape(CHUNKS, 2, 4 * chunk_rows // TILE, TILE), axis=-1)

        def gather(chunk, side, after):
            return gather_rows(pair_ids[chunk, side], counts[chunk, side], cols[chunk, side][:, None], table_rows, after)

        pieces = []
        after, late, late_next = [], [], []
        for chunk in range(CHUNKS):
            other = gather(chunk, 1, after + late + ([wq_all] if chunk == 2 else []))
            got = exchange(other, 1)
            mine = gather(chunk, 0, [other])
            after, late = [], late_next
            late_next = []
            for part, bits in ((0, (2, 4)), (1, (4, 2))):
                base = part * 4 * half
                keep = [slice(base + k * half, base + (k + 1) * half) for k in range(4)]
                far = slice(base + 2 * half, base + 4 * half)
                sent = mine[far] + got[far]
                back = exchange(sent, bits[0])
                near_send = mine[keep[1]] + got[keep[1]] + back[half:]
                back2 = exchange(near_send, bits[1])
                after.append(sent)
                late_next.append(near_send)
                pieces.append(mine[keep[0]] + got[keep[0]] + back[:half] + back2)
        residual = jnp.concatenate(pieces, axis=0)
        own = lax.dynamic_slice_in_dim(positions, dev_index * block_rows, block_rows)
        cosines, sines = rope_tables(own)
        queries, keys_values = project_heads(residual, (1.0 + norm_scale)[None, :], cosines, sines, wq_all, w_key, w_value)
        return residual, queries[:, None, :], keys_values[0][:, None, :], keys_values[1][:, None, :]

    head_spec = P("dp", "tp", None)
    return jax.shard_map(local_body, mesh=mesh, in_specs=(P("dp"), P("dp"), P("tp", None), P(), P(None, "tp"), P(), P()), out_specs=(P(("dp", "tp"), None), head_spec, head_spec, head_spec), check_vma=False)
```

```python
import functools
import math
import jax
import jax.numpy as jnp
from jax import lax
from jax.experimental import pallas as pl
from jax.experimental.pallas import tpu as pltpu
from jax.sharding import PartitionSpec as P

HEAD_DIM = 256
EPSILON = 1e-6
ROPE_BASE = 10000.0
TILE = 128
CHUNKS = 5
HEAD_ROWS = 640
TAIL_ROWS = 640
SEND_ROWS = 512
CHIPS = 4
MESH_IDS = pl.DeviceIdType.MESH


def rope_tables(positions):
    inv_freq = ROPE_BASE ** (-jnp.arange(0, HEAD_DIM, 2, dtype=jnp.float32) / HEAD_DIM)
    angles = positions.astype(jnp.float32)[:, None] * inv_freq[None, :]
    return jnp.cos(angles), jnp.sin(angles)


def gather_kernel(base, tiles, width, pair_ids, counts, cols_ref, table_ref, *rest):
    out_ref, pairs, sems = rest[-3:]
    step = pl.program_id(0)
    normalizer = jnp.asarray(math.sqrt(width), dtype=jnp.bfloat16)

    def start(tile, slot):
        @pl.loop(0, TILE // 8)
        def _(group):
            for row in range(8):
                src = pair_ids[(base + tile) * TILE + group * 8 + row]

                @pl.when(src >= 0)
                def _():
                    pltpu.make_async_copy(table_ref.at[pl.ds(pl.multiple_of(src, 2), 2), :], pairs.at[slot, group, pl.ds(2 * row, 2), :], sems.at[slot]).start()

    def wait(tile, slot):
        count = counts[base + tile]
        size = TILE // 8
        while size:
            @pl.when((count // (8 * size)) % 2 == 1)
            def _():
                pltpu.make_async_copy(pairs.at[slot, pl.ds(0, size)], pairs.at[slot, pl.ds(0, size)], sems.at[slot]).wait()

            size //= 2
        for size in (1, 2, 4):
            @pl.when((count // size) % 2 == 1)
            def _():
                pltpu.make_async_copy(table_ref.at[pl.ds(0, 2 * size), :], pairs.at[slot, 0, pl.ds(0, 2 * size), :], sems.at[slot]).wait()

    @pl.when(step == 0)
    def _():
        pairs[...] = jnp.zeros_like(pairs)
        start(0, 0)
        start(1, 1)

    slot = lax.rem(step, 3)

    @pl.when(step + 2 < tiles)
    def _():
        start(step + 2, lax.rem(step + 2, 3))

    wait(step, slot)
    lanes = lax.broadcasted_iota(jnp.int32, (TILE, 2 * TILE), 1).astype(jnp.float32)
    wanted = jnp.broadcast_to(cols_ref[0], (TILE, TILE)).T
    select = jnp.where(lanes == jnp.concatenate([wanted, wanted], axis=1), normalizer, jnp.zeros((), jnp.bfloat16))
    for piece in range(width // 256):
        cols = pl.ds(piece * 256, 256)
        picked = jnp.dot(select, pairs[slot, :, :, cols].reshape(2 * TILE, 256), preferred_element_type=jnp.float32)
        out_ref[:, cols] = picked.astype(jnp.bfloat16)


def gather_rows(base, count, pair_ids, counts, cols, table_rows, after):
    width = table_rows.shape[1]
    tiles = count // TILE
    base = base // TILE
    anywhere = pl.BlockSpec(memory_space=pl.ANY)
    grid_spec = pltpu.PrefetchScalarGridSpec(
        num_scalar_prefetch=2,
        grid=(tiles,),
        in_specs=[pl.BlockSpec((1, 1, TILE), lambda i, *_: (base + i, 0, 0)), anywhere] + [anywhere] * len(after),
        out_specs=pl.BlockSpec((TILE, width), lambda i, *_: (i, 0)),
        scratch_shapes=[pltpu.VMEM((3, TILE // 8, 16, width), jnp.bfloat16), pltpu.SemaphoreType.DMA((3,))],
    )
    return pl.pallas_call(
        functools.partial(gather_kernel, base, tiles, width),
        grid_spec=grid_spec,
        out_shape=jax.ShapeDtypeStruct((count, width), jnp.bfloat16),
        compiler_params=pltpu.CompilerParams(dimension_semantics=("arbitrary",)),
        cost_estimate=pl.CostEstimate(flops=count * 20_000_000, bytes_accessed=count * width * 6, transcendentals=0),
        name="gather_rows",
    )(pair_ids, counts, cols, table_rows, *after)


def finish_kernel(pieces, more, cols_ref, gain_ref, head_ref, extra_ref, *refs):
    tail_refs, (resid_ref, normed_ref, tail) = refs[:pieces], refs[pieces:]
    rows, width = resid_ref.shape
    part = TAIL_ROWS // (pieces // 2)
    extra_rows = extra_ref.shape[0]
    normalizer = jnp.asarray(math.sqrt(width), dtype=jnp.bfloat16)
    for index in range(pieces // 2):
        tail[pl.ds(index * part, part), :] = tail_refs[2 * index][...] + tail_refs[2 * index + 1][...]

    def one_hot(span, first, count, value):
        lanes = lax.broadcasted_iota(jnp.int32, (256, count), 1) + first
        return jnp.where(lanes == cols_ref[span, :], value, jnp.zeros((), jnp.bfloat16))

    @pl.loop(0, rows // 256)
    def _(block):
        span = pl.ds(pl.multiple_of(block * 256, 256), 256)
        from_head = one_hot(span, 0, HEAD_ROWS, normalizer)
        from_tail = one_hot(span, HEAD_ROWS, TAIL_ROWS, jnp.ones((), jnp.bfloat16))
        for piece in range(width // 256):
            cols = pl.ds(piece * 256, 256)
            picked = jnp.dot(from_head, head_ref[:, cols], preferred_element_type=jnp.float32)
            picked += jnp.dot(from_tail, tail[:, cols], preferred_element_type=jnp.float32)
            resid_ref[span, cols] = picked.astype(jnp.bfloat16)

        @pl.when(more[0] > 0)
        def _():
            from_extra = one_hot(span, HEAD_ROWS + TAIL_ROWS, extra_rows, jnp.ones((), jnp.bfloat16))
            for piece in range(width // 256):
                cols = pl.ds(piece * 256, 256)
                picked = jnp.dot(from_extra, extra_ref[:, cols], preferred_element_type=jnp.float32)
                resid_ref[span, cols] = (resid_ref[span, cols].astype(jnp.float32) + picked).astype(jnp.bfloat16)

        for quarter in range(4):
            rows_here = pl.ds(pl.multiple_of(block * 256 + quarter * 64, 64), 64)
            widened = resid_ref[rows_here, :].astype(jnp.float32)
            inv_rms = lax.rsqrt(jnp.mean(widened * widened, axis=-1, keepdims=True) + EPSILON)
            normed_ref[rows_here, :] = (widened * inv_rms * gain_ref[...]).astype(jnp.bfloat16)


def finish_rows(more, cols, gain, head, extra, tail_pieces):
    rows = cols.shape[0]
    width = head.shape[1]
    vmem = pl.BlockSpec(memory_space=pltpu.VMEM)
    shape = jax.ShapeDtypeStruct((rows, width), jnp.bfloat16)
    return pl.pallas_call(
        functools.partial(finish_kernel, len(tail_pieces)),
        out_shape=(shape, shape),
        in_specs=[pl.BlockSpec(memory_space=pltpu.SMEM)] + [vmem] * (4 + len(tail_pieces)),
        out_specs=(vmem, vmem),
        scratch_shapes=[pltpu.VMEM((TAIL_ROWS, width), jnp.bfloat16)],
        compiler_params=pltpu.CompilerParams(vmem_limit_bytes=40 * 1024 * 1024),
        cost_estimate=pl.CostEstimate(flops=2 * rows * width * (HEAD_ROWS + TAIL_ROWS), bytes_accessed=16_000_000, transcendentals=0),
        name="finish_rows",
    )(more, cols, gain, head, extra, *tail_pieces)


def heads_kernel(rows, normed, cos_ref, sin_ref, wq_hbm, wk_hbm, wv_hbm, q_out, kv_out,
                 wq, wk, wv, q_stage, kv_stage, w_sem, q_send, q_recv, kv_send, kv_recv,
                 own_recv, fwd_send, fwd_recv, keep_sem):
    group = lax.axis_index("dp")
    me = lax.axis_index("tp")
    core = lax.rem(me, 2)
    chip = me // 2
    partner = me + 1 - 2 * core
    tiles = rows // SEND_ROWS
    half = HEAD_DIM // 2

    loads = [pltpu.make_async_copy(src, dst, w_sem.at[n]) for n, (src, dst) in enumerate(((wk_hbm, wk), (wv_hbm, wv), (wq_hbm, wq)))]
    for load in loads:
        load.start()

    barrier = pltpu.get_barrier_semaphore()
    for step in range(1, 2 * CHIPS):
        pl.semaphore_signal(barrier, inc=1, device_id=(group, lax.rem(me + step, 2 * CHIPS)), device_id_type=MESH_IDS)

    pl.semaphore_wait(barrier, 2 * CHIPS - 1)
    for load in loads:
        load.wait()

    def block(source, tile):
        return pl.ds(pl.multiple_of(source * rows + tile * SEND_ROWS, SEND_ROWS), SEND_ROWS)

    def whole(source):
        return pl.ds(pl.multiple_of(source * rows, rows), rows)

    def remote(src, dst, send, recv, device):
        return pltpu.make_async_remote_copy(src_ref=src, dst_ref=dst, send_sem=send, recv_sem=recv, device_id=(group, device), device_id_type=MESH_IDS)

    def rotated(linear, span, factor):
        front = linear[:, :half]
        back = linear[:, half:]
        cosines = cos_ref[span, :]
        sines = sin_ref[span, :]
        return jnp.concatenate([((front * cosines - back * sines) * factor).astype(jnp.bfloat16), ((back * cosines + front * sines) * factor).astype(jnp.bfloat16)], axis=-1)

    @pl.loop(0, CHIPS * tiles)
    def _(turn):
        offset = lax.rem(turn // tiles + 1, CHIPS)
        tile = lax.rem(turn, tiles)
        there = lax.rem(chip + offset, CHIPS)
        columns = pl.ds(pl.multiple_of(there * HEAD_DIM, HEAD_DIM), HEAD_DIM)
        sent = pl.ds(pl.multiple_of(tile * SEND_ROWS, SEND_ROWS), SEND_ROWS)

        @pl.loop(0, SEND_ROWS // 256)
        def _(part):
            span = pl.ds(pl.multiple_of(tile * SEND_ROWS + part * 256, 256), 256)
            lhs = normed[span, :]

            def linear(weight):
                return jnp.dot(lhs, weight, preferred_element_type=jnp.float32).astype(jnp.bfloat16)

            kv_stage[0, there, span, :] = rotated(linear(wk[:, columns]).astype(jnp.float32), span, 1.0)
            kv_stage[1, there, span, :] = linear(wv[:, columns])
            for side in range(2):
                q_stage[2 * there + side, span, :] = rotated(linear(wq[2 * there + side]).astype(jnp.float32), span, HEAD_DIM ** -0.5)

        @pl.when(offset != 0)
        def _():
            for side in range(2):
                remote(kv_stage.at[side, there, sent, :], kv_out.at[side, block(me, tile), :], kv_send.at[offset, side], kv_recv.at[offset, core, tile], 2 * there + side).start()
            for side in range(2):
                remote(q_stage.at[2 * there + side, sent, :], q_out.at[block(me, tile), :], q_send.at[offset, side], q_recv.at[offset, core], 2 * there + side).start()

    for side in range(2):
        remote(kv_stage.at[side, chip], kv_out.at[side, whole(me), :], kv_send.at[0, side], own_recv.at[side], partner).start()
    remote(q_stage.at[partner], q_out.at[whole(me), :], q_send.at[0, 0], q_recv.at[0, 0], partner).start()
    keeps = [pltpu.make_async_copy(q_stage.at[me], q_out.at[whole(me), :], keep_sem.at[0])]
    for side in range(2):
        keeps.append(pltpu.make_async_copy(kv_stage.at[side, chip], kv_out.at[side, whole(me), :], keep_sem.at[1 + side]))
    for keep in keeps:
        keep.start()

    for tile in range(tiles):
        for offset in range(1, CHIPS):
            for side in range(2):
                source = 2 * lax.rem(chip + CHIPS - offset, CHIPS) + side
                region = kv_out.at[core, block(source, tile), :]
                remote(region, region, kv_send.at[offset, side], kv_recv.at[offset, side, tile], partner).wait_recv()
                remote(region, region, fwd_send.at[offset, side], fwd_recv.at[offset, side], partner).start()

    for keep in keeps:
        keep.wait()
    for offset in range(1, CHIPS):
        there = lax.rem(chip + offset, CHIPS)
        for side in range(2):
            source = 2 * lax.rem(chip + CHIPS - offset, CHIPS) + side
            remote(kv_stage.at[side, there], kv_out.at[side, whole(me), :], kv_send.at[offset, side], own_recv.at[side], partner).wait_send()
            remote(q_stage.at[2 * there + side], q_out.at[whole(source), :], q_send.at[offset, side], q_recv.at[offset, side], partner).wait()
            mine = kv_out.at[core, whole(source), :]
            remote(mine, mine, fwd_send.at[offset, side], fwd_recv.at[offset, side], partner).wait_send()
            other = kv_out.at[1 - core, whole(source), :]
            remote(other, other, fwd_send.at[offset, side], fwd_recv.at[offset, side], partner).wait_recv()
    for side in range(2):
        remote(kv_stage.at[side, chip], kv_out.at[side, whole(partner), :], kv_send.at[0, side], own_recv.at[side], partner).wait()
    remote(q_stage.at[partner], q_out.at[whole(partner), :], q_send.at[0, 0], q_recv.at[0, 0], partner).wait()


def project_heads(normed, cosines, sines, wq_all, w_key, w_value):
    rows, width = normed.shape
    heads = wq_all.shape[0]
    tokens = rows * heads
    tiles = rows // SEND_ROWS
    vmem = pl.BlockSpec(memory_space=pltpu.VMEM)
    anywhere = pl.BlockSpec(memory_space=pl.ANY)
    dma = pltpu.SemaphoreType.DMA
    return pl.pallas_call(
        functools.partial(heads_kernel, rows),
        out_shape=(jax.ShapeDtypeStruct((tokens, HEAD_DIM), jnp.bfloat16), jax.ShapeDtypeStruct((2, tokens, HEAD_DIM), jnp.bfloat16)),
        in_specs=[vmem, vmem, vmem, anywhere, anywhere, anywhere],
        out_specs=(anywhere, anywhere),
        scratch_shapes=[
            pltpu.VMEM(wq_all.shape, jnp.bfloat16),
            pltpu.VMEM(w_key.shape, jnp.bfloat16),
            pltpu.VMEM(w_value.shape, jnp.bfloat16),
            pltpu.VMEM((heads, rows, HEAD_DIM), jnp.bfloat16),
            pltpu.VMEM((2, CHIPS, rows, HEAD_DIM), jnp.bfloat16),
            dma((3,)),
            dma((CHIPS, 2)), dma((CHIPS, 2)),
            dma((CHIPS, 2)), dma((CHIPS, 2, tiles)),
            dma((2,)),
            dma((CHIPS, 2)), dma((CHIPS, 2)),
            dma((3,)),
        ],
        compiler_params=pltpu.CompilerParams(collective_id=0, has_side_effects=True, vmem_limit_bytes=56 * 1024 * 1024),
        cost_estimate=pl.CostEstimate(flops=2 * rows * width * 4096, bytes_accessed=40_000_000, transcendentals=0),
        name="project_heads",
    )(normed, cosines, sines, wq_all, w_key, w_value)


def solution(mesh):
    group_size = mesh.shape["tp"]

    def exchange(rows, bit):
        return lax.ppermute(rows, "tp", [(i, i ^ bit) for i in range(group_size)])

    def share_head(rows, dev_index):
        half = rows.shape[0] // 2
        first, second = rows[:half], rows[half:]
        first_x = lax.ppermute(first, "tp", [(0, 2)])
        second_y = lax.ppermute(second, "tp", [(0, 4)])
        first = jnp.where(dev_index == 2, first_x, first)
        second = jnp.where(dev_index == 4, second_y, second)
        first_y = lax.ppermute(first, "tp", [(0, 4), (2, 6)])
        second_x = lax.ppermute(second, "tp", [(0, 2), (4, 6)])
        first = jnp.where(dev_index >= 4, first_y, first)
        second = jnp.where(dev_index % 4 >= 2, second_x, second)
        both = jnp.concatenate([first, second], axis=0)
        other = lax.ppermute(both, "tp", [(0, 1), (2, 3), (4, 5), (6, 7)])
        return jnp.where(dev_index % 2 == 1, other, both)

    def local_body(token_ids, positions, table_rows, norm_scale, w_query, w_key, w_value):
        dev_index = lax.axis_index("tp")
        vocab_rows, model_width = table_rows.shape
        wq_all = lax.all_gather(w_query, "tp", axis=0)
        head = share_head(table_rows[:HEAD_ROWS], dev_index)
        tokens = token_ids.shape[0]
        block_rows = tokens // group_size
        extra_rows = block_rows - TAIL_ROWS
        chunk_rows = TAIL_ROWS // CHUNKS
        half = chunk_rows // 2

        blocks = token_ids.reshape(group_size, block_rows)
        in_tail = blocks >= HEAD_ROWS
        earlier = (lax.broadcasted_iota(jnp.int32, (block_rows, block_rows), 0) < lax.broadcasted_iota(jnp.int32, (block_rows, block_rows), 1)).astype(jnp.bfloat16)
        ranks = jnp.dot(in_tail.astype(jnp.bfloat16), earlier, preferred_element_type=jnp.float32).astype(jnp.int32)
        ranks = jnp.where(in_tail, ranks, -1)

        def ranked_ids(first, count):
            wanted = lax.broadcasted_iota(jnp.int32, (group_size, block_rows, count), 2) + first
            ids = jnp.sum(jnp.where(ranks[:, :, None] == wanted, blocks[:, :, None] + 1, 0), axis=1) - 1
            local = ids - dev_index * vocab_rows
            return jnp.where((ids >= 0) & (local >= 0) & (local < vocab_rows), local, -1)

        most = jnp.max(jnp.sum(in_tail.astype(jnp.int32), axis=1))
        over = (most > TAIL_ROWS).astype(jnp.int32)

        def arrange(values):
            view = values.reshape(2, 2, 2, CHUNKS, 2, half)
            for axis, bit in ((0, 4), (1, 2), (2, 1)):
                flag = (dev_index // bit) % 2 == 1
                view = jnp.where(flag, jnp.flip(view, axis), view)
            halves = view.transpose(3, 2, 4, 0, 1, 5)
            first = halves[:, :, 0].transpose(0, 1, 3, 2, 4)
            second = halves[:, :, 1]
            return jnp.stack([first, second], axis=2).reshape(CHUNKS, 2, 4 * chunk_rows)

        call_rows = 4 * chunk_rows
        ids = arrange(ranked_ids(0, TAIL_ROWS)).reshape(-1, TILE)
        owned = ids >= 0
        pair_ids = jnp.where(owned, (ids // 2) * 2, -1).reshape(-1)
        lane = jnp.arange(TILE, dtype=jnp.int32) * 2
        cols = jnp.where(owned, lane + ids % 2, -1).astype(jnp.float32)[:, None, :]
        counts = jnp.sum(owned.astype(jnp.int32), axis=-1)

        def gather(chunk, side, after):
            return gather_rows((2 * chunk + side) * call_rows, call_rows, pair_ids, counts, cols, table_rows, after)

        pieces, sums = [], []
        after, late, late_next = [], [], []
        for chunk in range(CHUNKS):
            other = gather(chunk, 1, after + late + ([wq_all] if chunk == 2 else []))
            got = exchange(other, 1)
            mine = gather(chunk, 0, [other])
            after, late = [], late_next
            late_next = []
            for part, bits in ((0, (2, 4)), (1, (4, 2))):
                base = part * 4 * half
                keep = [slice(base + k * half, base + (k + 1) * half) for k in range(4)]
                far = slice(base + 2 * half, base + 4 * half)
                sent = mine[far] + got[far]
                back = exchange(sent, bits[0])
                near_send = mine[keep[1]] + got[keep[1]] + back[half:]
                back2 = exchange(near_send, bits[1])
                after.append(sent)
                sums.append(sent)
                late_next.append(near_send)
                pieces += [mine[keep[0]] + got[keep[0]] + back[:half], back2]

        def second_exchange(rows):
            ids = ranked_ids(TAIL_ROWS, extra_rows).reshape(-1)
            normalizer = jnp.asarray(math.sqrt(model_width), dtype=jnp.bfloat16)
            picked = jnp.take(rows, jnp.maximum(ids, 0), axis=0, mode="clip") * normalizer
            partial = jnp.where(ids[:, None] >= 0, picked, jnp.zeros((), jnp.bfloat16))
            return lax.psum_scatter(partial, "tp", scatter_dimension=0, tiled=True)

        def no_exchange(rows):
            return jnp.zeros((extra_rows, model_width), jnp.bfloat16)

        over, _ = lax.optimization_barrier((over, sums[2]))
        more = lax.pmax(over, "dp")
        asked, _ = lax.optimization_barrier((more, pieces[-5]))
        extra = lax.cond(asked > 0, second_exchange, no_exchange, table_rows)
        places = jnp.where(in_tail, HEAD_ROWS + ranks, blocks)
        own_places = lax.dynamic_index_in_dim(places, dev_index, 0, keepdims=False)
        residual, normed = finish_rows(more.reshape(1), own_places[:, None], (1.0 + norm_scale)[None, :], head, extra, pieces)
        own = lax.dynamic_slice_in_dim(positions, dev_index * block_rows, block_rows)
        cosines, sines = rope_tables(own)
        queries, keys_values = project_heads(normed, cosines, sines, wq_all, w_key, w_value)
        return residual, queries[:, None, :], keys_values[0][:, None, :], keys_values[1][:, None, :]

    head_spec = P("dp", "tp", None)
    return jax.shard_map(local_body, mesh=mesh, in_specs=(P("dp"), P("dp"), P("tp", None), P(), P(None, "tp"), P(), P()), out_specs=(P(("dp", "tp"), None), head_spec, head_spec, head_spec), check_vma=False)
```

```python
import functools
import math
import jax
import jax.numpy as jnp
from jax import lax
from jax.experimental import pallas as pl
from jax.experimental.pallas import tpu as pltpu
from jax.sharding import PartitionSpec as P

HEAD_DIM = 256
EPSILON = 1e-6
ROPE_BASE = 10000.0
TILE = 128
CHUNKS = 5
HEAD_ROWS = 640
TAIL_ROWS = 640
SEND_ROWS = 512
CHIPS = 4
MESH_IDS = pl.DeviceIdType.MESH


def rope_tables(positions):
    inv_freq = ROPE_BASE ** (-jnp.arange(0, HEAD_DIM, 2, dtype=jnp.float32) / HEAD_DIM)
    angles = positions.astype(jnp.float32)[:, None] * inv_freq[None, :]
    return jnp.cos(angles), jnp.sin(angles)


def gather_kernel(base, tiles, width, pair_ids, counts, cols_ref, table_ref, *rest):
    out_ref, pairs, sems = rest[-3:]
    step = pl.program_id(0)
    normalizer = jnp.asarray(math.sqrt(width), dtype=jnp.bfloat16)

    def start(tile, slot):
        count = counts[base + tile]

        def copy(group, row):
            src = pair_ids[(base + tile) * TILE + group * 8 + row]
            pltpu.make_async_copy(table_ref.at[pl.ds(pl.multiple_of(src, 2), 2), :], pairs.at[slot, group, pl.ds(2 * row, 2), :], sems.at[slot]).start()

        @pl.loop(0, count // 8)
        def _(group):
            for row in range(8):
                copy(group, row)

        for row in range(7):
            @pl.when(row < lax.rem(count, 8))
            def _():
                copy(count // 8, row)

    def wait(tile, slot):
        count = counts[base + tile]
        size = TILE // 8
        while size:
            @pl.when((count // (8 * size)) % 2 == 1)
            def _():
                pltpu.make_async_copy(pairs.at[slot, pl.ds(0, size)], pairs.at[slot, pl.ds(0, size)], sems.at[slot]).wait()

            size //= 2
        for size in (1, 2, 4):
            @pl.when((count // size) % 2 == 1)
            def _():
                pltpu.make_async_copy(table_ref.at[pl.ds(0, 2 * size), :], pairs.at[slot, 0, pl.ds(0, 2 * size), :], sems.at[slot]).wait()

    @pl.when(step == 0)
    def _():
        pairs[...] = jnp.zeros_like(pairs)
        start(0, 0)
        start(1, 1)

    slot = lax.rem(step, 3)

    @pl.when(step + 2 < tiles)
    def _():
        start(step + 2, lax.rem(step + 2, 3))

    wait(step, slot)
    lanes = lax.broadcasted_iota(jnp.int32, (TILE, 2 * TILE), 1).astype(jnp.float32)
    wanted = jnp.broadcast_to(cols_ref[0], (TILE, TILE)).T
    select = jnp.where(lanes == jnp.concatenate([wanted, wanted], axis=1), normalizer, jnp.zeros((), jnp.bfloat16))
    for piece in range(width // 256):
        cols = pl.ds(piece * 256, 256)
        picked = jnp.dot(select, pairs[slot, :, :, cols].reshape(2 * TILE, 256), preferred_element_type=jnp.float32)
        out_ref[:, cols] = picked.astype(jnp.bfloat16)


def gather_rows(base, count, pair_ids, counts, cols, table_rows, after):
    width = table_rows.shape[1]
    tiles = count // TILE
    base = base // TILE
    anywhere = pl.BlockSpec(memory_space=pl.ANY)
    grid_spec = pltpu.PrefetchScalarGridSpec(
        num_scalar_prefetch=2,
        grid=(tiles,),
        in_specs=[pl.BlockSpec((1, 1, TILE), lambda i, *_: (base + i, 0, 0)), anywhere] + [anywhere] * len(after),
        out_specs=pl.BlockSpec((TILE, width), lambda i, *_: (i, 0)),
        scratch_shapes=[pltpu.VMEM((3, TILE // 8, 16, width), jnp.bfloat16), pltpu.SemaphoreType.DMA((3,))],
    )
    return pl.pallas_call(
        functools.partial(gather_kernel, base, tiles, width),
        grid_spec=grid_spec,
        out_shape=jax.ShapeDtypeStruct((count, width), jnp.bfloat16),
        compiler_params=pltpu.CompilerParams(dimension_semantics=("arbitrary",)),
        cost_estimate=pl.CostEstimate(flops=count * 20_000_000, bytes_accessed=count * width * 6, transcendentals=0),
        name="gather_rows",
    )(pair_ids, counts, cols, table_rows, *after)


def finish_kernel(pieces, more, cols_ref, gain_ref, head_hbm, extra_hbm, *refs):
    piece_refs, (resid_hbm, normed_hbm, source, parts, extra, resid, normed, in_sems, out_sems) = refs[:pieces], refs[pieces:]
    rows, width = resid.shape
    part = TAIL_ROWS // (pieces // 2)
    known = HEAD_ROWS + TAIL_ROWS
    normalizer = jnp.asarray(math.sqrt(width), dtype=jnp.bfloat16)
    one = jnp.ones((), jnp.bfloat16)
    zero = jnp.zeros((), jnp.bfloat16)
    head_copy = pltpu.make_async_copy(head_hbm, source.at[pl.ds(0, HEAD_ROWS), :], in_sems.at[pieces])
    extra_copy = pltpu.make_async_copy(extra_hbm, extra, in_sems.at[pieces + 1])
    copies = []
    for index, ref in enumerate(piece_refs):
        there = source.at[pl.ds(HEAD_ROWS + index // 2 * part, part), :] if index % 2 == 0 else parts.at[index // 2]
        copies.append(pltpu.make_async_copy(ref, there, in_sems.at[index]))
    for copy in copies:
        copy.start()
    head_copy.start()
    extra_copy.start()
    for index in range(pieces // 2):
        copies[2 * index].wait()
        copies[2 * index + 1].wait()
        span = pl.ds(HEAD_ROWS + index * part, part)
        source[span, :] = source[span, :] + parts[index]
    head_copy.wait()
    extra_copy.wait()

    def results(block):
        span = pl.ds(pl.multiple_of(block * 256, 256), 256)
        return (pltpu.make_async_copy(resid.at[span, :], resid_hbm.at[span, :], out_sems.at[0]),
                pltpu.make_async_copy(normed.at[span, :], normed_hbm.at[span, :], out_sems.at[1]))

    @pl.loop(0, rows // 256)
    def _(block):
        span = pl.ds(pl.multiple_of(block * 256, 256), 256)
        lanes = lax.broadcasted_iota(jnp.int32, (256, known), 1)
        value = jnp.where(lax.broadcasted_iota(jnp.int32, (1, known), 1) < HEAD_ROWS, normalizer, one)
        select = jnp.where(lanes == cols_ref[span, :], jnp.broadcast_to(value, (256, known)), zero)
        for piece in range(width // 256):
            cols = pl.ds(piece * 256, 256)
            resid[span, cols] = jnp.dot(select, source[:, cols], preferred_element_type=jnp.float32).astype(jnp.bfloat16)

        @pl.when(more[0] > 0)
        def _():
            places = lax.broadcasted_iota(jnp.int32, (256, extra.shape[0]), 1) + known
            from_extra = jnp.where(places == cols_ref[span, :], one, zero)
            for piece in range(width // 256):
                cols = pl.ds(piece * 256, 256)
                picked = jnp.dot(from_extra, extra[:, cols], preferred_element_type=jnp.float32)
                resid[span, cols] = (resid[span, cols].astype(jnp.float32) + picked).astype(jnp.bfloat16)

        for quarter in range(4):
            rows_here = pl.ds(pl.multiple_of(block * 256 + quarter * 64, 64), 64)
            widened = resid[rows_here, :].astype(jnp.float32)
            inv_rms = lax.rsqrt(jnp.mean(widened * widened, axis=-1, keepdims=True) + EPSILON)
            normed[rows_here, :] = (widened * inv_rms * gain_ref[...]).astype(jnp.bfloat16)
        for result in results(block):
            result.start()

    @pl.loop(0, rows // 256)
    def _(block):
        for result in results(block):
            result.wait()


def finish_rows(more, cols, gain, head, extra, pieces):
    rows = cols.shape[0]
    width = head.shape[1]
    vmem = pl.BlockSpec(memory_space=pltpu.VMEM)
    hbm = pl.BlockSpec(memory_space=pltpu.HBM)
    shape = jax.ShapeDtypeStruct((rows, width), jnp.bfloat16)
    dma = pltpu.SemaphoreType.DMA
    return pl.pallas_call(
        functools.partial(finish_kernel, len(pieces)),
        out_shape=(shape, shape),
        in_specs=[pl.BlockSpec(memory_space=pltpu.SMEM), vmem, vmem, hbm, hbm] + [hbm] * len(pieces),
        out_specs=(hbm, hbm),
        scratch_shapes=[
            pltpu.VMEM((HEAD_ROWS + TAIL_ROWS, width), jnp.bfloat16),
            pltpu.VMEM((len(pieces) // 2,) + pieces[0].shape, jnp.bfloat16),
            pltpu.VMEM(extra.shape, jnp.bfloat16),
            pltpu.VMEM((rows, width), jnp.bfloat16),
            pltpu.VMEM((rows, width), jnp.bfloat16),
            dma((len(pieces) + 2,)), dma((2,)),
        ],
        compiler_params=pltpu.CompilerParams(vmem_limit_bytes=40 * 1024 * 1024),
        cost_estimate=pl.CostEstimate(flops=2 * rows * width * (HEAD_ROWS + TAIL_ROWS), bytes_accessed=16_000_000, transcendentals=0),
        name="finish_rows",
    )(more, cols, gain, head, extra, *pieces)


def heads_kernel(rows, normed, cos_ref, sin_ref, wq_hbm, wk_hbm, wv_hbm, q_out, kv_out,
                 wq, wk, wv, q_stage, kv_stage, w_sem, q_send, q_recv, kv_send, kv_recv,
                 own_recv, fwd_send, fwd_recv, keep_sem):
    group = lax.axis_index("dp")
    me = lax.axis_index("tp")
    core = lax.rem(me, 2)
    chip = me // 2
    partner = me + 1 - 2 * core
    tiles = rows // SEND_ROWS
    half = HEAD_DIM // 2

    loads = [pltpu.make_async_copy(src, dst, w_sem.at[n]) for n, (src, dst) in enumerate(((wk_hbm, wk), (wv_hbm, wv), (wq_hbm, wq)))]
    for load in loads:
        load.start()

    barrier = pltpu.get_barrier_semaphore()
    for step in range(1, 2 * CHIPS):
        pl.semaphore_signal(barrier, inc=1, device_id=(group, lax.rem(me + step, 2 * CHIPS)), device_id_type=MESH_IDS)

    pl.semaphore_wait(barrier, 2 * CHIPS - 1)
    for load in loads:
        load.wait()

    def block(source, tile):
        return pl.ds(pl.multiple_of(source * rows + tile * SEND_ROWS, SEND_ROWS), SEND_ROWS)

    def whole(source):
        return pl.ds(pl.multiple_of(source * rows, rows), rows)

    def remote(src, dst, send, recv, device):
        return pltpu.make_async_remote_copy(src_ref=src, dst_ref=dst, send_sem=send, recv_sem=recv, device_id=(group, device), device_id_type=MESH_IDS)

    def rotated(linear, span, factor):
        front = linear[:, :half]
        back = linear[:, half:]
        cosines = cos_ref[span, :]
        sines = sin_ref[span, :]
        return jnp.concatenate([((front * cosines - back * sines) * factor).astype(jnp.bfloat16), ((back * cosines + front * sines) * factor).astype(jnp.bfloat16)], axis=-1)

    @pl.loop(0, CHIPS * tiles)
    def _(turn):
        offset = lax.rem(turn // tiles + 1, CHIPS)
        tile = lax.rem(turn, tiles)
        there = lax.rem(chip + offset, CHIPS)
        columns = pl.ds(pl.multiple_of(there * HEAD_DIM, HEAD_DIM), HEAD_DIM)
        sent = pl.ds(pl.multiple_of(tile * SEND_ROWS, SEND_ROWS), SEND_ROWS)

        @pl.loop(0, SEND_ROWS // 256)
        def _(part):
            span = pl.ds(pl.multiple_of(tile * SEND_ROWS + part * 256, 256), 256)
            lhs = normed[span, :]

            def linear(weight):
                return jnp.dot(lhs, weight, preferred_element_type=jnp.float32).astype(jnp.bfloat16)

            kv_stage[0, there, span, :] = rotated(linear(wk[:, columns]).astype(jnp.float32), span, 1.0)
            kv_stage[1, there, span, :] = linear(wv[:, columns])
            for side in range(2):
                q_stage[2 * there + side, span, :] = rotated(linear(wq[2 * there + side]).astype(jnp.float32), span, HEAD_DIM ** -0.5)

        @pl.when(offset != 0)
        def _():
            for side in range(2):
                remote(kv_stage.at[side, there, sent, :], kv_out.at[side, block(me, tile), :], kv_send.at[offset, side], kv_recv.at[offset, core, tile], 2 * there + side).start()
            for side in range(2):
                remote(q_stage.at[2 * there + side, sent, :], q_out.at[block(me, tile), :], q_send.at[offset, side], q_recv.at[offset, core], 2 * there + side).start()

    for side in range(2):
        remote(kv_stage.at[side, chip], kv_out.at[side, whole(me), :], kv_send.at[0, side], own_recv.at[side], partner).start()
    remote(q_stage.at[partner], q_out.at[whole(me), :], q_send.at[0, 0], q_recv.at[0, 0], partner).start()
    keeps = [pltpu.make_async_copy(q_stage.at[me], q_out.at[whole(me), :], keep_sem.at[0])]
    for side in range(2):
        keeps.append(pltpu.make_async_copy(kv_stage.at[side, chip], kv_out.at[side, whole(me), :], keep_sem.at[1 + side]))
    for keep in keeps:
        keep.start()

    for tile in range(tiles):
        for offset in range(1, CHIPS):
            for side in range(2):
                source = 2 * lax.rem(chip + CHIPS - offset, CHIPS) + side
                region = kv_out.at[core, block(source, tile), :]
                remote(region, region, kv_send.at[offset, side], kv_recv.at[offset, side, tile], partner).wait_recv()
                remote(region, region, fwd_send.at[offset, side], fwd_recv.at[offset, side], partner).start()

    for keep in keeps:
        keep.wait()
    for offset in range(1, CHIPS):
        there = lax.rem(chip + offset, CHIPS)
        for side in range(2):
            source = 2 * lax.rem(chip + CHIPS - offset, CHIPS) + side
            remote(kv_stage.at[side, there], kv_out.at[side, whole(me), :], kv_send.at[offset, side], own_recv.at[side], partner).wait_send()
            remote(q_stage.at[2 * there + side], q_out.at[whole(source), :], q_send.at[offset, side], q_recv.at[offset, side], partner).wait()
            mine = kv_out.at[core, whole(source), :]
            remote(mine, mine, fwd_send.at[offset, side], fwd_recv.at[offset, side], partner).wait_send()
            other = kv_out.at[1 - core, whole(source), :]
            remote(other, other, fwd_send.at[offset, side], fwd_recv.at[offset, side], partner).wait_recv()
    for side in range(2):
        remote(kv_stage.at[side, chip], kv_out.at[side, whole(partner), :], kv_send.at[0, side], own_recv.at[side], partner).wait()
    remote(q_stage.at[partner], q_out.at[whole(partner), :], q_send.at[0, 0], q_recv.at[0, 0], partner).wait()


def project_heads(normed, cosines, sines, wq_all, w_key, w_value):
    rows, width = normed.shape
    heads = wq_all.shape[0]
    tokens = rows * heads
    tiles = rows // SEND_ROWS
    vmem = pl.BlockSpec(memory_space=pltpu.VMEM)
    anywhere = pl.BlockSpec(memory_space=pl.ANY)
    dma = pltpu.SemaphoreType.DMA
    return pl.pallas_call(
        functools.partial(heads_kernel, rows),
        out_shape=(jax.ShapeDtypeStruct((tokens, HEAD_DIM), jnp.bfloat16), jax.ShapeDtypeStruct((2, tokens, HEAD_DIM), jnp.bfloat16)),
        in_specs=[vmem, vmem, vmem, anywhere, anywhere, anywhere],
        out_specs=(anywhere, anywhere),
        scratch_shapes=[
            pltpu.VMEM(wq_all.shape, jnp.bfloat16),
            pltpu.VMEM(w_key.shape, jnp.bfloat16),
            pltpu.VMEM(w_value.shape, jnp.bfloat16),
            pltpu.VMEM((heads, rows, HEAD_DIM), jnp.bfloat16),
            pltpu.VMEM((2, CHIPS, rows, HEAD_DIM), jnp.bfloat16),
            dma((3,)),
            dma((CHIPS, 2)), dma((CHIPS, 2)),
            dma((CHIPS, 2)), dma((CHIPS, 2, tiles)),
            dma((2,)),
            dma((CHIPS, 2)), dma((CHIPS, 2)),
            dma((3,)),
        ],
        compiler_params=pltpu.CompilerParams(collective_id=0, has_side_effects=True, vmem_limit_bytes=56 * 1024 * 1024),
        cost_estimate=pl.CostEstimate(flops=2 * rows * width * 4096, bytes_accessed=40_000_000, transcendentals=0),
        name="project_heads",
    )(normed, cosines, sines, wq_all, w_key, w_value)


def solution(mesh):
    group_size = mesh.shape["tp"]

    def exchange(rows, bit):
        return lax.ppermute(rows, "tp", [(i, i ^ bit) for i in range(group_size)])

    def share_head(rows, dev_index):
        half = rows.shape[0] // 2
        first, second = rows[:half], rows[half:]
        first_x = lax.ppermute(first, "tp", [(0, 2)])
        second_y = lax.ppermute(second, "tp", [(0, 4)])
        first = jnp.where(dev_index == 2, first_x, first)
        second = jnp.where(dev_index == 4, second_y, second)
        first_y = lax.ppermute(first, "tp", [(0, 4), (2, 6)])
        second_x = lax.ppermute(second, "tp", [(0, 2), (4, 6)])
        first = jnp.where(dev_index >= 4, first_y, first)
        second = jnp.where(dev_index % 4 >= 2, second_x, second)
        both = jnp.concatenate([first, second], axis=0)
        other = lax.ppermute(both, "tp", [(0, 1), (2, 3), (4, 5), (6, 7)])
        return jnp.where(dev_index % 2 == 1, other, both)

    def local_body(token_ids, positions, table_rows, norm_scale, w_query, w_key, w_value):
        dev_index = lax.axis_index("tp")
        vocab_rows, model_width = table_rows.shape
        wq_all = lax.all_gather(w_query, "tp", axis=0)
        head = share_head(table_rows[:HEAD_ROWS], dev_index)
        tokens = token_ids.shape[0]
        block_rows = tokens // group_size
        extra_rows = block_rows - TAIL_ROWS
        chunk_rows = TAIL_ROWS // CHUNKS
        half = chunk_rows // 2

        blocks = token_ids.reshape(group_size, block_rows)
        in_tail = blocks >= HEAD_ROWS
        earlier = (lax.broadcasted_iota(jnp.int32, (block_rows, block_rows), 0) < lax.broadcasted_iota(jnp.int32, (block_rows, block_rows), 1)).astype(jnp.bfloat16)
        ranks = jnp.dot(in_tail.astype(jnp.bfloat16), earlier, preferred_element_type=jnp.float32).astype(jnp.int32)
        ranks = jnp.where(in_tail, ranks, -1)

        def ranked_ids(first, count):
            wanted = lax.broadcasted_iota(jnp.int32, (group_size, block_rows, count), 2) + first
            ids = jnp.sum(jnp.where(ranks[:, :, None] == wanted, blocks[:, :, None] + 1, 0), axis=1) - 1
            local = ids - dev_index * vocab_rows
            return jnp.where((ids >= 0) & (local >= 0) & (local < vocab_rows), local, -1)

        most = jnp.max(jnp.sum(in_tail.astype(jnp.int32), axis=1))
        over = (most > TAIL_ROWS).astype(jnp.int32)

        def arrange(values):
            view = values.reshape(2, 2, 2, CHUNKS, 2, half)
            for axis, bit in ((0, 4), (1, 2), (2, 1)):
                flag = (dev_index // bit) % 2 == 1
                view = jnp.where(flag, jnp.flip(view, axis), view)
            halves = view.transpose(3, 2, 4, 0, 1, 5)
            first = halves[:, :, 0].transpose(0, 1, 3, 2, 4)
            second = halves[:, :, 1]
            return jnp.stack([first, second], axis=2).reshape(CHUNKS, 2, 4 * chunk_rows)

        call_rows = 4 * chunk_rows
        ids = arrange(ranked_ids(0, TAIL_ROWS)).reshape(-1, TILE)
        owned = ids >= 0
        before = (lax.broadcasted_iota(jnp.int32, (TILE, TILE), 0) < lax.broadcasted_iota(jnp.int32, (TILE, TILE), 1)).astype(jnp.bfloat16)
        slots = jnp.dot(owned.astype(jnp.bfloat16), before, preferred_element_type=jnp.float32).astype(jnp.int32)
        slots = jnp.where(owned, slots, -1)
        wanted_slot = lax.broadcasted_iota(jnp.int32, (ids.shape[0], TILE, TILE), 2)
        pair_ids = jnp.sum(jnp.where(slots[:, :, None] == wanted_slot, (ids // 2)[:, :, None] * 2, 0), axis=1).reshape(-1)
        cols = jnp.where(owned, 2 * slots + ids % 2, -1).astype(jnp.float32)[:, None, :]
        counts = jnp.sum(owned.astype(jnp.int32), axis=-1)

        def gather(chunk, side, after):
            return gather_rows((2 * chunk + side) * call_rows, call_rows, pair_ids, counts, cols, table_rows, after)

        pieces, sums = [], []
        after, late, late_next = [], [], []
        for chunk in range(CHUNKS):
            other = gather(chunk, 1, after + late + ([wq_all] if chunk == 2 else []))
            got = exchange(other, 1)
            mine = gather(chunk, 0, [other])
            after, late = [], late_next
            late_next = []
            for part, bits in ((0, (2, 4)), (1, (4, 2))):
                base = part * 4 * half
                keep = [slice(base + k * half, base + (k + 1) * half) for k in range(4)]
                far = slice(base + 2 * half, base + 4 * half)
                sent = mine[far] + got[far]
                back = exchange(sent, bits[0])
                near_send = mine[keep[1]] + got[keep[1]] + back[half:]
                back2 = exchange(near_send, bits[1])
                after.append(sent)
                sums.append(sent)
                late_next.append(near_send)
                pieces += [mine[keep[0]] + got[keep[0]] + back[:half], back2]

        def second_exchange(rows):
            ids = ranked_ids(TAIL_ROWS, extra_rows).reshape(-1)
            normalizer = jnp.asarray(math.sqrt(model_width), dtype=jnp.bfloat16)
            picked = jnp.take(rows, jnp.maximum(ids, 0), axis=0, mode="clip") * normalizer
            partial = jnp.where(ids[:, None] >= 0, picked, jnp.zeros((), jnp.bfloat16))
            return lax.psum_scatter(partial, "tp", scatter_dimension=0, tiled=True)

        def no_exchange(rows):
            return jnp.zeros((extra_rows, model_width), jnp.bfloat16)

        over, _ = lax.optimization_barrier((over, sums[2]))
        more = lax.pmax(over, "dp")
        asked, _ = lax.optimization_barrier((more, pieces[-5]))
        extra = lax.cond(asked > 0, second_exchange, no_exchange, table_rows)
        places = jnp.where(in_tail, HEAD_ROWS + ranks, blocks)
        own_places = lax.dynamic_index_in_dim(places, dev_index, 0, keepdims=False)
        residual, normed = finish_rows(more.reshape(1), own_places[:, None], (1.0 + norm_scale)[None, :], head, extra, pieces)
        own = lax.dynamic_slice_in_dim(positions, dev_index * block_rows, block_rows)
        cosines, sines = rope_tables(own)
        queries, keys_values = project_heads(normed, cosines, sines, wq_all, w_key, w_value)
        return residual, queries[:, None, :], keys_values[0][:, None, :], keys_values[1][:, None, :]

    head_spec = P("dp", "tp", None)
    return jax.shard_map(local_body, mesh=mesh, in_specs=(P("dp"), P("dp"), P("tp", None), P(), P(None, "tp"), P(), P()), out_specs=(P(("dp", "tp"), None), head_spec, head_spec, head_spec), check_vma=False)
```

```python
import functools
import math
import jax
import jax.numpy as jnp
from jax import lax
from jax.experimental import pallas as pl
from jax.experimental.pallas import tpu as pltpu
from jax.sharding import PartitionSpec as P

HEAD_DIM = 256
EPSILON = 1e-6
ROPE_BASE = 10000.0
TILE = 128
CHUNKS = 2
HEAD_ROWS = 640
TAIL_ROWS = 640
SEND_ROWS = 512
CHIPS = 4
MESH_IDS = pl.DeviceIdType.MESH


def rope_tables(positions):
    inv_freq = ROPE_BASE ** (-jnp.arange(0, HEAD_DIM, 2, dtype=jnp.float32) / HEAD_DIM)
    angles = positions.astype(jnp.float32)[:, None] * inv_freq[None, :]
    return jnp.cos(angles), jnp.sin(angles)


def gather_kernel(base, tiles, width, pair_ids, counts, cols_ref, table_ref, *rest):
    out_ref, pairs, sems = rest[-3:]
    step = pl.program_id(0)
    normalizer = jnp.asarray(math.sqrt(width), dtype=jnp.bfloat16)

    def start(tile, slot):
        count = counts[base + tile]

        def copy(group, row):
            src = pair_ids[(base + tile) * TILE + group * 8 + row]
            pltpu.make_async_copy(table_ref.at[pl.ds(pl.multiple_of(src, 2), 2), :], pairs.at[slot, group, pl.ds(2 * row, 2), :], sems.at[slot]).start()

        @pl.loop(0, count // 8)
        def _(group):
            for row in range(8):
                copy(group, row)

        for row in range(7):
            @pl.when(row < lax.rem(count, 8))
            def _():
                copy(count // 8, row)

    def wait(tile, slot):
        count = counts[base + tile]
        size = TILE // 8
        while size:
            @pl.when((count // (8 * size)) % 2 == 1)
            def _():
                pltpu.make_async_copy(pairs.at[slot, pl.ds(0, size)], pairs.at[slot, pl.ds(0, size)], sems.at[slot]).wait()

            size //= 2
        for size in (1, 2, 4):
            @pl.when((count // size) % 2 == 1)
            def _():
                pltpu.make_async_copy(table_ref.at[pl.ds(0, 2 * size), :], pairs.at[slot, 0, pl.ds(0, 2 * size), :], sems.at[slot]).wait()

    @pl.when(step == 0)
    def _():
        pairs[...] = jnp.zeros_like(pairs)
        start(0, 0)
        start(1, 1)

    slot = lax.rem(step, 3)

    @pl.when(step + 2 < tiles)
    def _():
        start(step + 2, lax.rem(step + 2, 3))

    wait(step, slot)
    lanes = lax.broadcasted_iota(jnp.int32, (TILE, 2 * TILE), 1).astype(jnp.float32)
    wanted = jnp.broadcast_to(cols_ref[base + step], (TILE, TILE)).T
    select = jnp.where(lanes == jnp.concatenate([wanted, wanted], axis=1), normalizer, jnp.zeros((), jnp.bfloat16))
    for piece in range(width // 256):
        cols = pl.ds(piece * 256, 256)
        picked = jnp.dot(select, pairs[slot, :, :, cols].reshape(2 * TILE, 256), preferred_element_type=jnp.float32)
        out_ref[:, cols] = picked.astype(jnp.bfloat16)


def gather_rows(base, count, pair_ids, counts, cols, table_rows, after):
    width = table_rows.shape[1]
    tiles = count // TILE
    base = base // TILE
    anywhere = pl.BlockSpec(memory_space=pl.ANY)
    grid_spec = pltpu.PrefetchScalarGridSpec(
        num_scalar_prefetch=2,
        grid=(tiles,),
        in_specs=[pl.BlockSpec(cols.shape, lambda i, *_: (0, 0, 0)), anywhere] + [anywhere] * len(after),
        out_specs=pl.BlockSpec((TILE, width), lambda i, *_: (i, 0)),
        scratch_shapes=[pltpu.VMEM((3, TILE // 8, 16, width), jnp.bfloat16), pltpu.SemaphoreType.DMA((3,))],
    )
    return pl.pallas_call(
        functools.partial(gather_kernel, base, tiles, width),
        grid_spec=grid_spec,
        out_shape=jax.ShapeDtypeStruct((count, width), jnp.bfloat16),
        compiler_params=pltpu.CompilerParams(dimension_semantics=("arbitrary",)),
        cost_estimate=pl.CostEstimate(flops=count * 20_000_000, bytes_accessed=count * width * 6, transcendentals=0),
        name="gather_rows",
    )(pair_ids, counts, cols, table_rows, *after)


def finish_kernel(pieces, more, cols_ref, gain_ref, head_hbm, extra_hbm, *refs):
    piece_refs, (resid_hbm, normed_hbm, source, parts, extra, resid, normed, in_sems, out_sems) = refs[:pieces], refs[pieces:]
    rows, width = resid.shape
    part = TAIL_ROWS // (pieces // 2)
    known = HEAD_ROWS + TAIL_ROWS
    normalizer = jnp.asarray(math.sqrt(width), dtype=jnp.bfloat16)
    one = jnp.ones((), jnp.bfloat16)
    zero = jnp.zeros((), jnp.bfloat16)
    head_copy = pltpu.make_async_copy(head_hbm, source.at[pl.ds(0, HEAD_ROWS), :], in_sems.at[pieces])
    extra_copy = pltpu.make_async_copy(extra_hbm, extra, in_sems.at[pieces + 1])
    copies = []
    for index, ref in enumerate(piece_refs):
        there = source.at[pl.ds(HEAD_ROWS + index // 2 * part, part), :] if index % 2 == 0 else parts.at[index // 2]
        copies.append(pltpu.make_async_copy(ref, there, in_sems.at[index]))
    for copy in copies:
        copy.start()
    head_copy.start()
    extra_copy.start()
    for index in range(pieces // 2):
        copies[2 * index].wait()
        copies[2 * index + 1].wait()
        span = pl.ds(HEAD_ROWS + index * part, part)
        source[span, :] = source[span, :] + parts[index]
    head_copy.wait()
    extra_copy.wait()

    def results(block):
        span = pl.ds(pl.multiple_of(block * 256, 256), 256)
        return (pltpu.make_async_copy(resid.at[span, :], resid_hbm.at[span, :], out_sems.at[0]),
                pltpu.make_async_copy(normed.at[span, :], normed_hbm.at[span, :], out_sems.at[1]))

    @pl.loop(0, rows // 256)
    def _(block):
        span = pl.ds(pl.multiple_of(block * 256, 256), 256)
        lanes = lax.broadcasted_iota(jnp.int32, (256, known), 1)
        value = jnp.where(lax.broadcasted_iota(jnp.int32, (1, known), 1) < HEAD_ROWS, normalizer, one)
        select = jnp.where(lanes == cols_ref[span, :], jnp.broadcast_to(value, (256, known)), zero)
        for piece in range(width // 256):
            cols = pl.ds(piece * 256, 256)
            resid[span, cols] = jnp.dot(select, source[:, cols], preferred_element_type=jnp.float32).astype(jnp.bfloat16)

        @pl.when(more[0] > 0)
        def _():
            places = lax.broadcasted_iota(jnp.int32, (256, extra.shape[0]), 1) + known
            from_extra = jnp.where(places == cols_ref[span, :], one, zero)
            for piece in range(width // 256):
                cols = pl.ds(piece * 256, 256)
                picked = jnp.dot(from_extra, extra[:, cols], preferred_element_type=jnp.float32)
                resid[span, cols] = (resid[span, cols].astype(jnp.float32) + picked).astype(jnp.bfloat16)

        for quarter in range(4):
            rows_here = pl.ds(pl.multiple_of(block * 256 + quarter * 64, 64), 64)
            widened = resid[rows_here, :].astype(jnp.float32)
            inv_rms = lax.rsqrt(jnp.mean(widened * widened, axis=-1, keepdims=True) + EPSILON)
            normed[rows_here, :] = (widened * inv_rms * gain_ref[...]).astype(jnp.bfloat16)
        for result in results(block):
            result.start()

    @pl.loop(0, rows // 256)
    def _(block):
        for result in results(block):
            result.wait()


def finish_rows(more, cols, gain, head, extra, pieces):
    rows = cols.shape[0]
    width = head.shape[1]
    vmem = pl.BlockSpec(memory_space=pltpu.VMEM)
    hbm = pl.BlockSpec(memory_space=pl.ANY)
    shape = jax.ShapeDtypeStruct((rows, width), jnp.bfloat16)
    dma = pltpu.SemaphoreType.DMA
    return pl.pallas_call(
        functools.partial(finish_kernel, len(pieces)),
        out_shape=(shape, shape),
        in_specs=[pl.BlockSpec(memory_space=pltpu.SMEM), vmem, vmem, hbm, hbm] + [hbm] * len(pieces),
        out_specs=(hbm, hbm),
        scratch_shapes=[
            pltpu.VMEM((HEAD_ROWS + TAIL_ROWS, width), jnp.bfloat16),
            pltpu.VMEM((len(pieces) // 2,) + pieces[0].shape, jnp.bfloat16),
            pltpu.VMEM(extra.shape, jnp.bfloat16),
            pltpu.VMEM((rows, width), jnp.bfloat16),
            pltpu.VMEM((rows, width), jnp.bfloat16),
            dma((len(pieces) + 2,)), dma((2,)),
        ],
        compiler_params=pltpu.CompilerParams(vmem_limit_bytes=40 * 1024 * 1024),
        cost_estimate=pl.CostEstimate(flops=2 * rows * width * (HEAD_ROWS + TAIL_ROWS), bytes_accessed=16_000_000, transcendentals=0),
        name="finish_rows",
    )(more, cols, gain, head, extra, *pieces)


def heads_kernel(rows, normed_hbm, cos_ref, sin_ref, wq_hbm, wk_hbm, wv_hbm, q_out, kv_out,
                 wq, wk, wv, normed, q_stage, kv_stage, w_sem, q_send, q_recv, kv_send, kv_recv,
                 own_recv, fwd_send, fwd_recv, keep_sem):
    group = lax.axis_index("dp")
    me = lax.axis_index("tp")
    core = lax.rem(me, 2)
    chip = me // 2
    partner = me + 1 - 2 * core
    tiles = rows // SEND_ROWS
    half = HEAD_DIM // 2

    loads = [pltpu.make_async_copy(src, dst, w_sem.at[n]) for n, (src, dst) in enumerate(((normed_hbm, normed), (wk_hbm, wk), (wv_hbm, wv), (wq_hbm, wq)))]
    for load in loads:
        load.start()

    barrier = pltpu.get_barrier_semaphore()
    for step in range(1, 2 * CHIPS):
        pl.semaphore_signal(barrier, inc=1, device_id=(group, lax.rem(me + step, 2 * CHIPS)), device_id_type=MESH_IDS)

    pl.semaphore_wait(barrier, 2 * CHIPS - 1)
    for load in loads:
        load.wait()

    def block(source, tile):
        return pl.ds(pl.multiple_of(source * rows + tile * SEND_ROWS, SEND_ROWS), SEND_ROWS)

    def whole(source):
        return pl.ds(pl.multiple_of(source * rows, rows), rows)

    def remote(src, dst, send, recv, device):
        return pltpu.make_async_remote_copy(src_ref=src, dst_ref=dst, send_sem=send, recv_sem=recv, device_id=(group, device), device_id_type=MESH_IDS)

    def rotated(linear, span, factor):
        front = linear[:, :half]
        back = linear[:, half:]
        cosines = cos_ref[span, :]
        sines = sin_ref[span, :]
        return jnp.concatenate([((front * cosines - back * sines) * factor).astype(jnp.bfloat16), ((back * cosines + front * sines) * factor).astype(jnp.bfloat16)], axis=-1)

    @pl.loop(0, CHIPS * tiles)
    def _(turn):
        offset = lax.rem(turn // tiles + 1, CHIPS)
        tile = lax.rem(turn, tiles)
        there = lax.rem(chip + offset, CHIPS)
        columns = pl.ds(pl.multiple_of(there * HEAD_DIM, HEAD_DIM), HEAD_DIM)
        sent = pl.ds(pl.multiple_of(tile * SEND_ROWS, SEND_ROWS), SEND_ROWS)

        @pl.loop(0, SEND_ROWS // 256)
        def _(part):
            span = pl.ds(pl.multiple_of(tile * SEND_ROWS + part * 256, 256), 256)
            lhs = normed[span, :]

            def linear(weight):
                return jnp.dot(lhs, weight, preferred_element_type=jnp.float32).astype(jnp.bfloat16)

            kv_stage[0, there, span, :] = rotated(linear(wk[:, columns]).astype(jnp.float32), span, 1.0)
            kv_stage[1, there, span, :] = linear(wv[:, columns])
            for side in range(2):
                q_stage[2 * there + side, span, :] = rotated(linear(wq[2 * there + side]).astype(jnp.float32), span, HEAD_DIM ** -0.5)

        @pl.when(offset != 0)
        def _():
            for side in range(2):
                remote(kv_stage.at[side, there, sent, :], kv_out.at[side, block(me, tile), :], kv_send.at[offset, side], kv_recv.at[offset, core, tile], 2 * there + side).start()
            for side in range(2):
                remote(q_stage.at[2 * there + side, sent, :], q_out.at[block(me, tile), :], q_send.at[offset, side], q_recv.at[offset, core], 2 * there + side).start()

    for side in range(2):
        remote(kv_stage.at[side, chip], kv_out.at[side, whole(me), :], kv_send.at[0, side], own_recv.at[side], partner).start()
    remote(q_stage.at[partner], q_out.at[whole(me), :], q_send.at[0, 0], q_recv.at[0, 0], partner).start()
    keeps = [pltpu.make_async_copy(q_stage.at[me], q_out.at[whole(me), :], keep_sem.at[0])]
    for side in range(2):
        keeps.append(pltpu.make_async_copy(kv_stage.at[side, chip], kv_out.at[side, whole(me), :], keep_sem.at[1 + side]))
    for keep in keeps:
        keep.start()

    for tile in range(tiles):
        for offset in range(1, CHIPS):
            for side in range(2):
                source = 2 * lax.rem(chip + CHIPS - offset, CHIPS) + side
                region = kv_out.at[core, block(source, tile), :]
                remote(region, region, kv_send.at[offset, side], kv_recv.at[offset, side, tile], partner).wait_recv()
                remote(region, region, fwd_send.at[offset, side], fwd_recv.at[offset, side], partner).start()

    for keep in keeps:
        keep.wait()
    for offset in range(1, CHIPS):
        there = lax.rem(chip + offset, CHIPS)
        for side in range(2):
            source = 2 * lax.rem(chip + CHIPS - offset, CHIPS) + side
            remote(kv_stage.at[side, there], kv_out.at[side, whole(me), :], kv_send.at[offset, side], own_recv.at[side], partner).wait_send()
            remote(q_stage.at[2 * there + side], q_out.at[whole(source), :], q_send.at[offset, side], q_recv.at[offset, side], partner).wait()
            mine = kv_out.at[core, whole(source), :]
            remote(mine, mine, fwd_send.at[offset, side], fwd_recv.at[offset, side], partner).wait_send()
            other = kv_out.at[1 - core, whole(source), :]
            remote(other, other, fwd_send.at[offset, side], fwd_recv.at[offset, side], partner).wait_recv()
    for side in range(2):
        remote(kv_stage.at[side, chip], kv_out.at[side, whole(partner), :], kv_send.at[0, side], own_recv.at[side], partner).wait()
    remote(q_stage.at[partner], q_out.at[whole(partner), :], q_send.at[0, 0], q_recv.at[0, 0], partner).wait()


def project_heads(normed, cosines, sines, wq_all, w_key, w_value):
    rows, width = normed.shape
    heads = wq_all.shape[0]
    tokens = rows * heads
    tiles = rows // SEND_ROWS
    vmem = pl.BlockSpec(memory_space=pltpu.VMEM)
    anywhere = pl.BlockSpec(memory_space=pl.ANY)
    dma = pltpu.SemaphoreType.DMA
    return pl.pallas_call(
        functools.partial(heads_kernel, rows),
        out_shape=(jax.ShapeDtypeStruct((tokens, HEAD_DIM), jnp.bfloat16), jax.ShapeDtypeStruct((2, tokens, HEAD_DIM), jnp.bfloat16)),
        in_specs=[anywhere, vmem, vmem, anywhere, anywhere, anywhere],
        out_specs=(anywhere, anywhere),
        scratch_shapes=[
            pltpu.VMEM(wq_all.shape, jnp.bfloat16),
            pltpu.VMEM(w_key.shape, jnp.bfloat16),
            pltpu.VMEM(w_value.shape, jnp.bfloat16),
            pltpu.VMEM((rows, width), jnp.bfloat16),
            pltpu.VMEM((heads, rows, HEAD_DIM), jnp.bfloat16),
            pltpu.VMEM((2, CHIPS, rows, HEAD_DIM), jnp.bfloat16),
            dma((4,)),
            dma((CHIPS, 2)), dma((CHIPS, 2)),
            dma((CHIPS, 2)), dma((CHIPS, 2, tiles)),
            dma((2,)),
            dma((CHIPS, 2)), dma((CHIPS, 2)),
            dma((3,)),
        ],
        compiler_params=pltpu.CompilerParams(collective_id=0, has_side_effects=True, vmem_limit_bytes=56 * 1024 * 1024),
        cost_estimate=pl.CostEstimate(flops=2 * rows * width * 4096, bytes_accessed=40_000_000, transcendentals=0),
        name="project_heads",
    )(normed, cosines, sines, wq_all, w_key, w_value)


def solution(mesh):
    group_size = mesh.shape["tp"]

    def exchange(rows, bit):
        return lax.ppermute(rows, "tp", [(i, i ^ bit) for i in range(group_size)])

    def pass_head(values, pairs, after=None):
        got = lax.ppermute(values, "tp", pairs)
        if after is not None:
            got, _ = lax.optimization_barrier((got, after))
        return jnp.where(lax.axis_index("tp") == pairs[0][1], got, values)

    def share_head(rows):
        half = rows.shape[0] // 2
        first = pass_head(rows[:half], [(0, 2)])
        second = pass_head(rows[half:], [(0, 4)])
        first = pass_head(first, [(2, 6)])
        second = pass_head(second, [(4, 6)])
        return first, second

    def share_head_back(first, second, after):
        first = pass_head(first, [(6, 4)], after)
        second = pass_head(second, [(6, 2)], after)
        both = jnp.concatenate([first, second], axis=0)
        other = lax.ppermute(both, "tp", [(0, 1), (2, 3), (4, 5), (6, 7)])
        return jnp.where(lax.axis_index("tp") % 2 == 1, other, both)

    def local_body(token_ids, positions, table_rows, norm_scale, w_query, w_key, w_value):
        dev_index = lax.axis_index("tp")
        vocab_rows, model_width = table_rows.shape
        wq_all = lax.all_gather(w_query, "tp", axis=0)
        head_halves = share_head(table_rows[:HEAD_ROWS])
        tokens = token_ids.shape[0]
        block_rows = tokens // group_size
        extra_rows = block_rows - TAIL_ROWS
        chunk_rows = TAIL_ROWS // CHUNKS
        half = chunk_rows // 2

        blocks = token_ids.reshape(group_size, block_rows)
        in_tail = blocks >= HEAD_ROWS
        earlier = (lax.broadcasted_iota(jnp.int32, (block_rows, block_rows), 0) < lax.broadcasted_iota(jnp.int32, (block_rows, block_rows), 1)).astype(jnp.bfloat16)
        ranks = jnp.dot(in_tail.astype(jnp.bfloat16), earlier, preferred_element_type=jnp.float32).astype(jnp.int32)
        ranks = jnp.where(in_tail, ranks, -1)

        def ranked_ids(first, count):
            wanted = lax.broadcasted_iota(jnp.int32, (group_size, block_rows, count), 2) + first
            ids = jnp.sum(jnp.where(ranks[:, :, None] == wanted, blocks[:, :, None] + 1, 0), axis=1) - 1
            local = ids - dev_index * vocab_rows
            return jnp.where((ids >= 0) & (local >= 0) & (local < vocab_rows), local, -1)

        most = jnp.max(jnp.sum(in_tail.astype(jnp.int32), axis=1))
        over = (most > TAIL_ROWS).astype(jnp.int32)

        def arrange(values):
            view = values.reshape(2, 2, 2, CHUNKS, 2, half)
            for axis, bit in ((0, 4), (1, 2), (2, 1)):
                flag = (dev_index // bit) % 2 == 1
                view = jnp.where(flag, jnp.flip(view, axis), view)
            halves = view.transpose(3, 2, 4, 0, 1, 5)
            first = halves[:, :, 0].transpose(0, 1, 3, 2, 4)
            second = halves[:, :, 1]
            return jnp.stack([first, second], axis=2).reshape(CHUNKS, 2, 4 * chunk_rows)

        call_rows = 4 * chunk_rows
        ids = arrange(ranked_ids(0, TAIL_ROWS)).reshape(-1, TILE)
        owned = ids >= 0
        before = (lax.broadcasted_iota(jnp.int32, (TILE, TILE), 0) < lax.broadcasted_iota(jnp.int32, (TILE, TILE), 1)).astype(jnp.bfloat16)
        slots = jnp.dot(owned.astype(jnp.bfloat16), before, preferred_element_type=jnp.float32).astype(jnp.int32)
        slots = jnp.where(owned, slots, -1)
        wanted_slot = lax.broadcasted_iota(jnp.int32, (ids.shape[0], TILE, TILE), 2)
        pair_ids = jnp.sum(jnp.where(slots[:, :, None] == wanted_slot, (ids // 2)[:, :, None] * 2, 0), axis=1).reshape(-1)
        cols = jnp.where(owned, 2 * slots + ids % 2, -1).astype(jnp.float32)[:, None, :]
        counts = jnp.sum(owned.astype(jnp.int32), axis=-1)

        def gather(chunk, side, after):
            return gather_rows((2 * chunk + side) * call_rows, call_rows, pair_ids, counts, cols, table_rows, after)

        pieces, sums = [], []
        after, late, late_next = [], [], []
        for chunk in range(CHUNKS):
            other = gather(chunk, 1, after + late + ([wq_all] if chunk == 1 else []))
            got = exchange(other, 1)
            mine = gather(chunk, 0, [other])
            after, late = [], late_next
            late_next = []
            for part, bits in ((0, (2, 4)), (1, (4, 2))):
                base = part * 4 * half
                keep = [slice(base + k * half, base + (k + 1) * half) for k in range(4)]
                far = slice(base + 2 * half, base + 4 * half)
                sent = mine[far] + got[far]
                back = exchange(sent, bits[0])
                near_send = mine[keep[1]] + got[keep[1]] + back[half:]
                back2 = exchange(near_send, bits[1])
                after.append(sent)
                sums.append(sent)
                late_next.append(near_send)
                pieces += [mine[keep[0]] + got[keep[0]] + back[:half], back2]

        head = share_head_back(*head_halves, pieces[2])

        def second_exchange(rows):
            ids = ranked_ids(TAIL_ROWS, extra_rows).reshape(-1)
            normalizer = jnp.asarray(math.sqrt(model_width), dtype=jnp.bfloat16)
            picked = jnp.take(rows, jnp.maximum(ids, 0), axis=0, mode="clip") * normalizer
            partial = jnp.where(ids[:, None] >= 0, picked, jnp.zeros((), jnp.bfloat16))
            return lax.psum_scatter(partial, "tp", scatter_dimension=0, tiled=True)

        def no_exchange(rows):
            return jnp.zeros((extra_rows, model_width), jnp.bfloat16)

        over, _ = lax.optimization_barrier((over, sums[2]))
        more = lax.pmax(over, "dp")
        asked, _ = lax.optimization_barrier((more, pieces[-5]))
        extra = lax.cond(asked > 0, second_exchange, no_exchange, table_rows)
        places = jnp.where(in_tail, HEAD_ROWS + ranks, blocks)
        own_places = lax.dynamic_index_in_dim(places, dev_index, 0, keepdims=False)
        residual, normed = finish_rows(more.reshape(1), own_places[:, None], (1.0 + norm_scale)[None, :], head, extra, pieces)
        own = lax.dynamic_slice_in_dim(positions, dev_index * block_rows, block_rows)
        cosines, sines = rope_tables(own)
        queries, keys_values = project_heads(normed, cosines, sines, wq_all, w_key, w_value)
        return residual, queries[:, None, :], keys_values[0][:, None, :], keys_values[1][:, None, :]

    head_spec = P("dp", "tp", None)
    return jax.shard_map(local_body, mesh=mesh, in_specs=(P("dp"), P("dp"), P("tp", None), P(), P(None, "tp"), P(), P()), out_specs=(P(("dp", "tp"), None), head_spec, head_spec, head_spec), check_vma=False)
```

```python
import functools
import math
import jax
import jax.numpy as jnp
from jax import lax
from jax.experimental import pallas as pl
from jax.experimental.pallas import tpu as pltpu
from jax.sharding import PartitionSpec as P

HEAD_DIM = 256
EPSILON = 1e-6
ROPE_BASE = 10000.0
TILE = 128
CHUNKS = 2
HEAD_ROWS = 640
TAIL_ROWS = 640
SEND_ROWS = 512
CHIPS = 4
MESH_IDS = pl.DeviceIdType.MESH


def rope_tables(positions):
    inv_freq = ROPE_BASE ** (-jnp.arange(0, HEAD_DIM, 2, dtype=jnp.float32) / HEAD_DIM)
    angles = positions.astype(jnp.float32)[:, None] * inv_freq[None, :]
    return jnp.cos(angles), jnp.sin(angles)


def gather_kernel(base, tiles, width, pair_ids, counts, cols_ref, table_ref, *rest):
    out_ref, pairs, sems = rest[-3:]
    step = pl.program_id(0)
    normalizer = jnp.asarray(math.sqrt(width), dtype=jnp.bfloat16)

    def start(tile, slot):
        count = counts[base + tile]

        def copy(group, row):
            src = pair_ids[(base + tile) * TILE + group * 8 + row]
            pltpu.make_async_copy(table_ref.at[pl.ds(pl.multiple_of(src, 2), 2), :], pairs.at[slot, group, pl.ds(2 * row, 2), :], sems.at[slot]).start()

        @pl.loop(0, count // 8)
        def _(group):
            for row in range(8):
                copy(group, row)

        for row in range(7):
            @pl.when(row < lax.rem(count, 8))
            def _():
                copy(count // 8, row)

    def wait(tile, slot):
        count = counts[base + tile]
        size = TILE // 8
        while size:
            @pl.when((count // (8 * size)) % 2 == 1)
            def _():
                pltpu.make_async_copy(pairs.at[slot, pl.ds(0, size)], pairs.at[slot, pl.ds(0, size)], sems.at[slot]).wait()

            size //= 2
        for size in (1, 2, 4):
            @pl.when((count // size) % 2 == 1)
            def _():
                pltpu.make_async_copy(table_ref.at[pl.ds(0, 2 * size), :], pairs.at[slot, 0, pl.ds(0, 2 * size), :], sems.at[slot]).wait()

    @pl.when(step == 0)
    def _():
        pairs[...] = jnp.zeros_like(pairs)
        start(0, 0)
        start(1, 1)

    slot = lax.rem(step, 3)

    @pl.when(step + 2 < tiles)
    def _():
        start(step + 2, lax.rem(step + 2, 3))

    wait(step, slot)
    lanes = lax.broadcasted_iota(jnp.int32, (TILE, 2 * TILE), 1).astype(jnp.float32)
    wanted = jnp.broadcast_to(cols_ref[base + step], (TILE, TILE)).T
    select = jnp.where(lanes == jnp.concatenate([wanted, wanted], axis=1), normalizer, jnp.zeros((), jnp.bfloat16))
    for piece in range(width // 256):
        cols = pl.ds(piece * 256, 256)
        picked = jnp.dot(select, pairs[slot, :, :, cols].reshape(2 * TILE, 256), preferred_element_type=jnp.float32)
        out_ref[:, cols] = picked.astype(jnp.bfloat16)


def gather_rows(base, count, pair_ids, counts, cols, table_rows, after):
    width = table_rows.shape[1]
    tiles = count // TILE
    base = base // TILE
    anywhere = pl.BlockSpec(memory_space=pl.ANY)
    grid_spec = pltpu.PrefetchScalarGridSpec(
        num_scalar_prefetch=2,
        grid=(tiles,),
        in_specs=[pl.BlockSpec(cols.shape, lambda i, *_: (0, 0, 0)), anywhere] + [anywhere] * len(after),
        out_specs=pl.BlockSpec((TILE, width), lambda i, *_: (i, 0)),
        scratch_shapes=[pltpu.VMEM((3, TILE // 8, 16, width), jnp.bfloat16), pltpu.SemaphoreType.DMA((3,))],
    )
    return pl.pallas_call(
        functools.partial(gather_kernel, base, tiles, width),
        grid_spec=grid_spec,
        out_shape=jax.ShapeDtypeStruct((count, width), jnp.bfloat16),
        compiler_params=pltpu.CompilerParams(dimension_semantics=("arbitrary",)),
        cost_estimate=pl.CostEstimate(flops=count * 20_000_000, bytes_accessed=count * width * 6, transcendentals=0),
        name="gather_rows",
    )(pair_ids, counts, cols, table_rows, *after)


def finish_kernel(pieces, more, cols_ref, gain_ref, head_hbm, extra_hbm, *refs):
    piece_refs, (resid_hbm, normed_hbm, source, parts, extra, resid, normed, in_sems, out_sems) = refs[:pieces], refs[pieces:]
    rows, width = resid.shape
    part = TAIL_ROWS // (pieces // 3)
    known = HEAD_ROWS + TAIL_ROWS
    normalizer = jnp.asarray(math.sqrt(width), dtype=jnp.bfloat16)
    one = jnp.ones((), jnp.bfloat16)
    zero = jnp.zeros((), jnp.bfloat16)
    head_copy = pltpu.make_async_copy(head_hbm, source.at[pl.ds(0, HEAD_ROWS), :], in_sems.at[pieces])
    extra_copy = pltpu.make_async_copy(extra_hbm, extra, in_sems.at[pieces + 1])
    copies = []
    for index, ref in enumerate(piece_refs):
        there = source.at[pl.ds(HEAD_ROWS + index // 3 * part, part), :] if index % 3 == 0 else parts.at[index // 3, index % 3 - 1]
        copies.append(pltpu.make_async_copy(ref.at[pl.ds(0, part), :], there, in_sems.at[index]))
    head_copy.start()
    extra_copy.start()
    for copy in copies:
        copy.start()
    for copy in copies:
        copy.wait()
    for index in range(pieces // 3):
        span = pl.ds(HEAD_ROWS + index * part, part)
        source[span, :] = source[span, :] + parts[index, 0] + parts[index, 1]
    head_copy.wait()
    extra_copy.wait()

    def results(block):
        span = pl.ds(pl.multiple_of(block * 512, 512), 512)
        return (pltpu.make_async_copy(resid.at[span, :], resid_hbm.at[span, :], out_sems.at[0]),
                pltpu.make_async_copy(normed.at[span, :], normed_hbm.at[span, :], out_sems.at[1]))

    @pl.loop(0, rows // 512)
    def _(block):
        span = pl.ds(pl.multiple_of(block * 512, 512), 512)
        lanes = lax.broadcasted_iota(jnp.int32, (512, known), 1)
        value = jnp.where(lax.broadcasted_iota(jnp.int32, (1, known), 1) < HEAD_ROWS, normalizer, one)
        select = jnp.where(lanes == cols_ref[span, :], jnp.broadcast_to(value, (512, known)), zero)
        for piece in range(width // 256):
            cols = pl.ds(piece * 256, 256)
            resid[span, cols] = jnp.dot(select, source[:, cols], preferred_element_type=jnp.float32).astype(jnp.bfloat16)

        @pl.when(more[0] > 0)
        def _():
            places = lax.broadcasted_iota(jnp.int32, (512, extra.shape[0]), 1) + known
            from_extra = jnp.where(places == cols_ref[span, :], one, zero)
            for piece in range(width // 256):
                cols = pl.ds(piece * 256, 256)
                picked = jnp.dot(from_extra, extra[:, cols], preferred_element_type=jnp.float32)
                resid[span, cols] = (resid[span, cols].astype(jnp.float32) + picked).astype(jnp.bfloat16)

        for quarter in range(8):
            rows_here = pl.ds(pl.multiple_of(block * 512 + quarter * 64, 64), 64)
            widened = resid[rows_here, :].astype(jnp.float32)
            inv_rms = lax.rsqrt(jnp.mean(widened * widened, axis=-1, keepdims=True) + EPSILON)
            normed[rows_here, :] = (widened * inv_rms * gain_ref[...]).astype(jnp.bfloat16)
        for result in results(block):
            result.start()

    @pl.loop(0, rows // 512)
    def _(block):
        for result in results(block):
            result.wait()


def finish_rows(more, cols, gain, head, extra, pieces):
    rows = cols.shape[0]
    width = head.shape[1]
    vmem = pl.BlockSpec(memory_space=pltpu.VMEM)
    hbm = pl.BlockSpec(memory_space=pl.ANY)
    shape = jax.ShapeDtypeStruct((rows, width), jnp.bfloat16)
    dma = pltpu.SemaphoreType.DMA
    return pl.pallas_call(
        functools.partial(finish_kernel, len(pieces)),
        out_shape=(shape, shape),
        in_specs=[pl.BlockSpec(memory_space=pltpu.SMEM), vmem, vmem, hbm, hbm] + [hbm] * len(pieces),
        out_specs=(hbm, hbm),
        scratch_shapes=[
            pltpu.VMEM((HEAD_ROWS + TAIL_ROWS, width), jnp.bfloat16),
            pltpu.VMEM((len(pieces) // 3, 2) + pieces[0].shape, jnp.bfloat16),
            pltpu.VMEM(extra.shape, jnp.bfloat16),
            pltpu.VMEM((rows, width), jnp.bfloat16),
            pltpu.VMEM((rows, width), jnp.bfloat16),
            dma((len(pieces) + 2,)), dma((2,)),
        ],
        compiler_params=pltpu.CompilerParams(vmem_limit_bytes=67_043_328),
        cost_estimate=pl.CostEstimate(flops=2 * rows * width * (HEAD_ROWS + TAIL_ROWS), bytes_accessed=16_000_000, transcendentals=0),
        name="finish_rows",
    )(more, cols, gain, head, extra, *pieces)


def heads_kernel(rows, normed_hbm, cos_ref, sin_ref, wq_hbm, wk_hbm, wv_hbm, q_out, k_out, v_out,
                 wq, wk, wv, normed, q_stage, kv_stage, w_sem, q_send, q_recv, kv_send, kv_recv,
                 own_recv, fwd_send, fwd_recv, keep_sem):
    group = lax.axis_index("dp")
    me = lax.axis_index("tp")
    core = lax.rem(me, 2)
    chip = me // 2
    partner = me + 1 - 2 * core
    kv_outs = (k_out, v_out)
    tiles = rows // SEND_ROWS
    half = HEAD_DIM // 2

    loads = [pltpu.make_async_copy(src, dst, w_sem.at[n]) for n, (src, dst) in enumerate(((normed_hbm, normed), (wk_hbm, wk), (wv_hbm, wv), (wq_hbm, wq)))]
    for load in loads:
        load.start()

    barrier = pltpu.get_barrier_semaphore()
    for step in range(1, 2 * CHIPS):
        pl.semaphore_signal(barrier, inc=1, device_id=(group, lax.rem(me + step, 2 * CHIPS)), device_id_type=MESH_IDS)

    pl.semaphore_wait(barrier, 2 * CHIPS - 1)
    for load in loads:
        load.wait()

    def block(source, tile):
        return pl.ds(pl.multiple_of(source * rows + tile * SEND_ROWS, SEND_ROWS), SEND_ROWS)

    def whole(source):
        return pl.ds(pl.multiple_of(source * rows, rows), rows)

    def remote(src, dst, send, recv, device):
        return pltpu.make_async_remote_copy(src_ref=src, dst_ref=dst, send_sem=send, recv_sem=recv, device_id=(group, device), device_id_type=MESH_IDS)

    def rotated(linear, span, factor):
        front = linear[:, :half]
        back = linear[:, half:]
        cosines = cos_ref[span, :]
        sines = sin_ref[span, :]
        return jnp.concatenate([((front * cosines - back * sines) * factor).astype(jnp.bfloat16), ((back * cosines + front * sines) * factor).astype(jnp.bfloat16)], axis=-1)

    @pl.loop(0, CHIPS * tiles)
    def _(turn):
        offset = lax.rem(turn // tiles + 1, CHIPS)
        tile = lax.rem(turn, tiles)
        there = lax.rem(chip + offset, CHIPS)
        columns = pl.ds(pl.multiple_of(there * HEAD_DIM, HEAD_DIM), HEAD_DIM)
        sent = pl.ds(pl.multiple_of(tile * SEND_ROWS, SEND_ROWS), SEND_ROWS)

        @pl.loop(0, SEND_ROWS // 256)
        def _(part):
            span = pl.ds(pl.multiple_of(tile * SEND_ROWS + part * 256, 256), 256)
            lhs = normed[span, :]

            def linear(weight):
                return jnp.dot(lhs, weight, preferred_element_type=jnp.float32).astype(jnp.bfloat16)

            kv_stage[0, there, span, :] = rotated(linear(wk[:, columns]).astype(jnp.float32), span, 1.0)
            kv_stage[1, there, span, :] = linear(wv[:, columns])
            for side in range(2):
                q_stage[2 * there + side, span, :] = rotated(linear(wq[2 * there + side]).astype(jnp.float32), span, HEAD_DIM ** -0.5)

        @pl.when(offset != 0)
        def _():
            for side in range(2):
                remote(kv_stage.at[side, there, sent, :], kv_outs[side].at[block(me, tile), :], kv_send.at[offset, side], kv_recv.at[offset, core, tile], 2 * there + side).start()
            for side in range(2):
                remote(q_stage.at[2 * there + side, sent, :], q_out.at[block(me, tile), :], q_send.at[offset, side], q_recv.at[offset, core], 2 * there + side).start()

    for side in range(2):
        remote(kv_stage.at[side, chip], kv_outs[side].at[whole(me), :], kv_send.at[0, side], own_recv.at[side], partner).start()
    remote(q_stage.at[partner], q_out.at[whole(me), :], q_send.at[0, 0], q_recv.at[0, 0], partner).start()
    keeps = [pltpu.make_async_copy(q_stage.at[me], q_out.at[whole(me), :], keep_sem.at[0])]
    for side in range(2):
        keeps.append(pltpu.make_async_copy(kv_stage.at[side, chip], kv_outs[side].at[whole(me), :], keep_sem.at[1 + side]))
    for keep in keeps:
        keep.start()

    def forward(mine_out, other_out):
        for tile in range(tiles):
            for offset in range(1, CHIPS):
                for side in range(2):
                    source = 2 * lax.rem(chip + CHIPS - offset, CHIPS) + side
                    region = mine_out.at[block(source, tile), :]
                    remote(region, region, kv_send.at[offset, side], kv_recv.at[offset, side, tile], partner).wait_recv()
                    remote(region, region, fwd_send.at[offset, side], fwd_recv.at[offset, side], partner).start()
        for offset in range(1, CHIPS):
            for side in range(2):
                source = 2 * lax.rem(chip + CHIPS - offset, CHIPS) + side
                mine = mine_out.at[whole(source), :]
                remote(mine, mine, fwd_send.at[offset, side], fwd_recv.at[offset, side], partner).wait_send()
                other = other_out.at[whole(source), :]
                remote(other, other, fwd_send.at[offset, side], fwd_recv.at[offset, side], partner).wait_recv()

    for kind in range(2):
        @pl.when(core == kind)
        def _():
            forward(kv_outs[kind], kv_outs[1 - kind])

    for keep in keeps:
        keep.wait()
    for offset in range(1, CHIPS):
        there = lax.rem(chip + offset, CHIPS)
        for side in range(2):
            source = 2 * lax.rem(chip + CHIPS - offset, CHIPS) + side
            remote(kv_stage.at[side, there], kv_outs[side].at[whole(me), :], kv_send.at[offset, side], own_recv.at[side], partner).wait_send()
            remote(q_stage.at[2 * there + side], q_out.at[whole(source), :], q_send.at[offset, side], q_recv.at[offset, side], partner).wait()
    for side in range(2):
        remote(kv_stage.at[side, chip], kv_outs[side].at[whole(partner), :], kv_send.at[0, side], own_recv.at[side], partner).wait()
    remote(q_stage.at[partner], q_out.at[whole(partner), :], q_send.at[0, 0], q_recv.at[0, 0], partner).wait()


def project_heads(normed, cosines, sines, wq_all, w_key, w_value):
    rows, width = normed.shape
    heads = wq_all.shape[0]
    tokens = rows * heads
    tiles = rows // SEND_ROWS
    vmem = pl.BlockSpec(memory_space=pltpu.VMEM)
    anywhere = pl.BlockSpec(memory_space=pl.ANY)
    dma = pltpu.SemaphoreType.DMA
    return pl.pallas_call(
        functools.partial(heads_kernel, rows),
        out_shape=(jax.ShapeDtypeStruct((tokens, HEAD_DIM), jnp.bfloat16),) * 3,
        in_specs=[anywhere, vmem, vmem, anywhere, anywhere, anywhere],
        out_specs=(anywhere,) * 3,
        scratch_shapes=[
            pltpu.VMEM(wq_all.shape, jnp.bfloat16),
            pltpu.VMEM(w_key.shape, jnp.bfloat16),
            pltpu.VMEM(w_value.shape, jnp.bfloat16),
            pltpu.VMEM((rows, width), jnp.bfloat16),
            pltpu.VMEM((heads, rows, HEAD_DIM), jnp.bfloat16),
            pltpu.VMEM((2, CHIPS, rows, HEAD_DIM), jnp.bfloat16),
            dma((4,)),
            dma((CHIPS, 2)), dma((CHIPS, 2)),
            dma((CHIPS, 2)), dma((CHIPS, 2, tiles)),
            dma((2,)),
            dma((CHIPS, 2)), dma((CHIPS, 2)),
            dma((3,)),
        ],
        compiler_params=pltpu.CompilerParams(collective_id=0, has_side_effects=True, vmem_limit_bytes=67_043_328),
        cost_estimate=pl.CostEstimate(flops=2 * rows * width * 4096, bytes_accessed=40_000_000, transcendentals=0),
        name="project_heads",
    )(normed, cosines, sines, wq_all, w_key, w_value)


def solution(mesh):
    group_size = mesh.shape["tp"]

    def exchange(rows, bit):
        return lax.ppermute(rows, "tp", [(i, i ^ bit) for i in range(group_size)])

    def pass_head(values, pairs, after=None):
        got = lax.ppermute(values, "tp", pairs)
        if after is not None:
            got, _ = lax.optimization_barrier((got, after))
        return jnp.where(lax.axis_index("tp") == pairs[0][1], got, values)

    def share_head(rows):
        half = rows.shape[0] // 2
        first = pass_head(rows[:half], [(0, 2)])
        second = pass_head(rows[half:], [(0, 4)])
        first = pass_head(first, [(2, 6)])
        second = pass_head(second, [(4, 6)])
        return first, second

    def share_head_back(first, second, after):
        first = pass_head(first, [(6, 4)], after)
        second = pass_head(second, [(6, 2)], after)
        both = jnp.concatenate([first, second], axis=0)
        other = lax.ppermute(both, "tp", [(0, 1), (2, 3), (4, 5), (6, 7)])
        return jnp.where(lax.axis_index("tp") % 2 == 1, other, both)

    def local_body(token_ids, positions, table_rows, norm_scale, w_query, w_key, w_value):
        dev_index = lax.axis_index("tp")
        vocab_rows, model_width = table_rows.shape
        wq_all = lax.all_gather(w_query, "tp", axis=0)
        head_halves = share_head(table_rows[:HEAD_ROWS])
        tokens = token_ids.shape[0]
        block_rows = tokens // group_size
        extra_rows = block_rows - TAIL_ROWS
        chunk_rows = TAIL_ROWS // CHUNKS
        half = chunk_rows // 2

        blocks = token_ids.reshape(group_size, block_rows)
        in_tail = blocks >= HEAD_ROWS
        earlier = (lax.broadcasted_iota(jnp.int32, (block_rows, block_rows), 0) < lax.broadcasted_iota(jnp.int32, (block_rows, block_rows), 1)).astype(jnp.bfloat16)
        ranks = jnp.dot(in_tail.astype(jnp.bfloat16), earlier, preferred_element_type=jnp.float32).astype(jnp.int32)
        ranks = jnp.where(in_tail, ranks, -1)

        def ranked_ids(first, count):
            wanted = lax.broadcasted_iota(jnp.int32, (group_size, block_rows, count), 2) + first
            ids = jnp.sum(jnp.where(ranks[:, :, None] == wanted, blocks[:, :, None] + 1, 0), axis=1) - 1
            local = ids - dev_index * vocab_rows
            return jnp.where((ids >= 0) & (local >= 0) & (local < vocab_rows), local, -1)

        most = jnp.max(jnp.sum(in_tail.astype(jnp.int32), axis=1))
        over = (most > TAIL_ROWS).astype(jnp.int32)

        def arrange(values):
            view = values.reshape(2, 2, 2, CHUNKS, 2, half)
            for axis, bit in ((0, 4), (1, 2), (2, 1)):
                flag = (dev_index // bit) % 2 == 1
                view = jnp.where(flag, jnp.flip(view, axis), view)
            halves = view.transpose(3, 2, 4, 0, 1, 5)
            first = halves[:, :, 0].transpose(0, 1, 3, 2, 4)
            second = halves[:, :, 1]
            return jnp.stack([first, second], axis=2).reshape(CHUNKS, 2, 4 * chunk_rows)

        call_rows = 4 * chunk_rows
        ids = arrange(ranked_ids(0, TAIL_ROWS)).reshape(-1, TILE)
        owned = ids >= 0
        before = (lax.broadcasted_iota(jnp.int32, (TILE, TILE), 0) < lax.broadcasted_iota(jnp.int32, (TILE, TILE), 1)).astype(jnp.bfloat16)
        slots = jnp.dot(owned.astype(jnp.bfloat16), before, preferred_element_type=jnp.float32).astype(jnp.int32)
        slots = jnp.where(owned, slots, -1)
        wanted_slot = lax.broadcasted_iota(jnp.int32, (ids.shape[0], TILE, TILE), 2)
        pair_ids = jnp.sum(jnp.where(slots[:, :, None] == wanted_slot, (ids // 2)[:, :, None] * 2, 0), axis=1).reshape(-1)
        cols = jnp.where(owned, 2 * slots + ids % 2, -1).astype(jnp.float32)[:, None, :]
        counts = jnp.sum(owned.astype(jnp.int32), axis=-1)

        def gather(chunk, side, after):
            return gather_rows((2 * chunk + side) * call_rows, call_rows, pair_ids, counts, cols, table_rows, after)

        pieces = []
        after, late, late_next = [], [], []
        for chunk in range(CHUNKS):
            other = gather(chunk, 1, after + late)
            got = exchange(other, 1)
            mine = gather(chunk, 0, [other] + ([wq_all] if chunk == CHUNKS - 1 else []))
            after, late = [], late_next
            late_next = []
            spans = []
            for part in range(2):
                first_row = part * 4 * half
                spans += [slice(first_row, first_row + half), slice(first_row + half, first_row + 2 * half), slice(first_row + 2 * half, first_row + 4 * half)]
            both = lax.optimization_barrier([mine[span] + got[span] for span in spans])
            for part, bits in ((0, (2, 4)), (1, (4, 2))):
                kept, near, sent = both[3 * part:3 * part + 3]
                back = exchange(sent, bits[0])
                near_send = near + back[half:]
                back2 = exchange(near_send, bits[1])
                after.append(sent)
                late_next.append(near_send)
                pieces += [kept, back, back2]

        head = share_head_back(*head_halves, pieces[5])

        def second_exchange(rows):
            ids = ranked_ids(TAIL_ROWS, extra_rows).reshape(-1)
            normalizer = jnp.asarray(math.sqrt(model_width), dtype=jnp.bfloat16)
            picked = jnp.take(rows, jnp.maximum(ids, 0), axis=0, mode="clip") * normalizer
            partial = jnp.where(ids[:, None] >= 0, picked, jnp.zeros((), jnp.bfloat16))
            return lax.psum_scatter(partial, "tp", scatter_dimension=0, tiled=True)

        def no_exchange(rows):
            return jnp.zeros((extra_rows, model_width), jnp.bfloat16)

        over, _ = lax.optimization_barrier((over, pieces[2]))
        more = lax.pmax(over, "dp")
        asked, _ = lax.optimization_barrier((more, pieces[5]))
        extra = lax.cond(asked > 0, second_exchange, no_exchange, table_rows)
        places = jnp.where(in_tail, HEAD_ROWS + ranks, blocks)
        own_places = lax.dynamic_index_in_dim(places, dev_index, 0, keepdims=False)
        residual, normed = finish_rows(more.reshape(1), own_places[:, None], (1.0 + norm_scale)[None, :], head, extra, pieces)
        own = lax.dynamic_slice_in_dim(positions, dev_index * block_rows, block_rows)
        cosines, sines = rope_tables(own)
        outs = project_heads(normed, cosines, sines, wq_all, w_key, w_value)
        return (residual,) + tuple(out[:, None, :] for out in outs)

    head_spec = P("dp", "tp", None)
    return jax.shard_map(local_body, mesh=mesh, in_specs=(P("dp"), P("dp"), P("tp", None), P(), P(None, "tp"), P(), P()), out_specs=(P(("dp", "tp"), None), head_spec, head_spec, head_spec), check_vma=False)
```

```python
import functools
import math
import jax
import jax.numpy as jnp
from jax import lax
from jax.experimental import pallas as pl
from jax.experimental.pallas import tpu as pltpu
from jax.sharding import PartitionSpec as P

HEAD_DIM = 256
EPSILON = 1e-6
ROPE_BASE = 10000.0
TILE = 128
CHUNKS = 2
HEAD_ROWS = 640
TAIL_ROWS = 640
SEND_ROWS = 512
CHIPS = 4
MESH_IDS = pl.DeviceIdType.MESH


def rope_tables(positions):
    inv_freq = ROPE_BASE ** (-jnp.arange(0, HEAD_DIM, 2, dtype=jnp.float32) / HEAD_DIM)
    angles = positions.astype(jnp.float32)[:, None] * inv_freq[None, :]
    return jnp.cos(angles), jnp.sin(angles)


def gather_kernel(base, tiles, width, pair_ids, counts, cols_ref, table_ref, *rest):
    out_ref, pairs, sems = rest[-3:]
    step = pl.program_id(0)
    normalizer = jnp.asarray(math.sqrt(width), dtype=jnp.bfloat16)

    def start(tile, slot):
        count = counts[base + tile]

        def copy(group, row):
            src = pair_ids[(base + tile) * TILE + group * 8 + row]
            pltpu.make_async_copy(table_ref.at[pl.ds(pl.multiple_of(src, 2), 2), :], pairs.at[slot, group, pl.ds(2 * row, 2), :], sems.at[slot]).start()

        @pl.loop(0, count // 8)
        def _(group):
            for row in range(8):
                copy(group, row)

        for row in range(7):
            @pl.when(row < lax.rem(count, 8))
            def _():
                copy(count // 8, row)

    def wait(tile, slot):
        count = counts[base + tile]
        size = TILE // 8
        while size:
            @pl.when((count // (8 * size)) % 2 == 1)
            def _():
                pltpu.make_async_copy(pairs.at[slot, pl.ds(0, size)], pairs.at[slot, pl.ds(0, size)], sems.at[slot]).wait()

            size //= 2
        for size in (1, 2, 4):
            @pl.when((count // size) % 2 == 1)
            def _():
                pltpu.make_async_copy(table_ref.at[pl.ds(0, 2 * size), :], pairs.at[slot, 0, pl.ds(0, 2 * size), :], sems.at[slot]).wait()

    @pl.when(step == 0)
    def _():
        pairs[...] = jnp.zeros_like(pairs)
        start(0, 0)
        start(1, 1)

    slot = lax.rem(step, 3)

    @pl.when(step + 2 < tiles)
    def _():
        start(step + 2, lax.rem(step + 2, 3))

    wait(step, slot)
    lanes = lax.broadcasted_iota(jnp.int32, (TILE, 2 * TILE), 1).astype(jnp.float32)
    wanted = jnp.broadcast_to(cols_ref[base + step], (TILE, TILE)).T
    select = jnp.where(lanes == jnp.concatenate([wanted, wanted], axis=1), normalizer, jnp.zeros((), jnp.bfloat16))
    for piece in range(width // 256):
        cols = pl.ds(piece * 256, 256)
        picked = jnp.dot(select, pairs[slot, :, :, cols].reshape(2 * TILE, 256), preferred_element_type=jnp.float32)
        out_ref[:, cols] = picked.astype(jnp.bfloat16)


def gather_rows(base, count, pair_ids, counts, cols, table_rows, after):
    width = table_rows.shape[1]
    tiles = count // TILE
    base = base // TILE
    anywhere = pl.BlockSpec(memory_space=pl.ANY)
    grid_spec = pltpu.PrefetchScalarGridSpec(
        num_scalar_prefetch=2,
        grid=(tiles,),
        in_specs=[pl.BlockSpec(cols.shape, lambda i, *_: (0, 0, 0)), anywhere] + [anywhere] * len(after),
        out_specs=pl.BlockSpec((TILE, width), lambda i, *_: (i, 0)),
        scratch_shapes=[pltpu.VMEM((3, TILE // 8, 16, width), jnp.bfloat16), pltpu.SemaphoreType.DMA((3,))],
    )
    return pl.pallas_call(
        functools.partial(gather_kernel, base, tiles, width),
        grid_spec=grid_spec,
        out_shape=jax.ShapeDtypeStruct((count, width), jnp.bfloat16),
        compiler_params=pltpu.CompilerParams(dimension_semantics=("arbitrary",)),
        cost_estimate=pl.CostEstimate(flops=count * 20_000_000, bytes_accessed=count * width * 6, transcendentals=0),
        name="gather_rows",
    )(pair_ids, counts, cols, table_rows, *after)


def finish_kernel(pieces, more, cols_ref, gain_ref, head_hbm, extra_hbm, *refs):
    piece_refs, (resid_hbm, normed_hbm, source, parts, extra, resid, normed, in_sems, out_sems) = refs[:pieces], refs[pieces:]
    rows, width = resid.shape
    part = TAIL_ROWS // (pieces // 3)
    known = HEAD_ROWS + TAIL_ROWS
    normalizer = jnp.asarray(math.sqrt(width), dtype=jnp.bfloat16)
    one = jnp.ones((), jnp.bfloat16)
    zero = jnp.zeros((), jnp.bfloat16)
    head_copy = pltpu.make_async_copy(head_hbm, source.at[pl.ds(0, HEAD_ROWS), :], in_sems.at[pieces])
    extra_copy = pltpu.make_async_copy(extra_hbm, extra, in_sems.at[pieces + 1])
    copies = []
    for index, ref in enumerate(piece_refs):
        there = source.at[pl.ds(HEAD_ROWS + index // 3 * part, part), :] if index % 3 == 0 else parts.at[index // 3, index % 3 - 1]
        copies.append(pltpu.make_async_copy(ref.at[pl.ds(0, part), :], there, in_sems.at[index]))
    head_copy.start()
    for copy in copies:
        copy.start()
    for copy in copies:
        copy.wait()
    for index in range(pieces // 3):
        span = pl.ds(HEAD_ROWS + index * part, part)
        source[span, :] = source[span, :] + parts[index, 0] + parts[index, 1]
    head_copy.wait()

    @pl.when(more[0] > 0)
    def _():
        extra_copy.start()
        extra_copy.wait()

    def results(block):
        span = pl.ds(pl.multiple_of(block * 256, 256), 256)
        return (pltpu.make_async_copy(resid.at[span, :], resid_hbm.at[span, :], out_sems.at[0]),
                pltpu.make_async_copy(normed.at[span, :], normed_hbm.at[span, :], out_sems.at[1]))

    @pl.loop(0, rows // 256)
    def _(block):
        span = pl.ds(pl.multiple_of(block * 256, 256), 256)
        lanes = lax.broadcasted_iota(jnp.int32, (256, known), 1)
        value = jnp.where(lax.broadcasted_iota(jnp.int32, (1, known), 1) < HEAD_ROWS, normalizer, one)
        select = jnp.where(lanes == cols_ref[span, :], jnp.broadcast_to(value, (256, known)), zero)
        for piece in range(width // 256):
            cols = pl.ds(piece * 256, 256)
            resid[span, cols] = jnp.dot(select, source[:, cols], preferred_element_type=jnp.float32).astype(jnp.bfloat16)

        @pl.when(more[0] > 0)
        def _():
            places = lax.broadcasted_iota(jnp.int32, (256, extra.shape[0]), 1) + known
            from_extra = jnp.where(places == cols_ref[span, :], one, zero)
            for piece in range(width // 256):
                cols = pl.ds(piece * 256, 256)
                picked = jnp.dot(from_extra, extra[:, cols], preferred_element_type=jnp.float32)
                resid[span, cols] = (resid[span, cols].astype(jnp.float32) + picked).astype(jnp.bfloat16)

        for quarter in range(4):
            rows_here = pl.ds(pl.multiple_of(block * 256 + quarter * 64, 64), 64)
            widened = resid[rows_here, :].astype(jnp.float32)
            inv_rms = lax.rsqrt(jnp.mean(widened * widened, axis=-1, keepdims=True) + EPSILON)
            normed[rows_here, :] = (widened * inv_rms * gain_ref[...]).astype(jnp.bfloat16)
        for result in results(block):
            result.start()

    @pl.loop(0, rows // 256)
    def _(block):
        for result in results(block):
            result.wait()


def finish_rows(more, cols, gain, head, extra, pieces):
    rows = cols.shape[0]
    width = head.shape[1]
    vmem = pl.BlockSpec(memory_space=pltpu.VMEM)
    hbm = pl.BlockSpec(memory_space=pl.ANY)
    shape = jax.ShapeDtypeStruct((rows, width), jnp.bfloat16)
    dma = pltpu.SemaphoreType.DMA
    return pl.pallas_call(
        functools.partial(finish_kernel, len(pieces)),
        out_shape=(shape, shape),
        in_specs=[pl.BlockSpec(memory_space=pltpu.SMEM), vmem, vmem, hbm, hbm] + [hbm] * len(pieces),
        out_specs=(hbm, hbm),
        scratch_shapes=[
            pltpu.VMEM((HEAD_ROWS + TAIL_ROWS, width), jnp.bfloat16),
            pltpu.VMEM((len(pieces) // 3, 2) + pieces[0].shape, jnp.bfloat16),
            pltpu.VMEM(extra.shape, jnp.bfloat16),
            pltpu.VMEM((rows, width), jnp.bfloat16),
            pltpu.VMEM((rows, width), jnp.bfloat16),
            dma((len(pieces) + 2,)), dma((2,)),
        ],
        compiler_params=pltpu.CompilerParams(vmem_limit_bytes=67_043_328),
        cost_estimate=pl.CostEstimate(flops=2 * rows * width * (HEAD_ROWS + TAIL_ROWS), bytes_accessed=16_000_000, transcendentals=0),
        name="finish_rows",
    )(more, cols, gain, head, extra, *pieces)


def heads_kernel(rows, normed_hbm, cos_ref, sin_ref, wq_mine, wq_far, wq_near, wk_hbm, wv_hbm, q_out, kv_out,
                 wq, wk, wv, normed, q_stage, kv_stage, w_sem, q_send, q_recv, kv_send, kv_recv,
                 own_recv, fwd_send, fwd_recv, keep_sem):
    group = lax.axis_index("dp")
    me = lax.axis_index("tp")
    core = lax.rem(me, 2)
    chip = me // 2
    partner = me + 1 - 2 * core
    kv_outs = (kv_out.at[0], kv_out.at[1])
    tiles = rows // SEND_ROWS
    half = HEAD_DIM // 2

    depth = wq_mine.shape[1]
    own_depth = pl.ds(pl.multiple_of(group * depth, depth), depth)
    far_depth = pl.ds(pl.multiple_of((1 - group) * depth, depth), depth)
    sources = ((normed_hbm, normed), (wk_hbm, wk), (wv_hbm, wv), (wq_mine, wq.at[:, own_depth, :]),
               (wq_far, wq.at[pl.ds(core * CHIPS, CHIPS), far_depth, :]), (wq_near, wq.at[pl.ds((1 - core) * CHIPS, CHIPS), far_depth, :]))
    loads = [pltpu.make_async_copy(src, dst, w_sem.at[n]) for n, (src, dst) in enumerate(sources)]
    for load in loads:
        load.start()

    barrier = pltpu.get_barrier_semaphore()
    for step in range(1, 2 * CHIPS):
        pl.semaphore_signal(barrier, inc=1, device_id=(group, lax.rem(me + step, 2 * CHIPS)), device_id_type=MESH_IDS)

    pl.semaphore_wait(barrier, 2 * CHIPS - 1)
    for load in loads:
        load.wait()

    def block(source, tile):
        return pl.ds(pl.multiple_of(source * rows + tile * SEND_ROWS, SEND_ROWS), SEND_ROWS)

    def whole(source):
        return pl.ds(pl.multiple_of(source * rows, rows), rows)

    def remote(src, dst, send, recv, device):
        return pltpu.make_async_remote_copy(src_ref=src, dst_ref=dst, send_sem=send, recv_sem=recv, device_id=(group, device), device_id_type=MESH_IDS)

    def rotated(linear, span, factor):
        front = linear[:, :half]
        back = linear[:, half:]
        cosines = cos_ref[span, :]
        sines = sin_ref[span, :]
        return jnp.concatenate([((front * cosines - back * sines) * factor).astype(jnp.bfloat16), ((back * cosines + front * sines) * factor).astype(jnp.bfloat16)], axis=-1)

    @pl.loop(0, CHIPS * tiles)
    def _(turn):
        offset = lax.rem(turn // tiles + 1, CHIPS)
        tile = lax.rem(turn, tiles)
        there = lax.rem(chip + offset, CHIPS)
        columns = pl.ds(pl.multiple_of(there * HEAD_DIM, HEAD_DIM), HEAD_DIM)
        sent = pl.ds(pl.multiple_of(tile * SEND_ROWS, SEND_ROWS), SEND_ROWS)

        @pl.loop(0, SEND_ROWS // 256)
        def _(part):
            span = pl.ds(pl.multiple_of(tile * SEND_ROWS + part * 256, 256), 256)
            lhs = normed[span, :]

            def linear(weight):
                return jnp.dot(lhs, weight, preferred_element_type=jnp.float32).astype(jnp.bfloat16)

            kv_stage[0, there, span, :] = rotated(linear(wk[:, columns]).astype(jnp.float32), span, 1.0)
            kv_stage[1, there, span, :] = linear(wv[:, columns])
            for side in range(2):
                q_stage[2 * there + side, span, :] = rotated(linear(wq[2 * there + side]).astype(jnp.float32), span, HEAD_DIM ** -0.5)

        @pl.when(offset != 0)
        def _():
            for side in range(2):
                remote(kv_stage.at[side, there, sent, :], kv_outs[side].at[block(me, tile), :], kv_send.at[offset, side], kv_recv.at[offset, core, tile], 2 * there + side).start()
            for side in range(2):
                remote(q_stage.at[2 * there + side, sent, :], q_out.at[block(me, tile), :], q_send.at[offset, side], q_recv.at[offset, core], 2 * there + side).start()

    for side in range(2):
        remote(kv_stage.at[side, chip], kv_outs[side].at[whole(me), :], kv_send.at[0, side], own_recv.at[side], partner).start()
    remote(q_stage.at[partner], q_out.at[whole(me), :], q_send.at[0, 0], q_recv.at[0, 0], partner).start()
    keeps = [pltpu.make_async_copy(q_stage.at[me], q_out.at[whole(me), :], keep_sem.at[0])]
    for side in range(2):
        keeps.append(pltpu.make_async_copy(kv_stage.at[side, chip], kv_outs[side].at[whole(me), :], keep_sem.at[1 + side]))
    for keep in keeps:
        keep.start()

    def forward(mine_out, other_out):
        for tile in range(tiles):
            for offset in range(1, CHIPS):
                for side in range(2):
                    source = 2 * lax.rem(chip + CHIPS - offset, CHIPS) + side
                    region = mine_out.at[block(source, tile), :]
                    remote(region, region, kv_send.at[offset, side], kv_recv.at[offset, side, tile], partner).wait_recv()
                    remote(region, region, fwd_send.at[offset, side], fwd_recv.at[offset, side], partner).start()
        for offset in range(1, CHIPS):
            for side in range(2):
                source = 2 * lax.rem(chip + CHIPS - offset, CHIPS) + side
                mine = mine_out.at[whole(source), :]
                remote(mine, mine, fwd_send.at[offset, side], fwd_recv.at[offset, side], partner).wait_send()
                other = other_out.at[whole(source), :]
                remote(other, other, fwd_send.at[offset, side], fwd_recv.at[offset, side], partner).wait_recv()

    forward(kv_out.at[core], kv_out.at[1 - core])

    for keep in keeps:
        keep.wait()
    for offset in range(1, CHIPS):
        there = lax.rem(chip + offset, CHIPS)
        for side in range(2):
            source = 2 * lax.rem(chip + CHIPS - offset, CHIPS) + side
            remote(kv_stage.at[side, there], kv_outs[side].at[whole(me), :], kv_send.at[offset, side], own_recv.at[side], partner).wait_send()
            remote(q_stage.at[2 * there + side], q_out.at[whole(source), :], q_send.at[offset, side], q_recv.at[offset, side], partner).wait()
    for side in range(2):
        remote(kv_stage.at[side, chip], kv_outs[side].at[whole(partner), :], kv_send.at[0, side], own_recv.at[side], partner).wait()
    remote(q_stage.at[partner], q_out.at[whole(partner), :], q_send.at[0, 0], q_recv.at[0, 0], partner).wait()


def project_heads(normed, cosines, sines, wq_parts, w_key, w_value):
    rows, width = normed.shape
    heads = wq_parts[0].shape[0]
    tokens = rows * heads
    tiles = rows // SEND_ROWS
    vmem = pl.BlockSpec(memory_space=pltpu.VMEM)
    anywhere = pl.BlockSpec(memory_space=pl.ANY)
    dma = pltpu.SemaphoreType.DMA
    return pl.pallas_call(
        functools.partial(heads_kernel, rows),
        out_shape=(jax.ShapeDtypeStruct((tokens, HEAD_DIM), jnp.bfloat16), jax.ShapeDtypeStruct((2, tokens, HEAD_DIM), jnp.bfloat16)),
        in_specs=[anywhere, vmem, vmem] + [anywhere] * 5,
        out_specs=(anywhere, anywhere),
        scratch_shapes=[
            pltpu.VMEM((heads, width, HEAD_DIM), jnp.bfloat16),
            pltpu.VMEM(w_key.shape, jnp.bfloat16),
            pltpu.VMEM(w_value.shape, jnp.bfloat16),
            pltpu.VMEM((rows, width), jnp.bfloat16),
            pltpu.VMEM((heads, rows, HEAD_DIM), jnp.bfloat16),
            pltpu.VMEM((2, CHIPS, rows, HEAD_DIM), jnp.bfloat16),
            dma((6,)),
            dma((CHIPS, 2)), dma((CHIPS, 2)),
            dma((CHIPS, 2)), dma((CHIPS, 2, tiles)),
            dma((2,)),
            dma((CHIPS, 2)), dma((CHIPS, 2)),
            dma((3,)),
        ],
        compiler_params=pltpu.CompilerParams(collective_id=0, has_side_effects=True, vmem_limit_bytes=67_043_328),
        cost_estimate=pl.CostEstimate(flops=2 * rows * width * 4096, bytes_accessed=40_000_000, transcendentals=0),
        name="project_heads",
    )(normed, cosines, sines, *wq_parts, w_key, w_value)


def solution(mesh):
    group_size = mesh.shape["tp"]

    def exchange(rows, bit):
        return lax.ppermute(rows, "tp", [(i, i ^ bit) for i in range(group_size)])

    def pass_head(values, pairs, after=None):
        got = lax.ppermute(values, "tp", pairs)
        if after is not None:
            got, _ = lax.optimization_barrier((got, after))
        return jnp.where(lax.axis_index("tp") == pairs[0][1], got, values)

    def share_head(rows):
        half = rows.shape[0] // 2
        first = pass_head(rows[:half], [(0, 2)])
        second = pass_head(rows[half:], [(0, 4)])
        first = pass_head(first, [(2, 6)])
        second = pass_head(second, [(4, 6)])
        return first, second

    def share_head_back(first, second, after):
        first = pass_head(first, [(6, 4)], after)
        second = pass_head(second, [(6, 2)], after)
        both = jnp.concatenate([first, second], axis=0)
        other = lax.ppermute(both, "tp", [(0, 1), (2, 3), (4, 5), (6, 7)])
        return jnp.where(lax.axis_index("tp") % 2 == 1, other, both)

    def local_body(token_ids, positions, table_rows, norm_scale, w_query, w_key, w_value):
        dev_index = lax.axis_index("tp")
        vocab_rows, model_width = table_rows.shape
        group = lax.axis_index("dp")
        core = dev_index % 2
        part_rows = w_query.shape[0] // 2
        wq_mine = lax.all_gather(lax.dynamic_slice_in_dim(w_query, group * part_rows, part_rows, axis=0), "tp", axis=0)
        wq_far = lax.ppermute(lax.dynamic_slice_in_dim(wq_mine, core * (group_size // 2), group_size // 2, axis=0), "dp", [(0, 1), (1, 0)])
        wq_near = exchange(wq_far, 1)
        head_halves = share_head(table_rows[:HEAD_ROWS])
        tokens = token_ids.shape[0]
        block_rows = tokens // group_size
        extra_rows = block_rows - TAIL_ROWS
        chunk_rows = TAIL_ROWS // CHUNKS
        half = chunk_rows // 2

        blocks = token_ids.reshape(group_size, block_rows)
        in_tail = blocks >= HEAD_ROWS
        earlier = (lax.broadcasted_iota(jnp.int32, (block_rows, block_rows), 0) < lax.broadcasted_iota(jnp.int32, (block_rows, block_rows), 1)).astype(jnp.bfloat16)
        ranks = jnp.dot(in_tail.astype(jnp.bfloat16), earlier, preferred_element_type=jnp.float32).astype(jnp.int32)
        ranks = jnp.where(in_tail, ranks, -1)

        def ranked_ids(first, count):
            wanted = lax.broadcasted_iota(jnp.int32, (group_size, block_rows, count), 2) + first
            ids = jnp.sum(jnp.where(ranks[:, :, None] == wanted, blocks[:, :, None] + 1, 0), axis=1) - 1
            local = ids - dev_index * vocab_rows
            return jnp.where((ids >= 0) & (local >= 0) & (local < vocab_rows), local, -1)

        most = jnp.max(jnp.sum(in_tail.astype(jnp.int32), axis=1))
        over = (most > TAIL_ROWS).astype(jnp.int32)

        def arrange(values):
            view = values.reshape(2, 2, 2, CHUNKS, 2, half)
            for axis, bit in ((0, 4), (1, 2), (2, 1)):
                flag = (dev_index // bit) % 2 == 1
                view = jnp.where(flag, jnp.flip(view, axis), view)
            halves = view.transpose(3, 2, 4, 0, 1, 5)
            first = halves[:, :, 0].transpose(0, 1, 3, 2, 4)
            second = halves[:, :, 1]
            return jnp.stack([first, second], axis=2).reshape(CHUNKS, 2, 4 * chunk_rows)

        call_rows = 4 * chunk_rows
        ids = arrange(ranked_ids(0, TAIL_ROWS)).reshape(-1, TILE)
        owned = ids >= 0
        before = (lax.broadcasted_iota(jnp.int32, (TILE, TILE), 0) < lax.broadcasted_iota(jnp.int32, (TILE, TILE), 1)).astype(jnp.bfloat16)
        slots = jnp.dot(owned.astype(jnp.bfloat16), before, preferred_element_type=jnp.float32).astype(jnp.int32)
        slots = jnp.where(owned, slots, -1)
        wanted_slot = lax.broadcasted_iota(jnp.int32, (ids.shape[0], TILE, TILE), 2)
        pair_ids = jnp.sum(jnp.where(slots[:, :, None] == wanted_slot, (ids // 2)[:, :, None] * 2, 0), axis=1).reshape(-1)
        cols = jnp.where(owned, 2 * slots + ids % 2, -1).astype(jnp.float32)[:, None, :]
        counts = jnp.sum(owned.astype(jnp.int32), axis=-1)

        def gather(chunk, side, after):
            return gather_rows((2 * chunk + side) * call_rows, call_rows, pair_ids, counts, cols, table_rows, after)

        pieces = []
        after, late, late_next = [], [], []
        for chunk in range(CHUNKS):
            other = gather(chunk, 1, after + late + ([wq_mine] if chunk == CHUNKS - 1 else []))
            got = exchange(other, 1)
            mine = gather(chunk, 0, [other])
            after, late = [], late_next
            late_next = []
            spans = []
            for part in range(2):
                first_row = part * 4 * half
                spans += [slice(first_row, first_row + half), slice(first_row + half, first_row + 2 * half), slice(first_row + 2 * half, first_row + 4 * half)]
            both = lax.optimization_barrier([mine[span] + got[span] for span in spans])
            for part, bits in ((0, (2, 4)), (1, (4, 2))):
                kept, near, sent = both[3 * part:3 * part + 3]
                back = exchange(sent, bits[0])
                near_send = near + back[half:]
                back2 = exchange(near_send, bits[1])
                after.append(sent)
                late_next.append(near_send)
                pieces += [kept, back, back2]

        head = share_head_back(*head_halves, pieces[5])

        def second_exchange(rows):
            ids = ranked_ids(TAIL_ROWS, extra_rows).reshape(-1)
            normalizer = jnp.asarray(math.sqrt(model_width), dtype=jnp.bfloat16)
            picked = jnp.take(rows, jnp.maximum(ids, 0), axis=0, mode="clip") * normalizer
            partial = jnp.where(ids[:, None] >= 0, picked, jnp.zeros((), jnp.bfloat16))
            return lax.psum_scatter(partial, "tp", scatter_dimension=0, tiled=True)

        def no_exchange(rows):
            return jnp.zeros((extra_rows, model_width), jnp.bfloat16)

        over, _ = lax.optimization_barrier((over, pieces[2]))
        more = lax.pmax(over, "dp")
        asked, _ = lax.optimization_barrier((more, pieces[5]))
        extra = lax.cond(asked > 0, second_exchange, no_exchange, table_rows)
        places = jnp.where(in_tail, HEAD_ROWS + ranks, blocks)
        own_places = lax.dynamic_index_in_dim(places, dev_index, 0, keepdims=False)
        residual, normed = finish_rows(more.reshape(1), own_places[:, None], (1.0 + norm_scale)[None, :], head, extra, pieces)
        own = lax.dynamic_slice_in_dim(positions, dev_index * block_rows, block_rows)
        cosines, sines = rope_tables(own)
        queries, keys_values = project_heads(normed, cosines, sines, (wq_mine, wq_far, wq_near), w_key, w_value)
        return residual, queries[:, None, :], keys_values[0][:, None, :], keys_values[1][:, None, :]

    head_spec = P("dp", "tp", None)
    return jax.shard_map(local_body, mesh=mesh, in_specs=(P("dp"), P("dp"), P("tp", None), P(), P(None, "tp"), P(), P()), out_specs=(P(("dp", "tp"), None), head_spec, head_spec, head_spec), check_vma=False)
```

```python
import functools
import math
import jax
import jax.numpy as jnp
from jax import lax
from jax.experimental import pallas as pl
from jax.experimental.pallas import tpu as pltpu
from jax.sharding import PartitionSpec as P

HEAD_DIM = 256
EPSILON = 1e-6
ROPE_BASE = 10000.0
TILE = 128
SLOTS = 6
CHUNKS = 2
HEAD_ROWS = 640
TAIL_ROWS = 640
SEND_ROWS = 512
CHIPS = 4
MESH_IDS = pl.DeviceIdType.MESH


def rope_tables(positions):
    inv_freq = ROPE_BASE ** (-jnp.arange(0, HEAD_DIM, 2, dtype=jnp.float32) / HEAD_DIM)
    angles = positions.astype(jnp.float32)[:, None] * inv_freq[None, :]
    return jnp.cos(angles), jnp.sin(angles)


def gather_kernel(base, tiles, width, pair_ids, counts, cols_ref, table_ref, *rest):
    out_ref, pairs, sems = rest[-3:]
    step = pl.program_id(0)
    normalizer = jnp.asarray(math.sqrt(width), dtype=jnp.bfloat16)

    def start(tile, slot):
        count = counts[base + tile]

        def copy(group, row):
            src = pair_ids[(base + tile) * TILE + group * 8 + row]
            pltpu.make_async_copy(table_ref.at[pl.ds(pl.multiple_of(src, 2), 2), :], pairs.at[slot, group, pl.ds(2 * row, 2), :], sems.at[slot]).start()

        @pl.loop(0, count // 8)
        def _(group):
            for row in range(8):
                copy(group, row)

        for row in range(7):
            @pl.when(row < lax.rem(count, 8))
            def _():
                copy(count // 8, row)

    def wait(tile, slot):
        count = counts[base + tile]
        size = TILE // 8
        while size:
            @pl.when((count // (8 * size)) % 2 == 1)
            def _():
                pltpu.make_async_copy(pairs.at[slot, pl.ds(0, size)], pairs.at[slot, pl.ds(0, size)], sems.at[slot]).wait()

            size //= 2
        for size in (1, 2, 4):
            @pl.when((count // size) % 2 == 1)
            def _():
                pltpu.make_async_copy(table_ref.at[pl.ds(0, 2 * size), :], pairs.at[slot, 0, pl.ds(0, 2 * size), :], sems.at[slot]).wait()

    @pl.when(step == 0)
    def _():
        pairs[...] = jnp.zeros_like(pairs)

        @pl.loop(0, min(SLOTS - 1, tiles))
        def _(tile):
            start(tile, tile)

    slot = lax.rem(step, SLOTS)

    @pl.when(step + SLOTS - 1 < tiles)
    def _():
        start(step + SLOTS - 1, lax.rem(step + SLOTS - 1, SLOTS))

    wait(step, slot)
    lanes = lax.broadcasted_iota(jnp.int32, (TILE, 2 * TILE), 1).astype(jnp.float32)
    wanted = jnp.broadcast_to(cols_ref[base + step], (TILE, TILE)).T
    select = jnp.where(lanes == jnp.concatenate([wanted, wanted], axis=1), normalizer, jnp.zeros((), jnp.bfloat16))
    for piece in range(width // 256):
        cols = pl.ds(piece * 256, 256)
        picked = jnp.dot(select, pairs[slot, :, :, cols].reshape(2 * TILE, 256), preferred_element_type=jnp.float32)
        out_ref[:, cols] = picked.astype(jnp.bfloat16)


def gather_rows(base, count, pair_ids, counts, cols, table_rows, after):
    width = table_rows.shape[1]
    tiles = count // TILE
    base = base // TILE
    anywhere = pl.BlockSpec(memory_space=pl.ANY)
    grid_spec = pltpu.PrefetchScalarGridSpec(
        num_scalar_prefetch=2,
        grid=(tiles,),
        in_specs=[pl.BlockSpec(cols.shape, lambda i, *_: (0, 0, 0)), anywhere] + [anywhere] * len(after),
        out_specs=pl.BlockSpec((TILE, width), lambda i, *_: (i, 0)),
        scratch_shapes=[pltpu.VMEM((SLOTS, TILE // 8, 16, width), jnp.bfloat16), pltpu.SemaphoreType.DMA((SLOTS,))],
    )
    return pl.pallas_call(
        functools.partial(gather_kernel, base, tiles, width),
        grid_spec=grid_spec,
        out_shape=jax.ShapeDtypeStruct((count, width), jnp.bfloat16),
        compiler_params=pltpu.CompilerParams(dimension_semantics=("arbitrary",)),
        cost_estimate=pl.CostEstimate(flops=count * 20_000_000, bytes_accessed=count * width * 6, transcendentals=0),
        name="gather_rows",
    )(pair_ids, counts, cols, table_rows, *after)


def rows_kernel(pieces, head_rows, first_place, last, more, cols_ref, gain_ref, base_hbm, extra_hbm, *refs):
    piece_refs, refs = refs[:pieces], refs[pieces:]
    if last:
        resid_hbm, normed_hbm, source, parts, extra, resid, normed, in_sems, out_sems = refs
    else:
        resid_hbm, source, parts, resid, in_sems, out_sems = refs
    rows, width = resid.shape
    known = source.shape[0]
    part = parts.shape[2]
    one = jnp.ones((), jnp.bfloat16)
    zero = jnp.zeros((), jnp.bfloat16)
    copies = [pltpu.make_async_copy(base_hbm, resid if last else source.at[pl.ds(0, head_rows), :], in_sems.at[pieces])]
    for index, ref in enumerate(piece_refs):
        there = source.at[pl.ds(head_rows + index // 3 * part, part), :] if index % 3 == 0 else parts.at[index // 3, index % 3 - 1]
        copies.append(pltpu.make_async_copy(ref.at[pl.ds(0, part), :], there, in_sems.at[index]))
    for copy in copies:
        copy.start()
    for copy in copies:
        copy.wait()
    for index in range(pieces // 3):
        span = pl.ds(head_rows + index * part, part)
        source[span, :] = source[span, :] + parts[index, 0] + parts[index, 1]
    if last:
        @pl.when(more[0] > 0)
        def _():
            extra_copy = pltpu.make_async_copy(extra_hbm, extra, in_sems.at[pieces + 1])
            extra_copy.start()
            extra_copy.wait()

    def results(block):
        span = pl.ds(pl.multiple_of(block * 256, 256), 256)
        copies = [pltpu.make_async_copy(resid.at[span, :], resid_hbm.at[span, :], out_sems.at[0])]
        if last:
            copies.append(pltpu.make_async_copy(normed.at[span, :], normed_hbm.at[span, :], out_sems.at[1]))
        return copies

    @pl.loop(0, rows // 256)
    def _(block):
        span = pl.ds(pl.multiple_of(block * 256, 256), 256)

        def add(values, first):
            count = values.shape[0]
            places = lax.broadcasted_iota(jnp.int32, (256, count), 1) + first
            select = jnp.where(places == cols_ref[span, :], one, zero)
            for piece in range(width // 256):
                cols = pl.ds(piece * 256, 256)
                picked = jnp.dot(select, values[:, cols], preferred_element_type=jnp.float32)
                resid[span, cols] = (resid[span, cols].astype(jnp.float32) + picked).astype(jnp.bfloat16)

        if last:
            add(source, first_place)

            @pl.when(more[0] > 0)
            def _():
                add(extra, first_place + known)

            for quarter in range(4):
                rows_here = pl.ds(pl.multiple_of(block * 256 + quarter * 64, 64), 64)
                widened = resid[rows_here, :].astype(jnp.float32)
                inv_rms = lax.rsqrt(jnp.mean(widened * widened, axis=-1, keepdims=True) + EPSILON)
                normed[rows_here, :] = (widened * inv_rms * gain_ref[...]).astype(jnp.bfloat16)
        else:
            normalizer = jnp.asarray(math.sqrt(width), dtype=jnp.bfloat16)
            lanes = lax.broadcasted_iota(jnp.int32, (256, known), 1)
            value = jnp.where(lax.broadcasted_iota(jnp.int32, (1, known), 1) < head_rows, normalizer, one)
            select = jnp.where(lanes == cols_ref[span, :], jnp.broadcast_to(value, (256, known)), zero)
            for piece in range(width // 256):
                cols = pl.ds(piece * 256, 256)
                resid[span, cols] = jnp.dot(select, source[:, cols], preferred_element_type=jnp.float32).astype(jnp.bfloat16)
        for result in results(block):
            result.start()

    @pl.loop(0, rows // 256)
    def _(block):
        for result in results(block):
            result.wait()


def pick_rows(first_place, last, more, cols, gain, base, extra, pieces):
    rows = cols.shape[0]
    width = base.shape[1]
    head_rows = 0 if last else base.shape[0]
    part = pieces[0].shape[0]
    known = head_rows + part * len(pieces) // 3
    vmem = pl.BlockSpec(memory_space=pltpu.VMEM)
    anywhere = pl.BlockSpec(memory_space=pl.ANY)
    shape = jax.ShapeDtypeStruct((rows, width), jnp.bfloat16)
    dma = pltpu.SemaphoreType.DMA
    block = pltpu.VMEM((rows, width), jnp.bfloat16)
    scratch = [pltpu.VMEM((known, width), jnp.bfloat16), pltpu.VMEM((len(pieces) // 3, 2, part, width), jnp.bfloat16)]
    scratch += [pltpu.VMEM(extra.shape, jnp.bfloat16), block, block] if last else [block]
    return pl.pallas_call(
        functools.partial(rows_kernel, len(pieces), head_rows, first_place, last),
        out_shape=(shape, shape) if last else shape,
        in_specs=[pl.BlockSpec(memory_space=pltpu.SMEM), vmem, vmem, anywhere, anywhere] + [anywhere] * len(pieces),
        out_specs=(anywhere, anywhere) if last else anywhere,
        scratch_shapes=scratch + [dma((len(pieces) + 2,)), dma((2,))],
        compiler_params=pltpu.CompilerParams(vmem_limit_bytes=67_043_328),
        cost_estimate=pl.CostEstimate(flops=2 * rows * width * known, bytes_accessed=16_000_000, transcendentals=0),
        name="pick_rows",
    )(more, cols, gain, base, extra, *pieces)


def heads_kernel(rows, normed_hbm, cos_ref, sin_ref, wq_mine, wq_far, wq_near, wk_hbm, wv_hbm, q_out, kv_out,
                 wq, wk, wv, normed, q_stage, kv_stage, w_sem, q_send, q_recv, kv_send, kv_recv,
                 own_recv, fwd_send, fwd_recv, keep_sem):
    group = lax.axis_index("dp")
    me = lax.axis_index("tp")
    core = lax.rem(me, 2)
    chip = me // 2
    partner = me + 1 - 2 * core
    kv_outs = (kv_out.at[0], kv_out.at[1])
    tiles = rows // SEND_ROWS
    half = HEAD_DIM // 2

    depth = wq_mine.shape[1]
    own_depth = pl.ds(pl.multiple_of(group * depth, depth), depth)
    far_depth = pl.ds(pl.multiple_of((1 - group) * depth, depth), depth)
    sources = ((normed_hbm, normed), (wk_hbm, wk), (wv_hbm, wv), (wq_mine, wq.at[:, own_depth, :]),
               (wq_far, wq.at[pl.ds(core * CHIPS, CHIPS), far_depth, :]), (wq_near, wq.at[pl.ds((1 - core) * CHIPS, CHIPS), far_depth, :]))
    loads = [pltpu.make_async_copy(src, dst, w_sem.at[n]) for n, (src, dst) in enumerate(sources)]
    for load in loads[:2]:
        load.start()

    barrier = pltpu.get_barrier_semaphore()
    for step in range(1, 2 * CHIPS):
        pl.semaphore_signal(barrier, inc=1, device_id=(group, lax.rem(me + step, 2 * CHIPS)), device_id_type=MESH_IDS)

    pl.semaphore_wait(barrier, 2 * CHIPS - 1)
    for load in loads[:2]:
        load.wait()
    for load in loads[2:]:
        load.start()

    def block(source, tile):
        return pl.ds(pl.multiple_of(source * rows + tile * SEND_ROWS, SEND_ROWS), SEND_ROWS)

    def whole(source):
        return pl.ds(pl.multiple_of(source * rows, rows), rows)

    def remote(src, dst, send, recv, device):
        return pltpu.make_async_remote_copy(src_ref=src, dst_ref=dst, send_sem=send, recv_sem=recv, device_id=(group, device), device_id_type=MESH_IDS)

    def rotated(linear, span, factor):
        front = linear[:, :half]
        back = linear[:, half:]
        cosines = cos_ref[span, :]
        sines = sin_ref[span, :]
        return jnp.concatenate([((front * cosines - back * sines) * factor).astype(jnp.bfloat16), ((back * cosines + front * sines) * factor).astype(jnp.bfloat16)], axis=-1)

    @pl.loop(0, CHIPS * tiles)
    def _(turn):
        offset = lax.rem(turn // tiles + 1, CHIPS)
        tile = lax.rem(turn, tiles)
        there = lax.rem(chip + offset, CHIPS)
        columns = pl.ds(pl.multiple_of(there * HEAD_DIM, HEAD_DIM), HEAD_DIM)
        sent = pl.ds(pl.multiple_of(tile * SEND_ROWS, SEND_ROWS), SEND_ROWS)

        @pl.loop(0, SEND_ROWS // 256)
        def _(part):
            span = pl.ds(pl.multiple_of(tile * SEND_ROWS + part * 256, 256), 256)
            lhs = normed[span, :]

            def linear(weight):
                return jnp.dot(lhs, weight, preferred_element_type=jnp.float32).astype(jnp.bfloat16)

            def arrived(weights):
                @pl.when(turn + part == 0)
                def _():
                    for load in weights:
                        load.wait()

            kv_stage[0, there, span, :] = rotated(linear(wk[:, columns]).astype(jnp.float32), span, 1.0)
            arrived(loads[2:3])
            kv_stage[1, there, span, :] = linear(wv[:, columns])
            arrived(loads[3:])
            for side in range(2):
                q_stage[2 * there + side, span, :] = rotated(linear(wq[2 * there + side]).astype(jnp.float32), span, HEAD_DIM ** -0.5)

        @pl.when(offset != 0)
        def _():
            for side in range(2):
                remote(kv_stage.at[side, there, sent, :], kv_outs[side].at[block(me, tile), :], kv_send.at[offset, side], kv_recv.at[offset, core, tile], 2 * there + side).start()
            for side in range(2):
                remote(q_stage.at[2 * there + side, sent, :], q_out.at[block(me, tile), :], q_send.at[offset, side], q_recv.at[offset, core], 2 * there + side).start()

    for side in range(2):
        remote(kv_stage.at[side, chip], kv_outs[side].at[whole(me), :], kv_send.at[0, side], own_recv.at[side], partner).start()
    remote(q_stage.at[partner], q_out.at[whole(me), :], q_send.at[0, 0], q_recv.at[0, 0], partner).start()
    keeps = [pltpu.make_async_copy(q_stage.at[me], q_out.at[whole(me), :], keep_sem.at[0])]
    for side in range(2):
        keeps.append(pltpu.make_async_copy(kv_stage.at[side, chip], kv_outs[side].at[whole(me), :], keep_sem.at[1 + side]))
    for keep in keeps:
        keep.start()

    def forward(mine_out, other_out):
        for tile in range(tiles):
            for offset in range(1, CHIPS):
                for side in range(2):
                    source = 2 * lax.rem(chip + CHIPS - offset, CHIPS) + side
                    region = mine_out.at[block(source, tile), :]
                    remote(region, region, kv_send.at[offset, side], kv_recv.at[offset, side, tile], partner).wait_recv()
                    remote(region, region, fwd_send.at[offset, side], fwd_recv.at[offset, side], partner).start()
        for offset in range(1, CHIPS):
            for side in range(2):
                source = 2 * lax.rem(chip + CHIPS - offset, CHIPS) + side
                mine = mine_out.at[whole(source), :]
                remote(mine, mine, fwd_send.at[offset, side], fwd_recv.at[offset, side], partner).wait_send()
                other = other_out.at[whole(source), :]
                remote(other, other, fwd_send.at[offset, side], fwd_recv.at[offset, side], partner).wait_recv()

    forward(kv_out.at[core], kv_out.at[1 - core])

    for keep in keeps:
        keep.wait()
    for offset in range(1, CHIPS):
        there = lax.rem(chip + offset, CHIPS)
        for side in range(2):
            source = 2 * lax.rem(chip + CHIPS - offset, CHIPS) + side
            remote(kv_stage.at[side, there], kv_outs[side].at[whole(me), :], kv_send.at[offset, side], own_recv.at[side], partner).wait_send()
            remote(q_stage.at[2 * there + side], q_out.at[whole(source), :], q_send.at[offset, side], q_recv.at[offset, side], partner).wait()
    for side in range(2):
        remote(kv_stage.at[side, chip], kv_outs[side].at[whole(partner), :], kv_send.at[0, side], own_recv.at[side], partner).wait()
    remote(q_stage.at[partner], q_out.at[whole(partner), :], q_send.at[0, 0], q_recv.at[0, 0], partner).wait()


def project_heads(normed, cosines, sines, wq_parts, w_key, w_value):
    rows, width = normed.shape
    heads = wq_parts[0].shape[0]
    tokens = rows * heads
    tiles = rows // SEND_ROWS
    vmem = pl.BlockSpec(memory_space=pltpu.VMEM)
    anywhere = pl.BlockSpec(memory_space=pl.ANY)
    dma = pltpu.SemaphoreType.DMA
    return pl.pallas_call(
        functools.partial(heads_kernel, rows),
        out_shape=(jax.ShapeDtypeStruct((tokens, HEAD_DIM), jnp.bfloat16), jax.ShapeDtypeStruct((2, tokens, HEAD_DIM), jnp.bfloat16)),
        in_specs=[anywhere, vmem, vmem] + [anywhere] * 5,
        out_specs=(anywhere, anywhere),
        scratch_shapes=[
            pltpu.VMEM((heads, width, HEAD_DIM), jnp.bfloat16),
            pltpu.VMEM(w_key.shape, jnp.bfloat16),
            pltpu.VMEM(w_value.shape, jnp.bfloat16),
            pltpu.VMEM((rows, width), jnp.bfloat16),
            pltpu.VMEM((heads, rows, HEAD_DIM), jnp.bfloat16),
            pltpu.VMEM((2, CHIPS, rows, HEAD_DIM), jnp.bfloat16),
            dma((6,)),
            dma((CHIPS, 2)), dma((CHIPS, 2)),
            dma((CHIPS, 2)), dma((CHIPS, 2, tiles)),
            dma((2,)),
            dma((CHIPS, 2)), dma((CHIPS, 2)),
            dma((3,)),
        ],
        compiler_params=pltpu.CompilerParams(collective_id=0, has_side_effects=True, vmem_limit_bytes=67_043_328),
        cost_estimate=pl.CostEstimate(flops=2 * rows * width * 4096, bytes_accessed=40_000_000, transcendentals=0),
        name="project_heads",
    )(normed, cosines, sines, *wq_parts, w_key, w_value)


def solution(mesh):
    group_size = mesh.shape["tp"]

    def exchange(rows, bit):
        return lax.ppermute(rows, "tp", [(i, i ^ bit) for i in range(group_size)])

    def pass_head(values, pairs, after=None):
        got = lax.ppermute(values, "tp", pairs)
        if after is not None:
            got, _ = lax.optimization_barrier((got, after))
        return jnp.where(lax.axis_index("tp") == pairs[0][1], got, values)

    def share_head(rows):
        half = rows.shape[0] // 2
        first = pass_head(rows[:half], [(0, 2)])
        second = pass_head(rows[half:], [(0, 4)])
        first = pass_head(first, [(2, 6)])
        second = pass_head(second, [(4, 6)])
        return first, second

    def share_head_back(first, second, after):
        first = pass_head(first, [(6, 4)], after)
        second = pass_head(second, [(6, 2)], after)
        both = jnp.concatenate([first, second], axis=0)
        other = lax.ppermute(both, "tp", [(0, 1), (2, 3), (4, 5), (6, 7)])
        return jnp.where(lax.axis_index("tp") % 2 == 1, other, both)

    def local_body(token_ids, positions, table_rows, norm_scale, w_query, w_key, w_value):
        dev_index = lax.axis_index("tp")
        vocab_rows, model_width = table_rows.shape
        group = lax.axis_index("dp")
        core = dev_index % 2
        part_rows = w_query.shape[0] // 2
        wq_mine = lax.all_gather(lax.dynamic_slice_in_dim(w_query, group * part_rows, part_rows, axis=0), "tp", axis=0)
        wq_far = lax.ppermute(lax.dynamic_slice_in_dim(wq_mine, core * (group_size // 2), group_size // 2, axis=0), "dp", [(0, 1), (1, 0)])
        wq_near = exchange(wq_far, 1)
        head_halves = share_head(table_rows[:HEAD_ROWS])
        tokens = token_ids.shape[0]
        block_rows = tokens // group_size
        extra_rows = block_rows - TAIL_ROWS
        chunk_rows = TAIL_ROWS // CHUNKS
        half = chunk_rows // 2

        blocks = token_ids.reshape(group_size, block_rows)
        in_tail = blocks >= HEAD_ROWS
        earlier = (lax.broadcasted_iota(jnp.int32, (block_rows, block_rows), 0) < lax.broadcasted_iota(jnp.int32, (block_rows, block_rows), 1)).astype(jnp.bfloat16)
        ranks = jnp.dot(in_tail.astype(jnp.bfloat16), earlier, preferred_element_type=jnp.float32).astype(jnp.int32)
        ranks = jnp.where(in_tail, ranks, -1)

        def ranked_ids(first, count):
            wanted = lax.broadcasted_iota(jnp.int32, (group_size, block_rows, count), 2) + first
            ids = jnp.sum(jnp.where(ranks[:, :, None] == wanted, blocks[:, :, None] + 1, 0), axis=1) - 1
            local = ids - dev_index * vocab_rows
            return jnp.where((ids >= 0) & (local >= 0) & (local < vocab_rows), local, -1)

        most = jnp.max(jnp.sum(in_tail.astype(jnp.int32), axis=1))
        over = (most > TAIL_ROWS).astype(jnp.int32)

        def arrange(values):
            view = values.reshape(2, 2, 2, CHUNKS, 2, half)
            for axis, bit in ((0, 4), (1, 2), (2, 1)):
                flag = (dev_index // bit) % 2 == 1
                view = jnp.where(flag, jnp.flip(view, axis), view)
            halves = view.transpose(3, 2, 4, 0, 1, 5)
            first = halves[:, :, 0].transpose(0, 1, 3, 2, 4)
            second = halves[:, :, 1]
            return jnp.stack([first, second], axis=2).reshape(CHUNKS, 2, 4 * chunk_rows)

        call_rows = 4 * chunk_rows
        ids = arrange(ranked_ids(0, TAIL_ROWS)).reshape(-1, TILE)
        owned = ids >= 0
        before = (lax.broadcasted_iota(jnp.int32, (TILE, TILE), 0) < lax.broadcasted_iota(jnp.int32, (TILE, TILE), 1)).astype(jnp.bfloat16)
        slots = jnp.dot(owned.astype(jnp.bfloat16), before, preferred_element_type=jnp.float32).astype(jnp.int32)
        slots = jnp.where(owned, slots, -1)
        wanted_slot = lax.broadcasted_iota(jnp.int32, (ids.shape[0], TILE, TILE), 2)
        pair_ids = jnp.sum(jnp.where(slots[:, :, None] == wanted_slot, (ids // 2)[:, :, None] * 2, 0), axis=1).reshape(-1)
        cols = jnp.where(owned, 2 * slots + ids % 2, -1).astype(jnp.float32)[:, None, :]
        counts = jnp.sum(owned.astype(jnp.int32), axis=-1)

        def gather(chunk, side, after):
            return gather_rows((2 * chunk + side) * call_rows, call_rows, pair_ids, counts, cols, table_rows, after)

        pieces, sums = [], []
        after, late, late_next = [], [], []
        for chunk in range(CHUNKS):
            other = gather(chunk, 1, after + late + ([wq_mine] if chunk == CHUNKS - 1 else []))
            got = exchange(other, 1)
            mine = gather(chunk, 0, [other])
            after, late = [], late_next
            late_next = []
            spans = []
            for part in range(2):
                first_row = part * 4 * half
                spans += [slice(first_row, first_row + half), slice(first_row + half, first_row + 2 * half), slice(first_row + 2 * half, first_row + 4 * half)]
            both = lax.optimization_barrier([mine[span] + got[span] for span in spans])
            for part, bits in ((0, (2, 4)), (1, (4, 2))):
                kept, near, sent = both[3 * part:3 * part + 3]
                back = exchange(sent, bits[0])
                near_send = near + back[half:]
                back2 = exchange(near_send, bits[1])
                after.append(sent)
                sums.append(near_send)
                late_next.append(near_send)
                pieces += [kept, back, back2]

        head = share_head_back(*head_halves, sums[1])

        def second_exchange(rows):
            ids = ranked_ids(TAIL_ROWS, extra_rows).reshape(-1)
            normalizer = jnp.asarray(math.sqrt(model_width), dtype=jnp.bfloat16)
            picked = jnp.take(rows, jnp.maximum(ids, 0), axis=0, mode="clip") * normalizer
            partial = jnp.where(ids[:, None] >= 0, picked, jnp.zeros((), jnp.bfloat16))
            return lax.psum_scatter(partial, "tp", scatter_dimension=0, tiled=True)

        def no_exchange(rows):
            return jnp.zeros((extra_rows, model_width), jnp.bfloat16)

        over, _ = lax.optimization_barrier((over, sums[1]))
        more = lax.pmax(over, "dp")
        extra = lax.cond(more > 0, second_exchange, no_exchange, table_rows)
        places = jnp.where(in_tail, HEAD_ROWS + ranks, blocks)
        own_places = lax.dynamic_index_in_dim(places, dev_index, 0, keepdims=False)
        asked, own_cols, gain = more.reshape(1), own_places[:, None], (1.0 + norm_scale)[None, :]
        split = len(pieces) // CHUNKS
        started = pick_rows(0, False, asked, own_cols, gain, head, extra, pieces[:split])
        residual, normed = pick_rows(HEAD_ROWS + TAIL_ROWS // CHUNKS, True, asked, own_cols, gain, started, extra, pieces[split:])
        own = lax.dynamic_slice_in_dim(positions, dev_index * block_rows, block_rows)
        cosines, sines = rope_tables(own)
        queries, keys_values = project_heads(normed, cosines, sines, (wq_mine, wq_far, wq_near), w_key, w_value)
        return residual, queries[:, None, :], keys_values[0][:, None, :], keys_values[1][:, None, :]

    head_spec = P("dp", "tp", None)
    return jax.shard_map(local_body, mesh=mesh, in_specs=(P("dp"), P("dp"), P("tp", None), P(), P(None, "tp"), P(), P()), out_specs=(P(("dp", "tp"), None), head_spec, head_spec, head_spec), check_vma=False)
```

```python
import functools
import math
import jax
import jax.numpy as jnp
from jax import lax
from jax.experimental import pallas as pl
from jax.experimental.pallas import tpu as pltpu
from jax.sharding import PartitionSpec as P

HEAD_DIM = 256
EPSILON = 1e-6
ROPE_BASE = 10000.0
TILE = 128
CHUNKS = 2
HEAD_ROWS = 512
TAIL_ROWS = 640
SEND_ROWS = 256
CHIPS = 4
MESH_IDS = pl.DeviceIdType.MESH


def rope_tables(positions):
    inv_freq = ROPE_BASE ** (-jnp.arange(0, HEAD_DIM, 2, dtype=jnp.float32) / HEAD_DIM)
    angles = positions.astype(jnp.float32)[:, None] * inv_freq[None, :]
    return jnp.cos(angles), jnp.sin(angles)


def gather_kernel(base, tiles, width, pair_ids, counts, cols_ref, table_ref, *rest):
    out_ref, pairs, sems = rest[-3:]
    step = pl.program_id(0)
    normalizer = jnp.asarray(math.sqrt(width), dtype=jnp.bfloat16)

    def start(tile, slot):
        count = counts[base + tile]

        def copy(group, row):
            src = pair_ids[(base + tile) * TILE + group * 8 + row]
            pltpu.make_async_copy(table_ref.at[pl.ds(pl.multiple_of(src, 2), 2), :], pairs.at[slot, group, pl.ds(2 * row, 2), :], sems.at[slot]).start()

        @pl.loop(0, count // 8)
        def _(group):
            for row in range(8):
                copy(group, row)

        for row in range(7):
            @pl.when(row < lax.rem(count, 8))
            def _():
                copy(count // 8, row)

    def wait(tile, slot):
        count = counts[base + tile]
        size = TILE // 8
        while size:
            @pl.when((count // (8 * size)) % 2 == 1)
            def _():
                pltpu.make_async_copy(pairs.at[slot, pl.ds(0, size)], pairs.at[slot, pl.ds(0, size)], sems.at[slot]).wait()

            size //= 2
        for size in (1, 2, 4):
            @pl.when((count // size) % 2 == 1)
            def _():
                pltpu.make_async_copy(table_ref.at[pl.ds(0, 2 * size), :], pairs.at[slot, 0, pl.ds(0, 2 * size), :], sems.at[slot]).wait()

    @pl.when(step == 0)
    def _():
        pairs[...] = jnp.zeros_like(pairs)
        start(0, 0)
        start(1, 1)

    slot = lax.rem(step, 3)

    @pl.when(step + 2 < tiles)
    def _():
        start(step + 2, lax.rem(step + 2, 3))

    wait(step, slot)
    lanes = lax.broadcasted_iota(jnp.int32, (TILE, 2 * TILE), 1).astype(jnp.float32)
    wanted = jnp.broadcast_to(cols_ref[base + step], (TILE, TILE)).T
    select = jnp.where(lanes == jnp.concatenate([wanted, wanted], axis=1), normalizer, jnp.zeros((), jnp.bfloat16))
    for piece in range(width // 256):
        cols = pl.ds(piece * 256, 256)
        picked = jnp.dot(select, pairs[slot, :, :, cols].reshape(2 * TILE, 256), preferred_element_type=jnp.float32)
        out_ref[:, cols] = picked.astype(jnp.bfloat16)


def gather_rows(base, count, pair_ids, counts, cols, table_rows, after):
    width = table_rows.shape[1]
    tiles = count // TILE
    base = base // TILE
    anywhere = pl.BlockSpec(memory_space=pl.ANY)
    grid_spec = pltpu.PrefetchScalarGridSpec(
        num_scalar_prefetch=2,
        grid=(tiles,),
        in_specs=[pl.BlockSpec(cols.shape, lambda i, *_: (0, 0, 0)), anywhere] + [anywhere] * len(after),
        out_specs=pl.BlockSpec((TILE, width), lambda i, *_: (i, 0)),
        scratch_shapes=[pltpu.VMEM((3, TILE // 8, 16, width), jnp.bfloat16), pltpu.SemaphoreType.DMA((3,))],
    )
    return pl.pallas_call(
        functools.partial(gather_kernel, base, tiles, width),
        grid_spec=grid_spec,
        out_shape=jax.ShapeDtypeStruct((count, width), jnp.bfloat16),
        compiler_params=pltpu.CompilerParams(dimension_semantics=("arbitrary",)),
        cost_estimate=pl.CostEstimate(flops=count * 20_000_000, bytes_accessed=count * width * 6, transcendentals=0),
        name="gather_rows",
    )(pair_ids, counts, cols, table_rows, *after)


def rows_kernel(pieces, head_rows, first_place, last, more, cols_ref, gain_ref, base_hbm, extra_hbm, *refs):
    piece_refs, refs = refs[:pieces], refs[pieces:]
    if last:
        resid_hbm, normed_hbm, source, parts, extra, resid, normed, in_sems, out_sems = refs
    else:
        resid_hbm, source, parts, resid, in_sems, out_sems = refs
    rows, width = resid.shape
    known = source.shape[0]
    part = parts.shape[2]
    one = jnp.ones((), jnp.bfloat16)
    zero = jnp.zeros((), jnp.bfloat16)
    copies = [pltpu.make_async_copy(base_hbm, resid if last else source.at[pl.ds(0, head_rows), :], in_sems.at[pieces])]
    for index, ref in enumerate(piece_refs):
        there = source.at[pl.ds(head_rows + index // 3 * part, part), :] if index % 3 == 0 else parts.at[index // 3, index % 3 - 1]
        copies.append(pltpu.make_async_copy(ref.at[pl.ds(0, part), :], there, in_sems.at[index]))
    for copy in copies:
        copy.start()
    for copy in copies:
        copy.wait()
    for index in range(pieces // 3):
        span = pl.ds(head_rows + index * part, part)
        source[span, :] = source[span, :] + parts[index, 0] + parts[index, 1]
    if last:
        @pl.when(more[0] > 0)
        def _():
            extra_copy = pltpu.make_async_copy(extra_hbm, extra, in_sems.at[pieces + 1])
            extra_copy.start()
            extra_copy.wait()

    def results(block):
        span = pl.ds(pl.multiple_of(block * 256, 256), 256)
        copies = [pltpu.make_async_copy(resid.at[span, :], resid_hbm.at[span, :], out_sems.at[0])]
        if last:
            copies.append(pltpu.make_async_copy(normed.at[span, :], normed_hbm.at[span, :], out_sems.at[1]))
        return copies

    @pl.loop(0, rows // 256)
    def _(block):
        span = pl.ds(pl.multiple_of(block * 256, 256), 256)

        def add(values, first):
            count = values.shape[0]
            places = lax.broadcasted_iota(jnp.int32, (256, count), 1) + first
            select = jnp.where(places == cols_ref[span, :], one, zero)
            for piece in range(width // 256):
                cols = pl.ds(piece * 256, 256)
                picked = jnp.dot(select, values[:, cols], preferred_element_type=jnp.float32)
                resid[span, cols] = (resid[span, cols].astype(jnp.float32) + picked).astype(jnp.bfloat16)

        if last:
            add(source, first_place)

            @pl.when(more[0] > 0)
            def _():
                add(extra, first_place + known)

            for quarter in range(4):
                rows_here = pl.ds(pl.multiple_of(block * 256 + quarter * 64, 64), 64)
                widened = resid[rows_here, :].astype(jnp.float32)
                inv_rms = lax.rsqrt(jnp.mean(widened * widened, axis=-1, keepdims=True) + EPSILON)
                normed[rows_here, :] = (widened * inv_rms * gain_ref[...]).astype(jnp.bfloat16)
        else:
            normalizer = jnp.asarray(math.sqrt(width), dtype=jnp.bfloat16)
            lanes = lax.broadcasted_iota(jnp.int32, (256, known), 1)
            value = jnp.where(lax.broadcasted_iota(jnp.int32, (1, known), 1) < head_rows, normalizer, one)
            select = jnp.where(lanes == cols_ref[span, :], jnp.broadcast_to(value, (256, known)), zero)
            for piece in range(width // 256):
                cols = pl.ds(piece * 256, 256)
                resid[span, cols] = jnp.dot(select, source[:, cols], preferred_element_type=jnp.float32).astype(jnp.bfloat16)
        for result in results(block):
            result.start()

    @pl.loop(0, rows // 256)
    def _(block):
        for result in results(block):
            result.wait()


def pick_rows(first_place, last, more, cols, gain, base, extra, pieces):
    rows = cols.shape[0]
    width = base.shape[1]
    head_rows = 0 if last else base.shape[0]
    part = pieces[0].shape[0]
    known = head_rows + part * len(pieces) // 3
    vmem = pl.BlockSpec(memory_space=pltpu.VMEM)
    anywhere = pl.BlockSpec(memory_space=pl.ANY)
    shape = jax.ShapeDtypeStruct((rows, width), jnp.bfloat16)
    dma = pltpu.SemaphoreType.DMA
    block = pltpu.VMEM((rows, width), jnp.bfloat16)
    scratch = [pltpu.VMEM((known, width), jnp.bfloat16), pltpu.VMEM((len(pieces) // 3, 2, part, width), jnp.bfloat16)]
    scratch += [pltpu.VMEM(extra.shape, jnp.bfloat16), block, block] if last else [block]
    return pl.pallas_call(
        functools.partial(rows_kernel, len(pieces), head_rows, first_place, last),
        out_shape=(shape, shape) if last else shape,
        in_specs=[pl.BlockSpec(memory_space=pltpu.SMEM), vmem, vmem, anywhere, anywhere] + [anywhere] * len(pieces),
        out_specs=(anywhere, anywhere) if last else anywhere,
        scratch_shapes=scratch + [dma((len(pieces) + 2,)), dma((2,))],
        compiler_params=pltpu.CompilerParams(vmem_limit_bytes=67_043_328),
        cost_estimate=pl.CostEstimate(flops=2 * rows * width * known, bytes_accessed=16_000_000, transcendentals=0),
        name="pick_rows",
    )(more, cols, gain, base, extra, *pieces)


def heads_kernel(rows, normed_hbm, cos_ref, sin_ref, wq_mine, wq_far, wq_near, wk_hbm, wv_hbm, q_out, kv_out,
                 wq, wk, wv, normed, q_stage, kv_stage, w_sem, q_send, q_recv, kv_send, kv_recv,
                 own_recv, fwd_send, fwd_recv, keep_sem):
    group = lax.axis_index("dp")
    me = lax.axis_index("tp")
    core = lax.rem(me, 2)
    chip = me // 2
    partner = me + 1 - 2 * core
    kv_outs = (kv_out.at[0], kv_out.at[1])
    tiles = rows // SEND_ROWS
    half = HEAD_DIM // 2

    depth = wq_mine.shape[1]
    own_depth = pl.ds(pl.multiple_of(group * depth, depth), depth)
    far_depth = pl.ds(pl.multiple_of((1 - group) * depth, depth), depth)
    sources = ((normed_hbm, normed), (wk_hbm, wk), (wv_hbm, wv), (wq_mine, wq.at[:, own_depth, :]),
               (wq_far, wq.at[pl.ds(core * CHIPS, CHIPS), far_depth, :]), (wq_near, wq.at[pl.ds((1 - core) * CHIPS, CHIPS), far_depth, :]))
    loads = [pltpu.make_async_copy(src, dst, w_sem.at[n]) for n, (src, dst) in enumerate(sources)]
    for load in loads:
        load.start()

    barrier = pltpu.get_barrier_semaphore()
    for step in range(1, 2 * CHIPS):
        pl.semaphore_signal(barrier, inc=1, device_id=(group, lax.rem(me + step, 2 * CHIPS)), device_id_type=MESH_IDS)

    pl.semaphore_wait(barrier, 2 * CHIPS - 1)
    for load in loads:
        load.wait()

    def block(source, tile):
        return pl.ds(pl.multiple_of(source * rows + tile * SEND_ROWS, SEND_ROWS), SEND_ROWS)

    def whole(source):
        return pl.ds(pl.multiple_of(source * rows, rows), rows)

    def remote(src, dst, send, recv, device):
        return pltpu.make_async_remote_copy(src_ref=src, dst_ref=dst, send_sem=send, recv_sem=recv, device_id=(group, device), device_id_type=MESH_IDS)

    def rotated(linear, span, factor):
        front = linear[:, :half]
        back = linear[:, half:]
        cosines = cos_ref[span, :]
        sines = sin_ref[span, :]
        return jnp.concatenate([((front * cosines - back * sines) * factor).astype(jnp.bfloat16), ((back * cosines + front * sines) * factor).astype(jnp.bfloat16)], axis=-1)

    @pl.loop(0, CHIPS * tiles)
    def _(turn):
        offset = lax.rem(turn // tiles + 1, CHIPS)
        tile = lax.rem(turn, tiles)
        there = lax.rem(chip + offset, CHIPS)
        columns = pl.ds(pl.multiple_of(there * HEAD_DIM, HEAD_DIM), HEAD_DIM)
        sent = pl.ds(pl.multiple_of(tile * SEND_ROWS, SEND_ROWS), SEND_ROWS)

        @pl.loop(0, SEND_ROWS // 256)
        def _(part):
            span = pl.ds(pl.multiple_of(tile * SEND_ROWS + part * 256, 256), 256)
            lhs = normed[span, :]

            def linear(weight):
                return jnp.dot(lhs, weight, preferred_element_type=jnp.float32).astype(jnp.bfloat16)

            kv_stage[0, there, span, :] = rotated(linear(wk[:, columns]).astype(jnp.float32), span, 1.0)
            kv_stage[1, there, span, :] = linear(wv[:, columns])
            for side in range(2):
                q_stage[2 * there + side, span, :] = rotated(linear(wq[2 * there + side]).astype(jnp.float32), span, HEAD_DIM ** -0.5)

        @pl.when(offset != 0)
        def _():
            for side in range(2):
                remote(kv_stage.at[side, there, sent, :], kv_outs[side].at[block(me, tile), :], kv_send.at[offset, side], kv_recv.at[offset, core, tile], 2 * there + side).start()
            for side in range(2):
                remote(q_stage.at[2 * there + side, sent, :], q_out.at[block(me, tile), :], q_send.at[offset, side], q_recv.at[offset, core], 2 * there + side).start()

    for side in range(2):
        remote(kv_stage.at[side, chip], kv_outs[side].at[whole(me), :], kv_send.at[0, side], own_recv.at[side], partner).start()
    remote(q_stage.at[partner], q_out.at[whole(me), :], q_send.at[0, 0], q_recv.at[0, 0], partner).start()
    keeps = [pltpu.make_async_copy(q_stage.at[me], q_out.at[whole(me), :], keep_sem.at[0])]
    for side in range(2):
        keeps.append(pltpu.make_async_copy(kv_stage.at[side, chip], kv_outs[side].at[whole(me), :], keep_sem.at[1 + side]))
    for keep in keeps:
        keep.start()

    def forward(mine_out, other_out):
        for tile in range(tiles):
            for offset in range(1, CHIPS):
                for side in range(2):
                    source = 2 * lax.rem(chip + CHIPS - offset, CHIPS) + side
                    region = mine_out.at[block(source, tile), :]
                    remote(region, region, kv_send.at[offset, side], kv_recv.at[offset, side, tile], partner).wait_recv()
                    remote(region, region, fwd_send.at[offset, side], fwd_recv.at[offset, side], partner).start()
        for offset in range(1, CHIPS):
            for side in range(2):
                source = 2 * lax.rem(chip + CHIPS - offset, CHIPS) + side
                mine = mine_out.at[whole(source), :]
                remote(mine, mine, fwd_send.at[offset, side], fwd_recv.at[offset, side], partner).wait_send()
                other = other_out.at[whole(source), :]
                remote(other, other, fwd_send.at[offset, side], fwd_recv.at[offset, side], partner).wait_recv()

    forward(kv_out.at[core], kv_out.at[1 - core])

    for keep in keeps:
        keep.wait()
    for offset in range(1, CHIPS):
        there = lax.rem(chip + offset, CHIPS)
        for side in range(2):
            source = 2 * lax.rem(chip + CHIPS - offset, CHIPS) + side
            remote(kv_stage.at[side, there], kv_outs[side].at[whole(me), :], kv_send.at[offset, side], own_recv.at[side], partner).wait_send()
            remote(q_stage.at[2 * there + side], q_out.at[whole(source), :], q_send.at[offset, side], q_recv.at[offset, side], partner).wait()
    for side in range(2):
        remote(kv_stage.at[side, chip], kv_outs[side].at[whole(partner), :], kv_send.at[0, side], own_recv.at[side], partner).wait()
    remote(q_stage.at[partner], q_out.at[whole(partner), :], q_send.at[0, 0], q_recv.at[0, 0], partner).wait()


def project_heads(normed, cosines, sines, wq_parts, w_key, w_value):
    rows, width = normed.shape
    heads = wq_parts[0].shape[0]
    tokens = rows * heads
    tiles = rows // SEND_ROWS
    vmem = pl.BlockSpec(memory_space=pltpu.VMEM)
    anywhere = pl.BlockSpec(memory_space=pl.ANY)
    dma = pltpu.SemaphoreType.DMA
    return pl.pallas_call(
        functools.partial(heads_kernel, rows),
        out_shape=(jax.ShapeDtypeStruct((tokens, HEAD_DIM), jnp.bfloat16), jax.ShapeDtypeStruct((2, tokens, HEAD_DIM), jnp.bfloat16)),
        in_specs=[anywhere, vmem, vmem] + [anywhere] * 5,
        out_specs=(anywhere, anywhere),
        scratch_shapes=[
            pltpu.VMEM((heads, width, HEAD_DIM), jnp.bfloat16),
            pltpu.VMEM(w_key.shape, jnp.bfloat16),
            pltpu.VMEM(w_value.shape, jnp.bfloat16),
            pltpu.VMEM((rows, width), jnp.bfloat16),
            pltpu.VMEM((heads, rows, HEAD_DIM), jnp.bfloat16),
            pltpu.VMEM((2, CHIPS, rows, HEAD_DIM), jnp.bfloat16),
            dma((6,)),
            dma((CHIPS, 2)), dma((CHIPS, 2)),
            dma((CHIPS, 2)), dma((CHIPS, 2, tiles)),
            dma((2,)),
            dma((CHIPS, 2)), dma((CHIPS, 2)),
            dma((3,)),
        ],
        compiler_params=pltpu.CompilerParams(collective_id=0, has_side_effects=True, vmem_limit_bytes=67_043_328),
        cost_estimate=pl.CostEstimate(flops=2 * rows * width * 4096, bytes_accessed=40_000_000, transcendentals=0),
        name="project_heads",
    )(normed, cosines, sines, *wq_parts, w_key, w_value)


def solution(mesh):
    group_size = mesh.shape["tp"]

    def exchange(rows, bit):
        return lax.ppermute(rows, "tp", [(i, i ^ bit) for i in range(group_size)])

    def pass_head(values, pairs, after=None):
        got = lax.ppermute(values, "tp", pairs)
        if after is not None:
            got, _ = lax.optimization_barrier((got, after))
        return jnp.where(lax.axis_index("tp") == pairs[0][1], got, values)

    def share_head(rows):
        half = rows.shape[0] // 2
        first = pass_head(rows[:half], [(0, 2)])
        second = pass_head(rows[half:], [(0, 4)])
        first = pass_head(first, [(2, 6)])
        second = pass_head(second, [(4, 6)])
        return first, second

    def share_head_back(first, second, after):
        first = pass_head(first, [(6, 4)], after)
        second = pass_head(second, [(6, 2)], after)
        both = jnp.concatenate([first, second], axis=0)
        other = lax.ppermute(both, "tp", [(0, 1), (2, 3), (4, 5), (6, 7)])
        return jnp.where(lax.axis_index("tp") % 2 == 1, other, both)

    def local_body(token_ids, positions, table_rows, norm_scale, w_query, w_key, w_value):
        dev_index = lax.axis_index("tp")
        vocab_rows, model_width = table_rows.shape
        group = lax.axis_index("dp")
        core = dev_index % 2
        part_rows = w_query.shape[0] // 2
        wq_mine = lax.all_gather(lax.dynamic_slice_in_dim(w_query, group * part_rows, part_rows, axis=0), "tp", axis=0)
        wq_far = lax.ppermute(lax.dynamic_slice_in_dim(wq_mine, core * (group_size // 2), group_size // 2, axis=0), "dp", [(0, 1), (1, 0)])
        wq_near = exchange(wq_far, 1)
        head_halves = share_head(table_rows[:HEAD_ROWS])
        tokens = token_ids.shape[0]
        block_rows = tokens // group_size
        extra_rows = block_rows - TAIL_ROWS
        chunk_rows = TAIL_ROWS // CHUNKS
        half = chunk_rows // 2

        blocks = token_ids.reshape(group_size, block_rows)
        in_tail = blocks >= HEAD_ROWS
        earlier = (lax.broadcasted_iota(jnp.int32, (block_rows, block_rows), 0) < lax.broadcasted_iota(jnp.int32, (block_rows, block_rows), 1)).astype(jnp.bfloat16)
        ranks = jnp.dot(in_tail.astype(jnp.bfloat16), earlier, preferred_element_type=jnp.float32).astype(jnp.int32)
        ranks = jnp.where(in_tail, ranks, -1)

        def ranked_ids(first, count):
            wanted = lax.broadcasted_iota(jnp.int32, (group_size, block_rows, count), 2) + first
            ids = jnp.sum(jnp.where(ranks[:, :, None] == wanted, blocks[:, :, None] + 1, 0), axis=1) - 1
            local = ids - dev_index * vocab_rows
            return jnp.where((ids >= 0) & (local >= 0) & (local < vocab_rows), local, -1)

        most = jnp.max(jnp.sum(in_tail.astype(jnp.int32), axis=1))
        over = (most > TAIL_ROWS).astype(jnp.int32)

        def arrange(values):
            view = values.reshape(2, 2, 2, CHUNKS, 2, half)
            for axis, bit in ((0, 4), (1, 2), (2, 1)):
                flag = (dev_index // bit) % 2 == 1
                view = jnp.where(flag, jnp.flip(view, axis), view)
            halves = view.transpose(3, 2, 4, 0, 1, 5)
            first = halves[:, :, 0].transpose(0, 1, 3, 2, 4)
            second = halves[:, :, 1]
            return jnp.stack([first, second], axis=2).reshape(CHUNKS, 2, 4 * chunk_rows)

        call_rows = 4 * chunk_rows
        ids = arrange(ranked_ids(0, TAIL_ROWS)).reshape(-1, TILE)
        owned = ids >= 0
        before = (lax.broadcasted_iota(jnp.int32, (TILE, TILE), 0) < lax.broadcasted_iota(jnp.int32, (TILE, TILE), 1)).astype(jnp.bfloat16)
        slots = jnp.dot(owned.astype(jnp.bfloat16), before, preferred_element_type=jnp.float32).astype(jnp.int32)
        slots = jnp.where(owned, slots, -1)
        wanted_slot = lax.broadcasted_iota(jnp.int32, (ids.shape[0], TILE, TILE), 2)
        pair_ids = jnp.sum(jnp.where(slots[:, :, None] == wanted_slot, (ids // 2)[:, :, None] * 2, 0), axis=1).reshape(-1)
        cols = jnp.where(owned, 2 * slots + ids % 2, -1).astype(jnp.float32)[:, None, :]
        counts = jnp.sum(owned.astype(jnp.int32), axis=-1)

        def gather(chunk, side, after):
            return gather_rows((2 * chunk + side) * call_rows, call_rows, pair_ids, counts, cols, table_rows, after)

        pieces, sums = [], []
        after, late, late_next = [], [], []
        for chunk in range(CHUNKS):
            other = gather(chunk, 1, after + late + ([wq_mine] if chunk == CHUNKS - 1 else []))
            got = exchange(other, 1)
            mine = gather(chunk, 0, [other])
            after, late = [], late_next
            late_next = []
            spans = []
            for part in range(2):
                first_row = part * 4 * half
                spans += [slice(first_row, first_row + half), slice(first_row + half, first_row + 2 * half), slice(first_row + 2 * half, first_row + 4 * half)]
            both = lax.optimization_barrier([mine[span] + got[span] for span in spans])
            for part, bits in ((0, (2, 4)), (1, (4, 2))):
                kept, near, sent = both[3 * part:3 * part + 3]
                back = exchange(sent, bits[0])
                near_send = near + back[half:]
                back2 = exchange(near_send, bits[1])
                after.append(sent)
                sums.append(near_send)
                late_next.append(near_send)
                pieces += [kept, back, back2]

        head = share_head_back(*head_halves, sums[1])

        def second_exchange(rows):
            ids = ranked_ids(TAIL_ROWS, extra_rows).reshape(-1)
            normalizer = jnp.asarray(math.sqrt(model_width), dtype=jnp.bfloat16)
            picked = jnp.take(rows, jnp.maximum(ids, 0), axis=0, mode="clip") * normalizer
            partial = jnp.where(ids[:, None] >= 0, picked, jnp.zeros((), jnp.bfloat16))
            return lax.psum_scatter(partial, "tp", scatter_dimension=0, tiled=True)

        def no_exchange(rows):
            return jnp.zeros((extra_rows, model_width), jnp.bfloat16)

        over, _ = lax.optimization_barrier((over, sums[1]))
        more = lax.pmax(over, "dp")
        extra = lax.cond(more > 0, second_exchange, no_exchange, table_rows)
        places = jnp.where(in_tail, HEAD_ROWS + ranks, blocks)
        own_places = lax.dynamic_index_in_dim(places, dev_index, 0, keepdims=False)
        asked, own_cols, gain = more.reshape(1), own_places[:, None], (1.0 + norm_scale)[None, :]
        split = len(pieces) // CHUNKS
        started = pick_rows(0, False, asked, own_cols, gain, head, extra, pieces[:split])
        residual, normed = pick_rows(HEAD_ROWS + TAIL_ROWS // CHUNKS, True, asked, own_cols, gain, started, extra, pieces[split:])
        own = lax.dynamic_slice_in_dim(positions, dev_index * block_rows, block_rows)
        cosines, sines = rope_tables(own)
        queries, keys_values = project_heads(normed, cosines, sines, (wq_mine, wq_far, wq_near), w_key, w_value)
        return residual, queries[:, None, :], keys_values[0][:, None, :], keys_values[1][:, None, :]

    head_spec = P("dp", "tp", None)
    return jax.shard_map(local_body, mesh=mesh, in_specs=(P("dp"), P("dp"), P("tp", None), P(), P(None, "tp"), P(), P()), out_specs=(P(("dp", "tp"), None), head_spec, head_spec, head_spec), check_vma=False)
```
